128 devices in a mesh: tiles: 32 (over x, y, core), reps: 4 (over z).
Axes of the slice: x: 4, y: 4, z: 4, core: 2. Of those that a mesh axis runs over, the one named last changes fastest.
Arguments:
- tiles_w: bfloat16 [4096, 128, 128], P('tiles'), may hold values from 0.0001 to 4
- tile_worker: int32 [4096], P('tiles'), may hold values from 0 to 15
- tile_owner: int32 [4096], P('tiles'), may hold values from 0 to 31
- owner_block: int32 [32, 32], P('tiles'), may hold values from 0 to 1
- worker_base: float32 [65536], P('tiles'), may hold values from -6 to 6
- worker_noise: float32 [65536], P('tiles'), may hold values from 0.2 to 1.5
- worker_cluster: int32 [65536], P('tiles'), may hold values from 0 to 255
- firm_base: float32 [8192], P('tiles'), may hold values from -6 to 6
- firm_noise: float32 [8192], P('tiles'), may hold values from 0.2 to 1.5
- firm_cluster: int32 [8192], P('tiles'), may hold values from 0 to 255
- signs: int32 [256, 256], P('reps'), may hold values from 0 to 1
- covariates: float32 [8192, 512], P('tiles'), may hold values from -0.0625 to 0.0625
- whitening: float32 [512, 512], replicated, may hold values from -0.25 to 0.25
Outputs:
- worker_effect: float32 [256, 65536], P('reps', 'tiles')
- firm_effect: float32 [256, 8192], P('reps', 'tiles')
- coefficients: float32 [256, 512], P('reps')
- covariance: float32 [512, 512], P('tiles')
The draws below stay inside these ranges and needn't reach their ends.
Inputs may be any that keep to these rules, and one draw needn't show every extreme that they name: `tile_worker`: local worker block of each tile. `tile_owner`: owner of each tile's firm block. `owner_block`: firm block among the owner's 2 blocks. `signs`: a bit that gives the sign 2 b - 1.
All inputs are finite; a program needn't handle non-finite values.
Results may differ from the reference program's by a relative error of at most 0.0023.
Values may be sent and summed in bfloat16 or wider, within the bound.
No kernel may reach another device: no remote copies, remote signals or barrier semaphores. Data moves between devices by JAX's collectives and lax.ppermute only.
A program may use at most 64 MiB of HBM per device.

```python
import math
import jax
import jax.numpy as jnp
import numpy as np
from jax import lax

TILE = 128
TILES_DEV = 128
WORK_BLOCKS = 16
FIRM_BLOCKS = 2
COVARS = 512
CLUSTERS = 256
SWEEPS = 6
TILES = 4096
WORKERS = 65536
FIRMS = 8192
REPLICAS = 256
N_TILES = 32


def draw_tiles_w(key, part):
    tile_shape = (TILES, TILE, TILE)
    key_mask = jax.random.fold_in(key, 701)
    key_strong = jax.random.fold_in(key, 702)
    key_weak = jax.random.fold_in(key, 703)
    resolution = 1 << 20
    cutoff = max(1, min(resolution // 2, 4 * WORK_BLOCKS * resolution // (TILES_DEV * TILE)))
    picked = jax.random.randint(key_mask, tile_shape, 0, resolution) < cutoff
    strong_draw = jax.random.uniform(key_strong, tile_shape, jnp.float32)
    weak_draw = jax.random.uniform(key_weak, tile_shape, jnp.float32)
    weak_value = jnp.exp(jnp.log(0.000101) + weak_draw * (jnp.log(0.02) - jnp.log(0.000101)))
    strong_value = jnp.exp(jnp.log(0.25) + strong_draw * jnp.log(16.0))
    strong_value = jnp.minimum(strong_value, 4.0)
    return jnp.where(picked, strong_value, weak_value).astype(jnp.bfloat16)


def touch_ends(drawn, own_key, smallest, top_value):
    longest = drawn.shape.index(max(drawn.shape))
    spots = []
    for shift in (0, 1):
        where = [jax.random.randint(jax.random.fold_in(own_key, axis), (), 0, length) for axis, length in enumerate(drawn.shape)]
        where[longest] = (where[longest] + shift) % drawn.shape[longest]
        spots.append(tuple(where))
    return drawn.at[spots[0]].set(smallest).at[spots[1]].set(top_value)


def levels(own_key, dims, shards, low, top_value):
    factor_of = 1.0
    for dim, parts in shards:
        steps = jax.random.uniform(jax.random.fold_in(jax.random.fold_in(own_key, 6), dim), (parts,), jnp.float32, low / len(shards), top_value / len(shards))
        factor_of = factor_of * jnp.repeat(jnp.exp(steps), dims[dim] // parts).reshape((-1,) + (1,) * (len(dims) - 1 - dim))
    return factor_of


def rank_table(count, lean):
    loads = [(1 << 20) // math.isqrt(rank ** lean) + 1 for rank in range(1, count + 1)]
    width = 1 + sum(loads) // (1 << 30)
    return np.cumsum(np.array([max(1, weight // width) for weight in loads]))


def ranked_ids(key, dims, count, slope):
    listing = rank_table(count, slope)
    pick = jax.random.randint(jax.random.fold_in(key, 1), dims, 0, int(listing[count - 1]))
    rank = jnp.searchsorted(jnp.asarray(listing, jnp.int32), pick, side="right")
    return jax.random.permutation(jax.random.fold_in(key, 2), count)[rank].astype(jnp.int32)


def noise(stream_key, extent, scale, reach, split=(), kind=jnp.bfloat16):
    entries = jax.random.normal(stream_key, extent, jnp.float32) * scale
    if len(split) > 0:
        entries = levels(stream_key, extent, split, -0.22, 0.18) * entries
    return jnp.clip(entries, min=-reach, max=reach).astype(kind)


def setup_inputs(seed: int = 0) -> dict:
    streams_of = jax.random.split(jax.random.key(seed), 14)
    tiles_w = draw_tiles_w(jax.random.fold_in(streams_of[13], 71), 0)
    tile_worker = touch_ends(ranked_ids(streams_of[1], (TILES,), WORK_BLOCKS, 2), jax.random.fold_in(streams_of[1], 3), 0, WORK_BLOCKS - 1).astype(jnp.int32)
    tile_owner = touch_ends(ranked_ids(streams_of[2], (TILES,), N_TILES, 1), jax.random.fold_in(streams_of[2], 3), 0, N_TILES - 1).astype(jnp.int32)
    owner_block = touch_ends(jax.random.randint(streams_of[3], (N_TILES, N_TILES), 0, FIRM_BLOCKS), jax.random.fold_in(streams_of[3], 1), 0, FIRM_BLOCKS - 1).astype(jnp.int32)
    worker_base = noise(streams_of[4], (WORKERS,), 1.0, 6.0, ((0, 32),), jnp.float32)
    worker_noise = jnp.clip(0.2 + 1.3 * jax.random.uniform(streams_of[5], (WORKERS,), jnp.float32) ** levels(streams_of[5], (WORKERS,), ((0, 32),), -0.2, 0.2), 0.2, 1.5)
    worker_cluster = touch_ends(jax.random.randint(streams_of[6], (WORKERS,), 0, CLUSTERS), jax.random.fold_in(streams_of[6], 1), 0, CLUSTERS - 1).astype(jnp.int32)
    firm_base = noise(streams_of[7], (FIRMS,), 1.0, 6.0, ((0, 32),), jnp.float32)
    firm_noise = jnp.clip(0.2 + 1.3 * jax.random.uniform(streams_of[8], (FIRMS,), jnp.float32) ** levels(streams_of[8], (FIRMS,), ((0, 32),), -0.2, 0.2), 0.2, 1.5)
    firm_cluster = touch_ends(jax.random.randint(streams_of[9], (FIRMS,), 0, CLUSTERS), jax.random.fold_in(streams_of[9], 1), 0, CLUSTERS - 1).astype(jnp.int32)
    signs = touch_ends(jax.random.randint(streams_of[10], (REPLICAS, CLUSTERS), 0, 2), jax.random.fold_in(streams_of[10], 1), 0, 1).astype(jnp.int32)
    covariates = noise(streams_of[11], (FIRMS, COVARS), FIRMS ** -0.5, 0.0625, ((0, 32),), jnp.float32)
    whitening = noise(streams_of[12], (COVARS, COVARS), COVARS ** -0.5, 0.25, (), jnp.float32)
    return {"tiles_w": tiles_w, "tile_worker": tile_worker, "tile_owner": tile_owner, "owner_block": owner_block, "worker_base": worker_base, "worker_noise": worker_noise, "worker_cluster": worker_cluster, "firm_base": firm_base, "firm_noise": firm_noise, "firm_cluster": firm_cluster, "signs": signs, "covariates": covariates, "whitening": whitening}


spectral_bound = 0.8


def chebyshev_weights(sweep_count):
    weights = [1.0]
    if sweep_count > 1:
        weights.append(1.0 / (1.0 - 0.5 * spectral_bound * spectral_bound))
    while len(weights) < sweep_count:
        weights.append(1.0 / (1.0 - 0.25 * spectral_bound * spectral_bound * weights[-1]))
    return weights


def reference(tiles_w, tile_worker, tile_owner, owner_block, worker_base, worker_noise, worker_cluster, firm_base, firm_noise, firm_cluster, signs, covariates, whitening):
    highest = lax.Precision.HIGHEST
    owners_count = N_TILES
    worker_total = owners_count * WORK_BLOCKS
    firm_total = owners_count * FIRM_BLOCKS
    tile_groups = tiles_w.reshape(owners_count, TILES_DEV, TILE, TILE)
    owner_grid = tile_owner.reshape(owners_count, TILES_DEV)
    worker_grid = tile_worker.reshape(owners_count, TILES_DEV)
    source_index = jnp.arange(owners_count, dtype=jnp.int32)[:, None]
    block_grid = (owner_grid * FIRM_BLOCKS + owner_block[source_index, owner_grid]).astype(jnp.int32)
    global_workers = (source_index * WORK_BLOCKS + worker_grid).astype(jnp.int32)
    row_mass = jnp.sum(tiles_w, axis=2, dtype=jnp.float32)
    col_mass = jnp.sum(tiles_w, axis=1, dtype=jnp.float32)
    worker_scale = 1.0 + jax.ops.segment_sum(row_mass, global_workers.reshape(-1), num_segments=worker_total)
    firm_scale = 1.0 + jax.ops.segment_sum(col_mass, block_grid.reshape(-1), num_segments=firm_total)
    flip_table = (2 * signs - 1).astype(jnp.float32)
    worker_outcome = worker_base[None, :] + worker_noise[None, :] * flip_table[:, worker_cluster]
    worker_outcome = worker_outcome.reshape(REPLICAS, worker_total, TILE)
    firm_outcome = firm_base[None, :] + firm_noise[None, :] * flip_table[:, firm_cluster]
    firm_outcome = firm_outcome.reshape(REPLICAS, firm_total, TILE)

    def pull(firm_round):
        def per_group(group_data):
            group_tiles, blocks, local_workers = group_data
            tile_firm = jnp.take(firm_round, blocks, axis=1).astype(jnp.float32)
            pulled = jnp.einsum("twf,rtf->rtw", group_tiles.astype(jnp.float32), tile_firm)
            return jax.ops.segment_sum(jnp.transpose(pulled, (1, 0, 2)), local_workers, num_segments=WORK_BLOCKS)
        sums = lax.map(per_group, (tile_groups, block_grid, worker_grid))
        return jnp.transpose(sums, (2, 0, 1, 3)).reshape(REPLICAS, worker_total, TILE)

    def push(worker_round):
        def per_group(carried, group_data):
            group_tiles, blocks, workers_here = group_data
            tile_values = jnp.take(worker_round, workers_here, axis=1).astype(jnp.float32)
            pushed = jnp.einsum("twf,rtw->rtf", group_tiles.astype(jnp.float32), tile_values)
            return carried + jax.ops.segment_sum(jnp.transpose(pushed, (1, 0, 2)), blocks, num_segments=firm_total), None
        start = jnp.zeros((firm_total, REPLICAS, TILE), jnp.float32)
        summed, _ = lax.scan(per_group, start, (tile_groups, block_grid, global_workers))
        return jnp.transpose(summed, (1, 0, 2))

    omegas = chebyshev_weights(SWEEPS)
    firm_older = jnp.zeros((REPLICAS, firm_total, TILE), jnp.float32)
    firm_newer = firm_older
    worker_now = worker_outcome
    firm_now = firm_older
    for sweep_index in range(SWEEPS):
        if sweep_index == 0:
            worker_now = worker_outcome
        else:
            worker_now = worker_outcome - pull(firm_newer.astype(jnp.bfloat16)) / worker_scale[None]
        firm_sum = push(worker_now.astype(jnp.bfloat16))
        firm_target = firm_outcome - firm_sum / firm_scale[None]
        firm_now = firm_older + omegas[sweep_index] * (firm_target - firm_older)
        firm_older, firm_newer = firm_newer, firm_now
    worker_effect = worker_now.reshape(REPLICAS, WORKERS)
    firm_effect = firm_now.reshape(REPLICAS, FIRMS)
    mixing = jnp.dot(covariates, whitening.T, precision=highest)
    coefficients = jnp.dot(firm_effect, mixing, precision=highest)
    covariance = jnp.dot(coefficients.T, coefficients, precision=highest) / REPLICAS
    return worker_effect, firm_effect, coefficients, covariance
```

```python
import jax
import jax.numpy as jnp
from jax import lax
from jax.experimental import pallas as pl
from jax.experimental.pallas import tpu as pltpu
from jax.sharding import PartitionSpec as P

WORK_BLOCKS = 16
FIRM_BLOCKS = 2
SWEEPS = 6
CELLS = 128
EXTRA = 16
SPECTRAL = 0.8
UNROLL = 8

F32 = jnp.float32
BF16 = jnp.bfloat16
HIGHEST = lax.Precision.HIGHEST

VMEM = pl.BlockSpec(memory_space=pltpu.VMEM)
SMEM = pl.BlockSpec(memory_space=pltpu.SMEM)
PARAMS = pltpu.CompilerParams(vmem_limit_bytes=40 << 20)


def chebyshev_weights(count):
    weights = [1.0, 1.0 / (1.0 - 0.5 * SPECTRAL * SPECTRAL)]
    while len(weights) < count:
        weights.append(1.0 / (1.0 - 0.25 * SPECTRAL * SPECTRAL * weights[-1]))
    return weights


def flip_table(signs_ref):
    return (2 * signs_ref[...] - 1).astype(F32).astype(BF16)


def outcome(flips, base, noise, cluster):
    hot = lax.broadcasted_iota(jnp.int32, (flips.shape[1], CELLS), 0) == cluster
    values = jnp.dot(flips, jnp.where(hot, 1.0, 0.0).astype(BF16), preferred_element_type=F32)
    return base + noise * values


def each_tile(count, step):
    def body(index, carry):
        step(index)
        return carry

    lax.fori_loop(0, count, body, 0, unroll=UNROLL)


def push_tiles(tw, to, w_ref, x_ref, acc_ref):
    acc_ref[...] = jnp.zeros_like(acc_ref)

    def step(t):
        acc_ref[to[t]] += jnp.dot(x_ref[tw[t]], w_ref[t], preferred_element_type=F32)

    each_tile(w_ref.shape[0], step)


def pull_tiles(tw, to, w_ref, f_ref, acc_ref):
    acc_ref[...] = jnp.zeros_like(acc_ref)
    rows = acc_ref.shape[1]

    def step(t):
        values = f_ref[to[t]]
        if rows > values.shape[0]:
            values = jnp.concatenate([values, jnp.ones((rows - values.shape[0], CELLS), BF16)], axis=0)
        acc_ref[tw[t]] += lax.dot_general(
            values, w_ref[t], (((1,), (1,)), ((), ())), preferred_element_type=F32
        )

    each_tile(w_ref.shape[0], step)


def first_kernel(tw, to, ob, w_ref, signs_ref, base_ref, noise_ref, cluster_ref, z_ref, wo_ref, x_ref, acc_ref):
    reps = signs_ref.shape[0]
    flips = flip_table(signs_ref)
    for b in range(WORK_BLOCKS):
        row = slice(b, b + 1)
        value = outcome(flips, base_ref[row], noise_ref[row], cluster_ref[row])
        wo_ref[b] = value
        x_ref[b, :reps] = value.astype(BF16)
        x_ref[b, reps:] = jnp.ones((EXTRA, CELLS), BF16)
    push_tiles(tw, to, w_ref, x_ref, acc_ref)
    place = lax.broadcasted_iota(jnp.int32, (EXTRA, CELLS), 0)

    def finish(o):
        z_ref[o, :reps] = acc_ref[o, :reps].astype(BF16)
        mass = acc_ref[o, reps:]
        high = mass.astype(BF16).astype(F32)
        middle = (mass - high).astype(BF16).astype(F32)
        low = (mass - high) - middle
        flag = ob[0, o].astype(F32)
        tail = jnp.where(place == 0, high, jnp.where(place == 1, middle, jnp.where(place == 2, low, flag)))
        z_ref[o, reps:] = tail.astype(BF16)

    each_tile(acc_ref.shape[0], finish)


def sweep_kernel(measure, last, *refs):
    if measure:
        tw, to, w_ref, f_ref, wo_ref, z_ref, inv_ref, accw_ref, x_ref, accz_ref = refs
    elif last:
        tw, to, w_ref, f_ref, wo_ref, inv_ref, z_ref, out_ref, accw_ref, x_ref, accz_ref = refs
    else:
        tw, to, w_ref, f_ref, wo_ref, inv_ref, z_ref, accw_ref, x_ref, accz_ref = refs
    reps = f_ref.shape[1]
    pull_tiles(tw, to, w_ref, f_ref, accw_ref)
    for b in range(WORK_BLOCKS):
        if measure:
            inverse = 1.0 / (1.0 + accw_ref[b, reps : reps + 8])
            inv_ref[b] = inverse
            inverse = inverse[:1]
        else:
            inverse = inv_ref[b, :1]
        worker = wo_ref[b] - accw_ref[b, :reps] * inverse
        if last:
            out_ref[:, b * CELLS : (b + 1) * CELLS] = worker
        x_ref[b] = worker.astype(BF16)
    push_tiles(tw, to, w_ref, x_ref, accz_ref)
    z_ref[...] = accz_ref[...].astype(BF16)


def gather_sums(z_ref, flags_ref, reps):
    zero = jnp.zeros((reps, CELLS), F32)

    def body(s, carry):
        first, second = carry
        part = z_ref[s, :reps].astype(F32)
        upper = jnp.broadcast_to(flags_ref[s, :1], part.shape) > 0.5
        return first + jnp.where(upper, 0.0, part), second + jnp.where(upper, part, 0.0)

    return lax.fori_loop(0, z_ref.shape[0], body, (zero, zero), unroll=4)


def scatter_firms(firms, flags_ref, send_ref):
    first, second = firms

    def step(s):
        upper = jnp.broadcast_to(flags_ref[s, :1], first.shape) > 0.5
        send_ref[s] = jnp.where(upper, second, first).astype(BF16)

    each_tile(send_ref.shape[0], step)


def open_firm_kernel(z_ref, signs_ref, base_ref, noise_ref, cluster_ref, send_ref, fo_ref, inv_ref, flags_ref, now_ref):
    reps = signs_ref.shape[0]
    owners = z_ref.shape[0]
    mass = [jnp.zeros((1, CELLS), F32), jnp.zeros((1, CELLS), F32)]
    for s in range(owners):
        tail = z_ref[s, reps:].astype(F32)
        flags_ref[s] = jnp.broadcast_to(tail[3:4], (8, CELLS))
        part = tail[0:1] + tail[1:2] + tail[2:3]
        upper = tail[3:4] > 0.5
        mass = [mass[0] + jnp.where(upper, 0.0, part), mass[1] + jnp.where(upper, part, 0.0)]
    sums = gather_sums(z_ref, flags_ref, reps)
    flips = flip_table(signs_ref)
    firms = []
    for j in range(FIRM_BLOCKS):
        row = slice(j, j + 1)
        inverse = 1.0 / (1.0 + mass[j])
        value = outcome(flips, base_ref[row], noise_ref[row], cluster_ref[row])
        fo_ref[j] = value
        inv_ref[j] = jnp.broadcast_to(inverse, (8, CELLS))
        firm = value - sums[j] * inverse
        now_ref[j] = firm
        firms.append(firm)
    scatter_firms(firms, flags_ref, send_ref)


def next_firms(omega, z_ref, fo_ref, inv_ref, flags_ref, older_ref):
    sums = gather_sums(z_ref, flags_ref, z_ref.shape[1])
    firms = []
    for j in range(FIRM_BLOCKS):
        target = fo_ref[j] - sums[j] * inv_ref[j, :1]
        if older_ref is None:
            firms.append(omega * target)
        else:
            firms.append(older_ref[j] + omega * (target - older_ref[j]))
    return firms


def firm_kernel(omega, has_older, *refs):
    if has_older:
        z_ref, fo_ref, inv_ref, flags_ref, older_ref, send_ref, now_ref = refs
    else:
        (z_ref, fo_ref, inv_ref, flags_ref, send_ref, now_ref), older_ref = refs, None
    firms = next_firms(omega, z_ref, fo_ref, inv_ref, flags_ref, older_ref)
    for j in range(FIRM_BLOCKS):
        now_ref[j] = firms[j]
    scatter_firms(firms, flags_ref, send_ref)


def close_firm_kernel(omega, z_ref, fo_ref, inv_ref, flags_ref, older_ref, cov_ref, white_ref, firm_ref, part_ref):
    firms = next_firms(omega, z_ref, fo_ref, inv_ref, flags_ref, older_ref)
    for j in range(FIRM_BLOCKS):
        firm_ref[:, j * CELLS : (j + 1) * CELLS] = firms[j]
    projected = jnp.dot(firm_ref[...], cov_ref[...], precision=HIGHEST, preferred_element_type=F32)
    whitened = lax.dot_general(
        projected, white_ref[...], (((1,), (1,)), ((), ())), precision=HIGHEST, preferred_element_type=F32
    )
    reps = whitened.shape[0]
    columns = whitened.shape[1] // CELLS
    for c in range(columns):
        part_ref[pl.ds(c, reps, stride=columns)] = whitened[:, c * CELLS : (c + 1) * CELLS]


def total_kernel(part_ref, out_ref):
    total = jnp.sum(part_ref[...], axis=0)
    for s in range(out_ref.shape[0]):
        out_ref[s] = total


def closing_kernel(owners, index, all_ref, coef_ref, moment_ref, rows_ref, order_ref):
    share, me = index[0], index[1]
    reps, covars = coef_ref.shape
    columns = covars // CELLS
    rows = all_ref.shape[0] // columns
    spread = rows // reps
    per = reps // owners
    for c in range(columns):
        for i in range(per):
            start = me * (per * columns) + i * columns + c
            piece = all_ref[pl.ds(start, owners, stride=spread * per * columns)]
            order_ref[pl.ds(i, owners, stride=per)] = piece
        coef_ref[:, c * CELLS : (c + 1) * CELLS] = order_ref[...]
    share_rows = moment_ref.shape[0]
    in_block = CELLS // share_rows
    own = all_ref[pl.ds(share // in_block, rows, stride=columns)]
    for c in range(columns):
        other = all_ref[pl.ds(c, rows, stride=columns)]
        rows_ref[:, c * CELLS : (c + 1) * CELLS] = lax.dot_general(
            own, other, (((0,), (0,)), ((), ())), precision=HIGHEST, preferred_element_type=F32
        )
    start = pl.multiple_of((share % in_block) * share_rows, share_rows)
    moment_ref[...] = rows_ref[pl.ds(start, share_rows)] / rows


def call(kernel, inputs, outputs, scratch=(), scalars=0, name=None):
    return pl.pallas_call(
        kernel,
        in_specs=[SMEM] * scalars + [VMEM] * (len(inputs) - scalars),
        out_specs=[VMEM] * len(outputs),
        out_shape=[jax.ShapeDtypeStruct(shape, dtype) for shape, dtype in outputs],
        scratch_shapes=[pltpu.VMEM(shape, dtype) for shape, dtype in scratch],
        compiler_params=PARAMS,
        name=name,
    )(*inputs)


def body(
    tiles_w,
    tile_worker,
    tile_owner,
    owner_block,
    worker_base,
    worker_noise,
    worker_cluster,
    firm_base,
    firm_noise,
    firm_cluster,
    signs,
    covariates,
    whitening,
):
    owners = lax.axis_size("tiles")
    groups = lax.axis_size("reps")
    reps = signs.shape[0]
    covars = whitening.shape[0]
    omegas = chebyshev_weights(SWEEPS)

    def exchange(values, axes="tiles"):
        return lax.all_to_all(values, axes, 0, 0, tiled=True)

    def rows(values):
        return values.reshape(-1, CELLS)

    push_shape = ((owners, reps, CELLS), BF16)
    work_shape = ((WORK_BLOCKS, reps, CELLS), F32)
    firm_shape = ((FIRM_BLOCKS, reps, CELLS), F32)
    z, worker_outcome = call(
        first_kernel,
        (tile_worker, tile_owner, owner_block, tiles_w, signs, rows(worker_base), rows(worker_noise), rows(worker_cluster)),
        (((owners, reps + EXTRA, CELLS), BF16), work_shape),
        (((WORK_BLOCKS, reps + EXTRA, CELLS), BF16), ((owners, reps + EXTRA, CELLS), F32)),
        scalars=3,
        name="first_push",
    )
    z = exchange(z)
    send, firm_outcome, firm_inverse, flags, newer = call(
        open_firm_kernel,
        (z, signs, rows(firm_base), rows(firm_noise), rows(firm_cluster)),
        (push_shape, firm_shape, ((FIRM_BLOCKS, 8, CELLS), F32), ((owners, 8, CELLS), F32), firm_shape),
        name="first_firm",
    )
    older = None
    worker_inverse = None
    scratch = (((WORK_BLOCKS, reps, CELLS), BF16), ((owners, reps, CELLS), F32))
    for k in range(1, SWEEPS):
        measure, last = k == 1, k == SWEEPS - 1
        f = exchange(send)
        inputs = (tile_worker, tile_owner, tiles_w, f, worker_outcome)
        outputs = (push_shape,)
        if measure:
            outputs += (((WORK_BLOCKS, 8, CELLS), F32),)
        else:
            inputs += (worker_inverse,)
        if last:
            outputs += (((reps, WORK_BLOCKS * CELLS), F32),)
        work_rows = reps + EXTRA if measure else reps
        results = call(
            lambda *refs, m=measure, e=last: sweep_kernel(m, e, *refs),
            inputs,
            outputs,
            (((WORK_BLOCKS, work_rows, CELLS), F32),) + scratch,
            scalars=2,
            name="sweep_open" if measure else "sweep_close" if last else "sweep",
        )
        z = results[0]
        if measure:
            worker_inverse = results[1]
        if last:
            worker_effect = results[1]
        z = exchange(z)
        inputs = (z, firm_outcome, firm_inverse, flags) + (() if older is None else (older,))
        if not last:
            send, now = call(
                lambda *refs, w=omegas[k], h=older is not None: firm_kernel(w, h, *refs),
                inputs,
                (push_shape, firm_shape),
                name="firm",
            )
            older, newer = newer, now
        else:
            firm_effect, part = call(
                lambda *refs, w=omegas[k]: close_firm_kernel(w, *refs),
                inputs + (covariates, whitening),
                (((reps, FIRM_BLOCKS * CELLS), F32), ((reps * covars // CELLS, CELLS), F32)),
                name="close_firm",
            )
    part = exchange(part.reshape(owners, -1, CELLS))
    (spread,) = call(total_kernel, (part,), (((owners * groups,) + part.shape[1:], F32),), name="total")
    everything = exchange(spread, ("tiles", "reps"))
    index = jnp.stack([lax.axis_index("tiles"), lax.axis_index("reps")]).astype(jnp.int32)
    coefficients, covariance = call(
        lambda *refs: closing_kernel(owners, *refs),
        (index, everything.reshape(-1, CELLS)),
        (((reps, covars), F32), ((covars // owners, covars), F32)),
        (((CELLS, covars), F32), ((reps, CELLS), F32)),
        scalars=1,
        name="closing",
    )
    return (worker_effect, firm_effect, coefficients, covariance)


def solution(mesh):
    placed = (
        P("tiles", None, None),
        P("tiles"),
        P("tiles"),
        P("tiles", None),
        P("tiles"),
        P("tiles"),
        P("tiles"),
        P("tiles"),
        P("tiles"),
        P("tiles"),
        P("reps", None),
        P("tiles", None),
        P(),
    )
    return jax.shard_map(
        body,
        mesh=mesh,
        in_specs=placed,
        out_specs=(P("reps", "tiles"), P("reps", "tiles"), P("reps", None), P("tiles", None)),
        check_vma=False,
    )
```

```python
import jax
import jax.numpy as jnp
from jax import lax
from jax.experimental import pallas as pl
from jax.experimental.pallas import tpu as pltpu
from jax.sharding import PartitionSpec as P

WORK_BLOCKS = 16
FIRM_BLOCKS = 2
SWEEPS = 6
CELLS = 128
EXTRA = 16
SPECTRAL = 0.8
UNROLL = 64
CHUNKS = 4

F32 = jnp.float32
BF16 = jnp.bfloat16
HIGHEST = lax.Precision.HIGHEST

VMEM = pl.BlockSpec(memory_space=pltpu.VMEM)
SMEM = pl.BlockSpec(memory_space=pltpu.SMEM)
HBM = pl.BlockSpec(memory_space=pltpu.HBM)
PARAMS = pltpu.CompilerParams(vmem_limit_bytes=20 << 20)


def chebyshev_weights(count):
    weights = [1.0, 1.0 / (1.0 - 0.5 * SPECTRAL * SPECTRAL)]
    while len(weights) < count:
        weights.append(1.0 / (1.0 - 0.25 * SPECTRAL * SPECTRAL * weights[-1]))
    return weights


def flip_table(signs_ref):
    return (2 * signs_ref[...] - 1).astype(F32).astype(BF16)


def outcome(flips, base, noise, cluster):
    hot = lax.broadcasted_iota(jnp.int32, (flips.shape[1], CELLS), 0) == cluster
    values = jnp.dot(flips, jnp.where(hot, 1.0, 0.0).astype(BF16), preferred_element_type=F32)
    return base + noise * values


def each_tile(count, step, unroll=UNROLL):
    def body(index, carry):
        step(index)
        return carry

    lax.fori_loop(0, count, body, 0, unroll=min(unroll, count))


def add_tiles(first, count, source, target, w_ref, x_ref, acc_ref):
    def step(i):
        t = first + i
        acc_ref[target[t]] += jnp.dot(x_ref[source[t]], w_ref[t], preferred_element_type=F32)

    each_tile(count, step)


def first_kernel(
    tw_hbm, to_hbm, ob_hbm, w_hbm, signs_hbm, base_hbm, noise_hbm, cluster_hbm,
    z_ref, wo_ref, turned_ref, inv_ref,
    tw, to, ob, signs_ref, base_ref, noise_ref, cluster_ref, w_ref, x_ref, acc_ref, mass_ref, sems,
):
    small = [
        (signs_hbm, signs_ref),
        (cluster_hbm, cluster_ref),
        (base_hbm, base_ref),
        (noise_hbm, noise_ref),
        (tw_hbm, tw),
        (to_hbm, to),
        (ob_hbm, ob),
    ]
    copies = [pltpu.make_async_copy(source, target, sems.at[i]) for i, (source, target) in enumerate(small)]
    chunk = w_ref.shape[0] // CHUNKS
    loads = []
    for c in range(CHUNKS):
        part = pl.ds(c * chunk, chunk)
        loads.append(pltpu.make_async_copy(w_hbm.at[part], w_ref.at[part], sems.at[len(small) + c]))
    for copy in copies + loads:
        copy.start()
    acc_ref[...] = jnp.zeros_like(acc_ref)
    mass_ref[...] = jnp.zeros_like(mass_ref)
    for copy in copies:
        copy.wait()
    reps = signs_ref.shape[0]
    flips = flip_table(signs_ref)
    for b in range(WORK_BLOCKS):
        row = slice(b, b + 1)
        value = outcome(flips, base_ref[row], noise_ref[row], cluster_ref[row])
        wo_ref[b] = value
        x_ref[b, :reps] = value.astype(BF16)
        x_ref[b, reps:] = jnp.ones((EXTRA, CELLS), BF16)

    def step(t):
        tile = w_ref[t]
        acc_ref[to[t]] += jnp.dot(x_ref[tw[t]], tile, preferred_element_type=F32)
        turned = tile.T
        turned_ref[t] = turned
        mass_ref[tw[t]] += jnp.sum(turned.astype(F32).reshape(CELLS // 8, 8, CELLS), axis=0)

    for c in range(CHUNKS):
        loads[c].wait()
        each_tile(chunk, lambda i, c=c: step(c * chunk + i))
    for b in range(WORK_BLOCKS):
        inverse = 1.0 / (1.0 + jnp.sum(mass_ref[b], axis=0, keepdims=True))
        inv_ref[b] = jnp.broadcast_to(inverse, (8, CELLS))
    place = lax.broadcasted_iota(jnp.int32, (EXTRA, CELLS), 0)

    def finish(o):
        z_ref[o, :reps] = acc_ref[o, :reps].astype(BF16)
        mass = acc_ref[o, reps:]
        high = mass.astype(BF16).astype(F32)
        middle = (mass - high).astype(BF16).astype(F32)
        low = (mass - high) - middle
        flag = ob[0, o].astype(F32)
        tail = jnp.where(place == 0, high, jnp.where(place == 1, middle, jnp.where(place == 2, low, flag)))
        z_ref[o, reps:] = tail.astype(BF16)

    each_tile(acc_ref.shape[0], finish, 8)


def sweep_kernel(last, *refs):
    if last:
        tw, to, w_ref, turned_ref, f_ref, wo_ref, inv_ref, z_ref, out_hbm, accw_ref, x_ref, accz_ref, out_ref, sem = refs
    else:
        tw, to, w_ref, turned_ref, f_ref, wo_ref, inv_ref, z_ref, accw_ref, x_ref, accz_ref = refs
    tiles = w_ref.shape[0]
    accw_ref[...] = jnp.zeros_like(accw_ref)
    accz_ref[...] = jnp.zeros_like(accz_ref)
    add_tiles(0, tiles, to, tw, turned_ref, f_ref, accw_ref)
    for b in range(WORK_BLOCKS):
        worker = wo_ref[b] - accw_ref[b] * inv_ref[b, :1]
        if last:
            out_ref[:, b * CELLS : (b + 1) * CELLS] = worker
        x_ref[b] = worker.astype(BF16)
    if last:
        copy = pltpu.make_async_copy(out_ref, out_hbm, sem)
        copy.start()
    add_tiles(0, tiles, tw, to, w_ref, x_ref, accz_ref)
    z_ref[...] = accz_ref[...].astype(BF16)
    if last:
        copy.wait()


def gather_sums(z_ref, flags_ref, reps):
    zero = jnp.zeros((reps, CELLS), F32)

    def body(s, carry):
        first, second = carry
        part = z_ref[s, :reps].astype(F32)
        upper = jnp.broadcast_to(flags_ref[s, :1], part.shape) > 0.5
        return first + jnp.where(upper, 0.0, part), second + jnp.where(upper, part, 0.0)

    return lax.fori_loop(0, z_ref.shape[0], body, (zero, zero), unroll=4)


def scatter_firms(firms, flags_ref, send_ref):
    first, second = firms

    def step(s):
        upper = jnp.broadcast_to(flags_ref[s, :1], first.shape) > 0.5
        send_ref[s] = jnp.where(upper, second, first).astype(BF16)

    each_tile(send_ref.shape[0], step, 8)


def open_firm_kernel(z_ref, signs_ref, base_ref, noise_ref, cluster_ref, send_ref, fo_ref, inv_ref, flags_ref, now_ref):
    reps = signs_ref.shape[0]
    owners = z_ref.shape[0]
    mass = [jnp.zeros((1, CELLS), F32), jnp.zeros((1, CELLS), F32)]
    for s in range(owners):
        tail = z_ref[s, reps:].astype(F32)
        flags_ref[s] = jnp.broadcast_to(tail[3:4], (8, CELLS))
        part = tail[0:1] + tail[1:2] + tail[2:3]
        upper = tail[3:4] > 0.5
        mass = [mass[0] + jnp.where(upper, 0.0, part), mass[1] + jnp.where(upper, part, 0.0)]
    sums = gather_sums(z_ref, flags_ref, reps)
    flips = flip_table(signs_ref)
    firms = []
    for j in range(FIRM_BLOCKS):
        row = slice(j, j + 1)
        inverse = 1.0 / (1.0 + mass[j])
        value = outcome(flips, base_ref[row], noise_ref[row], cluster_ref[row])
        fo_ref[j] = value
        inv_ref[j] = jnp.broadcast_to(inverse, (8, CELLS))
        firm = value - sums[j] * inverse
        now_ref[j] = firm
        firms.append(firm)
    scatter_firms(firms, flags_ref, send_ref)


def next_firms(omega, z_ref, fo_ref, inv_ref, flags_ref, older_ref):
    sums = gather_sums(z_ref, flags_ref, z_ref.shape[1])
    firms = []
    for j in range(FIRM_BLOCKS):
        target = fo_ref[j] - sums[j] * inv_ref[j, :1]
        if older_ref is None:
            firms.append(omega * target)
        else:
            firms.append(older_ref[j] + omega * (target - older_ref[j]))
    return firms


def firm_kernel(omega, has_older, *refs):
    if has_older:
        z_ref, fo_ref, inv_ref, flags_ref, older_ref, send_ref, now_ref = refs
    else:
        (z_ref, fo_ref, inv_ref, flags_ref, send_ref, now_ref), older_ref = refs, None
    firms = next_firms(omega, z_ref, fo_ref, inv_ref, flags_ref, older_ref)
    for j in range(FIRM_BLOCKS):
        now_ref[j] = firms[j]
    scatter_firms(firms, flags_ref, send_ref)


def close_firm_kernel(omega, z_ref, fo_ref, inv_ref, flags_ref, older_ref, cov_ref, white_ref, firm_ref, part_ref):
    firms = next_firms(omega, z_ref, fo_ref, inv_ref, flags_ref, older_ref)
    for j in range(FIRM_BLOCKS):
        firm_ref[:, j * CELLS : (j + 1) * CELLS] = firms[j]
    projected = jnp.dot(firm_ref[...], cov_ref[...], precision=HIGHEST, preferred_element_type=F32)
    whitened = lax.dot_general(
        projected, white_ref[...], (((1,), (1,)), ((), ())), precision=HIGHEST, preferred_element_type=F32
    )
    reps = whitened.shape[0]
    columns = whitened.shape[1] // CELLS
    for c in range(columns):
        part_ref[pl.ds(c, reps, stride=columns)] = whitened[:, c * CELLS : (c + 1) * CELLS]


def total_kernel(part_ref, out_ref):
    total = jnp.sum(part_ref[...], axis=0)
    for s in range(out_ref.shape[0]):
        out_ref[s] = total


def moment_kernel(share, all_ref, coef_ref, moment_ref, rows_ref):
    reps, covars = coef_ref.shape
    columns = covars // CELLS
    share_rows = moment_ref.shape[0]
    in_block = CELLS // share_rows
    own = all_ref[pl.ds(share[0] // in_block, reps, stride=columns)]
    for c in range(columns):
        other = all_ref[pl.ds(c, reps, stride=columns)]
        coef_ref[:, c * CELLS : (c + 1) * CELLS] = other
        rows_ref[:, c * CELLS : (c + 1) * CELLS] = lax.dot_general(
            own, other, (((0,), (0,)), ((), ())), precision=HIGHEST, preferred_element_type=F32
        )
    start = pl.multiple_of((share[0] % in_block) * share_rows, share_rows)
    moment_ref[...] = rows_ref[pl.ds(start, share_rows)]


def keep(value):
    return pltpu.with_memory_space_constraint(value, pltpu.VMEM)


def call(kernel, inputs, outputs, scratch=(), scalars=0, name=None, specs=None, out_specs=None):
    return pl.pallas_call(
        kernel,
        in_specs=specs or [SMEM] * scalars + [VMEM] * (len(inputs) - scalars),
        out_specs=out_specs or [VMEM] * len(outputs),
        out_shape=[pltpu.VMEM(*item[:2]) if len(item) > 2 else jax.ShapeDtypeStruct(*item) for item in outputs],
        scratch_shapes=[item if not isinstance(item, tuple) else pltpu.VMEM(*item) for item in scratch],
        compiler_params=PARAMS,
        name=name,
    )(*inputs)


def body(
    tiles_w,
    tile_worker,
    tile_owner,
    owner_block,
    worker_base,
    worker_noise,
    worker_cluster,
    firm_base,
    firm_noise,
    firm_cluster,
    signs,
    covariates,
    whitening,
):
    owners = lax.axis_size("tiles")
    groups = lax.axis_size("reps")
    reps = signs.shape[0]
    covars = whitening.shape[0]
    omegas = chebyshev_weights(SWEEPS)

    def exchange(values, axes="tiles"):
        return lax.all_to_all(values, axes, 0, 0, tiled=True)

    def rows(values):
        return values.reshape(-1, CELLS)

    push_shape = ((owners, reps, CELLS), BF16)
    work_shape = ((WORK_BLOCKS, reps, CELLS), F32)
    firm_shape = ((FIRM_BLOCKS, reps, CELLS), F32)
    tiles = tiles_w.shape[0]
    inverse_shape = ((WORK_BLOCKS, 8, CELLS), F32)
    inputs = (tile_worker, tile_owner, owner_block, tiles_w, signs)
    inputs += (rows(worker_base), rows(worker_noise), rows(worker_cluster))
    z, worker_outcome, turned, worker_inverse = call(
        first_kernel,
        tuple(pltpu.with_memory_space_constraint(x, pltpu.HBM) for x in inputs),
        (((owners, reps + EXTRA, CELLS), BF16), work_shape, (tiles_w.shape, BF16, "keep"), inverse_shape),
        (
            pltpu.SMEM((tiles,), jnp.int32),
            pltpu.SMEM((tiles,), jnp.int32),
            pltpu.SMEM(owner_block.shape, jnp.int32),
            (signs.shape, jnp.int32),
            ((WORK_BLOCKS, CELLS), F32),
            ((WORK_BLOCKS, CELLS), F32),
            ((WORK_BLOCKS, CELLS), jnp.int32),
            (tiles_w.shape, BF16),
            ((WORK_BLOCKS, reps + EXTRA, CELLS), BF16),
            ((owners, reps + EXTRA, CELLS), F32),
            inverse_shape,
            pltpu.SemaphoreType.DMA((7 + CHUNKS,)),
        ),
        specs=[HBM] * 8,
        name="first_push",
    )
    share = lax.axis_index("tiles").astype(jnp.int32).reshape(1)
    share, z = lax.optimization_barrier((share, z))
    z = exchange(z)
    send, firm_outcome, firm_inverse, flags, newer = call(
        open_firm_kernel,
        (z, signs, rows(firm_base), rows(firm_noise), rows(firm_cluster)),
        (push_shape, firm_shape, ((FIRM_BLOCKS, 8, CELLS), F32), ((owners, 8, CELLS), F32), firm_shape),
        name="first_firm",
    )
    older = None
    scratch = (work_shape, ((WORK_BLOCKS, reps, CELLS), BF16), ((owners, reps, CELLS), F32))
    for k in range(1, SWEEPS):
        last = k == SWEEPS - 1
        f = exchange(send)
        outputs, more, out_specs = (push_shape,), (), [VMEM]
        if last:
            whole = ((reps, WORK_BLOCKS * CELLS), F32)
            outputs += (whole,)
            more = (whole, pltpu.SemaphoreType.DMA)
            out_specs.append(HBM)
        z, *rest = call(
            lambda *refs, e=last: sweep_kernel(e, *refs),
            (tile_worker, tile_owner, tiles_w, keep(turned), f, worker_outcome, worker_inverse),
            outputs,
            scratch + more,
            scalars=2,
            out_specs=out_specs,
            name="sweep_close" if last else "sweep",
        )
        z = exchange(z)
        inputs = (z, firm_outcome, firm_inverse, flags) + (() if older is None else (older,))
        if not last:
            send, now = call(
                lambda *refs, w=omegas[k], h=older is not None: firm_kernel(w, h, *refs),
                inputs,
                (push_shape, firm_shape),
                name="firm",
            )
            older, newer = newer, now
        else:
            firm_effect, part = call(
                lambda *refs, w=omegas[k]: close_firm_kernel(w, *refs),
                inputs + (covariates, whitening),
                (((reps, FIRM_BLOCKS * CELLS), F32), ((reps * covars // CELLS, CELLS), F32)),
                name="close_firm",
            )
    part = exchange(part.reshape(owners, -1, CELLS))
    (spread,) = call(total_kernel, (part,), ((part.shape, F32),), name="total")
    everything = exchange(spread)
    coefficients, moment = call(
        moment_kernel,
        (share, everything.reshape(-1, CELLS)),
        (((reps, covars), F32), ((covars // owners, covars), F32)),
        (((CELLS, covars), F32),),
        scalars=1,
        name="moment",
    )
    step = 1
    while step < groups:
        flip = step if step == 1 else 2 * step - 1
        moment = moment + lax.ppermute(moment, "reps", [(g, g ^ flip) for g in range(groups)])
        step *= 2
    covariance = moment / (reps * groups)
    return (rest[0], firm_effect, coefficients, covariance)


def solution(mesh):
    placed = (
        P("tiles", None, None),
        P("tiles"),
        P("tiles"),
        P("tiles", None),
        P("tiles"),
        P("tiles"),
        P("tiles"),
        P("tiles"),
        P("tiles"),
        P("tiles"),
        P("reps", None),
        P("tiles", None),
        P(),
    )
    return jax.shard_map(
        body,
        mesh=mesh,
        in_specs=placed,
        out_specs=(P("reps", "tiles"), P("reps", "tiles"), P("reps", None), P("tiles", None)),
        check_vma=False,
    )
```

```python
import jax
import jax.numpy as jnp
from jax import lax
from jax.experimental import pallas as pl
from jax.experimental.pallas import tpu as pltpu
from jax.sharding import PartitionSpec as P

WORK_BLOCKS = 16
FIRM_BLOCKS = 2
SWEEPS = 6
CELLS = 128
EXTRA = 8
SPECTRAL = 0.8
UNROLL = 64
CHUNKS = 4

F32 = jnp.float32
BF16 = jnp.bfloat16
HIGHEST = lax.Precision.HIGHEST

VMEM = pl.BlockSpec(memory_space=pltpu.VMEM)
SMEM = pl.BlockSpec(memory_space=pltpu.SMEM)
HBM = pl.BlockSpec(memory_space=pltpu.HBM)
PARAMS = pltpu.CompilerParams(vmem_limit_bytes=20 << 20)


def chebyshev_weights(count):
    weights = [1.0, 1.0 / (1.0 - 0.5 * SPECTRAL * SPECTRAL)]
    while len(weights) < count:
        weights.append(1.0 / (1.0 - 0.25 * SPECTRAL * SPECTRAL * weights[-1]))
    return weights


def flip_table(signs_ref):
    return (2 * signs_ref[...] - 1).astype(F32).astype(BF16)


def outcome(flips, base, noise, cluster):
    hot = lax.broadcasted_iota(jnp.int32, (flips.shape[1], CELLS), 0) == cluster
    values = jnp.dot(flips, jnp.where(hot, 1.0, 0.0).astype(BF16), preferred_element_type=F32)
    return base + noise * values


def each_tile(count, step, unroll=UNROLL):
    def body(index, carry):
        step(index)
        return carry

    lax.fori_loop(0, count, body, 0, unroll=min(unroll, count))


def add_tiles(first, count, source, target, w_ref, x_ref, acc_ref):
    def step(i):
        t = first + i
        acc_ref[target[t]] += jnp.dot(x_ref[source[t]], w_ref[t], preferred_element_type=F32)

    each_tile(count, step)


def first_kernel(
    tw_hbm, to_hbm, ob_hbm, w_hbm, signs_hbm, base_hbm, noise_hbm, cluster_hbm,
    z_ref, wo_ref, turned_ref, inv_ref,
    tw, to, ob, signs_ref, base_ref, noise_ref, cluster_ref, w_ref, x_ref, acc_ref, mass_ref, sems,
):
    small = [
        (signs_hbm, signs_ref),
        (cluster_hbm, cluster_ref),
        (base_hbm, base_ref),
        (noise_hbm, noise_ref),
        (tw_hbm, tw),
        (to_hbm, to),
        (ob_hbm, ob),
    ]
    copies = [pltpu.make_async_copy(source, target, sems.at[i]) for i, (source, target) in enumerate(small)]
    chunk = w_ref.shape[0] // CHUNKS
    loads = []
    for c in range(CHUNKS):
        part = pl.ds(c * chunk, chunk)
        loads.append(pltpu.make_async_copy(w_hbm.at[part], w_ref.at[part], sems.at[len(small) + c]))
    for copy in copies + loads:
        copy.start()
    acc_ref[...] = jnp.zeros_like(acc_ref)
    mass_ref[...] = jnp.zeros_like(mass_ref)
    for copy in copies:
        copy.wait()
    reps = signs_ref.shape[0]
    flips = flip_table(signs_ref)
    for b in range(WORK_BLOCKS):
        row = slice(b, b + 1)
        value = outcome(flips, base_ref[row], noise_ref[row], cluster_ref[row])
        wo_ref[b] = value
        x_ref[b, :reps] = value.astype(BF16)
        x_ref[b, reps:] = jnp.ones((EXTRA, CELLS), BF16)

    def step(t):
        tile = w_ref[t]
        acc_ref[to[t]] += jnp.dot(x_ref[tw[t]], tile, preferred_element_type=F32)
        turned = tile.T
        turned_ref[t] = turned
        mass_ref[tw[t]] += jnp.sum(turned.astype(F32).reshape(CELLS // 8, 8, CELLS), axis=0)

    for c in range(CHUNKS):
        loads[c].wait()
        each_tile(chunk, lambda i, c=c: step(c * chunk + i))
    for b in range(WORK_BLOCKS):
        inverse = 1.0 / (1.0 + jnp.sum(mass_ref[b], axis=0, keepdims=True))
        inv_ref[b] = jnp.broadcast_to(inverse, (8, CELLS))
    place = lax.broadcasted_iota(jnp.int32, (EXTRA, CELLS), 0)

    def finish(o):
        z_ref[o, :reps] = acc_ref[o, :reps].astype(BF16)
        mass = acc_ref[o, reps:]
        high = mass.astype(BF16).astype(F32)
        middle = (mass - high).astype(BF16).astype(F32)
        low = (mass - high) - middle
        flag = ob[0, o].astype(F32)
        tail = jnp.where(place == 0, high, jnp.where(place == 1, middle, jnp.where(place == 2, low, flag)))
        z_ref[o, reps:] = tail.astype(BF16)

    each_tile(acc_ref.shape[0], finish, 8)


def sweep_kernel(last, *refs):
    if last:
        tw, to, w_ref, turned_ref, f_ref, wo_ref, inv_ref, z_ref, out_hbm, accw_ref, x_ref, accz_ref, out_ref, sem = refs
    else:
        tw, to, w_ref, turned_ref, f_ref, wo_ref, inv_ref, z_ref, accw_ref, x_ref, accz_ref = refs
    tiles = w_ref.shape[0]
    accw_ref[...] = jnp.zeros_like(accw_ref)
    accz_ref[...] = jnp.zeros_like(accz_ref)
    add_tiles(0, tiles, to, tw, turned_ref, f_ref, accw_ref)
    for b in range(WORK_BLOCKS):
        worker = wo_ref[b] - accw_ref[b] * inv_ref[b, :1]
        if last:
            out_ref[:, b * CELLS : (b + 1) * CELLS] = worker
        x_ref[b] = worker.astype(BF16)
    if last:
        copy = pltpu.make_async_copy(out_ref, out_hbm, sem)
        copy.start()
    add_tiles(0, tiles, tw, to, w_ref, x_ref, accz_ref)
    z_ref[...] = accz_ref[...].astype(BF16)
    if last:
        copy.wait()


def gather_sums(z_ref, flags_ref, reps):
    zero = jnp.zeros((reps, CELLS), F32)

    def body(s, carry):
        first, second = carry
        part = z_ref[s, :reps].astype(F32)
        upper = jnp.broadcast_to(flags_ref[s, :1], part.shape) > 0.5
        return first + jnp.where(upper, 0.0, part), second + jnp.where(upper, part, 0.0)

    return lax.fori_loop(0, z_ref.shape[0], body, (zero, zero), unroll=4)


def scatter_firms(firms, flags_ref, send_ref):
    first, second = firms

    def step(s):
        upper = jnp.broadcast_to(flags_ref[s, :1], first.shape) > 0.5
        send_ref[s] = jnp.where(upper, second, first).astype(BF16)

    each_tile(send_ref.shape[0], step, 8)


def open_firm_kernel(z_ref, signs_ref, base_ref, noise_ref, cluster_ref, send_ref, fo_ref, inv_ref, flags_ref, now_ref):
    reps = signs_ref.shape[0]
    owners = z_ref.shape[0]
    mass = [jnp.zeros((1, CELLS), F32), jnp.zeros((1, CELLS), F32)]
    for s in range(owners):
        tail = z_ref[s, reps:].astype(F32)
        flags_ref[s] = jnp.broadcast_to(tail[3:4], (8, CELLS))
        part = tail[0:1] + tail[1:2] + tail[2:3]
        upper = tail[3:4] > 0.5
        mass = [mass[0] + jnp.where(upper, 0.0, part), mass[1] + jnp.where(upper, part, 0.0)]
    sums = gather_sums(z_ref, flags_ref, reps)
    flips = flip_table(signs_ref)
    firms = []
    for j in range(FIRM_BLOCKS):
        row = slice(j, j + 1)
        inverse = 1.0 / (1.0 + mass[j])
        value = outcome(flips, base_ref[row], noise_ref[row], cluster_ref[row])
        fo_ref[j] = value
        inv_ref[j] = jnp.broadcast_to(inverse, (8, CELLS))
        firm = value - sums[j] * inverse
        now_ref[j] = firm
        firms.append(firm)
    scatter_firms(firms, flags_ref, send_ref)


def next_firms(omega, z_ref, fo_ref, inv_ref, flags_ref, older_ref):
    sums = gather_sums(z_ref, flags_ref, z_ref.shape[1])
    firms = []
    for j in range(FIRM_BLOCKS):
        target = fo_ref[j] - sums[j] * inv_ref[j, :1]
        if older_ref is None:
            firms.append(omega * target)
        else:
            firms.append(older_ref[j] + omega * (target - older_ref[j]))
    return firms


def firm_kernel(omega, has_older, *refs):
    (z_ref, fo_ref, inv_ref, flags_ref), refs = refs[:4], refs[4:]
    older_ref = refs[0] if has_older else None
    send_ref, *now_ref = refs[1:] if has_older else refs
    firms = next_firms(omega, z_ref, fo_ref, inv_ref, flags_ref, older_ref)
    if now_ref:
        for j in range(FIRM_BLOCKS):
            now_ref[0][j] = firms[j]
    scatter_firms(firms, flags_ref, send_ref)


def close_firm_kernel(omega, z_ref, fo_ref, inv_ref, flags_ref, older_ref, cov_ref, white_ref, firm_ref, part_ref):
    firms = next_firms(omega, z_ref, fo_ref, inv_ref, flags_ref, older_ref)
    for j in range(FIRM_BLOCKS):
        firm_ref[:, j * CELLS : (j + 1) * CELLS] = firms[j]
    projected = jnp.dot(firm_ref[...], cov_ref[...], precision=HIGHEST, preferred_element_type=F32)
    whitened = lax.dot_general(
        projected, white_ref[...], (((1,), (1,)), ((), ())), precision=HIGHEST, preferred_element_type=F32
    )
    reps = whitened.shape[0]
    columns = whitened.shape[1] // CELLS
    for c in range(columns):
        part_ref[pl.ds(c, reps, stride=columns)] = whitened[:, c * CELLS : (c + 1) * CELLS]


def total_kernel(part_ref, out_ref):
    total = jnp.sum(part_ref[...], axis=0)
    for s in range(out_ref.shape[0]):
        out_ref[s] = total


def moment_kernel(share, all_ref, coef_ref, moment_ref, rows_ref):
    reps, covars = coef_ref.shape
    columns = covars // CELLS
    share_rows = moment_ref.shape[0]
    in_block = CELLS // share_rows
    own = all_ref[pl.ds(share[0] // in_block, reps, stride=columns)]
    for c in range(columns):
        other = all_ref[pl.ds(c, reps, stride=columns)]
        coef_ref[:, c * CELLS : (c + 1) * CELLS] = other
        rows_ref[:, c * CELLS : (c + 1) * CELLS] = lax.dot_general(
            own, other, (((0,), (0,)), ((), ())), precision=HIGHEST, preferred_element_type=F32
        )
    start = pl.multiple_of((share[0] % in_block) * share_rows, share_rows)
    moment_ref[...] = rows_ref[pl.ds(start, share_rows)]


def keep(value):
    return pltpu.with_memory_space_constraint(value, pltpu.VMEM)


def call(kernel, inputs, outputs, scratch=(), scalars=0, name=None, specs=None, out_specs=None):
    return pl.pallas_call(
        kernel,
        in_specs=specs or [SMEM] * scalars + [VMEM] * (len(inputs) - scalars),
        out_specs=out_specs or [VMEM] * len(outputs),
        out_shape=[pltpu.VMEM(*item[:2]) if len(item) > 2 else jax.ShapeDtypeStruct(*item) for item in outputs],
        scratch_shapes=[item if not isinstance(item, tuple) else pltpu.VMEM(*item) for item in scratch],
        compiler_params=PARAMS,
        name=name,
    )(*inputs)


def body(
    tiles_w,
    tile_worker,
    tile_owner,
    owner_block,
    worker_base,
    worker_noise,
    worker_cluster,
    firm_base,
    firm_noise,
    firm_cluster,
    signs,
    covariates,
    whitening,
):
    owners = lax.axis_size("tiles")
    groups = lax.axis_size("reps")
    reps = signs.shape[0]
    covars = whitening.shape[0]
    omegas = chebyshev_weights(SWEEPS)

    def exchange(values, axes="tiles"):
        return lax.all_to_all(values, axes, 0, 0, tiled=True)

    def rows(values):
        return values.reshape(-1, CELLS)

    push_shape = ((owners, reps, CELLS), BF16)
    work_shape = ((WORK_BLOCKS, reps, CELLS), F32)
    firm_shape = ((FIRM_BLOCKS, reps, CELLS), F32)
    tiles = tiles_w.shape[0]
    inverse_shape = ((WORK_BLOCKS, 8, CELLS), F32)
    inputs = (tile_worker, tile_owner, owner_block, tiles_w, signs)
    inputs += (rows(worker_base), rows(worker_noise), rows(worker_cluster))
    z, worker_outcome, turned, worker_inverse = call(
        first_kernel,
        tuple(pltpu.with_memory_space_constraint(x, pltpu.HBM) for x in inputs),
        (((owners, reps + EXTRA, CELLS), BF16), work_shape, (tiles_w.shape, BF16, "keep"), inverse_shape),
        (
            pltpu.SMEM((tiles,), jnp.int32),
            pltpu.SMEM((tiles,), jnp.int32),
            pltpu.SMEM(owner_block.shape, jnp.int32),
            (signs.shape, jnp.int32),
            ((WORK_BLOCKS, CELLS), F32),
            ((WORK_BLOCKS, CELLS), F32),
            ((WORK_BLOCKS, CELLS), jnp.int32),
            (tiles_w.shape, BF16),
            ((WORK_BLOCKS, reps + EXTRA, CELLS), BF16),
            ((owners, reps + EXTRA, CELLS), F32),
            inverse_shape,
            pltpu.SemaphoreType.DMA((7 + CHUNKS,)),
        ),
        specs=[HBM] * 8,
        name="first_push",
    )
    share = lax.axis_index("tiles").astype(jnp.int32).reshape(1)
    share, z = lax.optimization_barrier((share, z))
    z = exchange(z)
    send, firm_outcome, firm_inverse, flags, newer = call(
        open_firm_kernel,
        (z, signs, rows(firm_base), rows(firm_noise), rows(firm_cluster)),
        (push_shape, firm_shape, ((FIRM_BLOCKS, 8, CELLS), F32), ((owners, 8, CELLS), F32), firm_shape),
        name="first_firm",
    )
    older = None
    scratch = (work_shape, ((WORK_BLOCKS, reps, CELLS), BF16), ((owners, reps, CELLS), F32))
    for k in range(1, SWEEPS):
        last = k == SWEEPS - 1
        f = exchange(send)
        outputs, more, out_specs = (push_shape,), (), [VMEM]
        if last:
            whole = ((reps, WORK_BLOCKS * CELLS), F32)
            outputs += (whole,)
            more = (whole, pltpu.SemaphoreType.DMA)
            out_specs.append(HBM)
        z, *rest = call(
            lambda *refs, e=last: sweep_kernel(e, *refs),
            (tile_worker, tile_owner, tiles_w, keep(turned), f, worker_outcome, worker_inverse),
            outputs,
            scratch + more,
            scalars=2,
            out_specs=out_specs,
            name="sweep_close" if last else "sweep",
        )
        z = exchange(z)
        inputs = (z, firm_outcome, firm_inverse, flags) + (() if older is None else (older,))
        if not last:
            send, *now = call(
                lambda *refs, w=omegas[k], h=older is not None: firm_kernel(w, h, *refs),
                inputs,
                (push_shape, firm_shape) if k < SWEEPS - 2 else (push_shape,),
                name="firm",
            )
            older, newer = newer, now[0] if now else None
        else:
            firm_effect, part = call(
                lambda *refs, w=omegas[k]: close_firm_kernel(w, *refs),
                inputs + (covariates, whitening),
                (((reps, FIRM_BLOCKS * CELLS), F32), ((reps * covars // CELLS, CELLS), F32)),
                name="close_firm",
            )
    part = exchange(part.reshape(owners, -1, CELLS))
    (spread,) = call(total_kernel, (part,), ((part.shape, F32),), name="total")
    everything = exchange(spread)
    coefficients, moment = call(
        moment_kernel,
        (share, everything.reshape(-1, CELLS)),
        (((reps, covars), F32), ((covars // owners, covars), F32)),
        (((CELLS, covars), F32),),
        scalars=1,
        name="moment",
    )
    shifted = [lax.ppermute(moment, "reps", [(g, (g + d) % groups) for g in range(groups)]) for d in range(1, groups)]
    covariance = ((moment + shifted[1]) + (shifted[0] + shifted[2])) / (reps * groups)
    return (rest[0], firm_effect, coefficients, covariance)


def solution(mesh):
    placed = (
        P("tiles", None, None),
        P("tiles"),
        P("tiles"),
        P("tiles", None),
        P("tiles"),
        P("tiles"),
        P("tiles"),
        P("tiles"),
        P("tiles"),
        P("tiles"),
        P("reps", None),
        P("tiles", None),
        P(),
    )
    return jax.shard_map(
        body,
        mesh=mesh,
        in_specs=placed,
        out_specs=(P("reps", "tiles"), P("reps", "tiles"), P("reps", None), P("tiles", None)),
        check_vma=False,
    )
```

```python
import jax
import jax.numpy as jnp
from jax import lax
from jax.experimental import pallas as pl
from jax.experimental.pallas import tpu as pltpu
from jax.sharding import PartitionSpec as P

WORK_BLOCKS = 16
FIRM_BLOCKS = 2
SWEEPS = 6
CELLS = 128
EXTRA = 8
SPECTRAL = 0.8
UNROLL = 64
CHUNKS = 4

F32 = jnp.float32
BF16 = jnp.bfloat16
HIGHEST = lax.Precision.HIGHEST

VMEM = pl.BlockSpec(memory_space=pltpu.VMEM)
SMEM = pl.BlockSpec(memory_space=pltpu.SMEM)
HBM = pl.BlockSpec(memory_space=pltpu.HBM)
PARAMS = pltpu.CompilerParams(vmem_limit_bytes=20 << 20)


def chebyshev_weights(count):
    weights = [1.0, 1.0 / (1.0 - 0.5 * SPECTRAL * SPECTRAL)]
    while len(weights) < count:
        weights.append(1.0 / (1.0 - 0.25 * SPECTRAL * SPECTRAL * weights[-1]))
    return weights


def flip_table(signs_ref):
    return (2 * signs_ref[...] - 1).astype(F32).astype(BF16)


def outcome(flips, base, noise, cluster):
    hot = lax.broadcasted_iota(jnp.int32, (flips.shape[1], CELLS), 0) == cluster
    values = jnp.dot(flips, jnp.where(hot, 1.0, 0.0).astype(BF16), preferred_element_type=F32)
    return base + noise * values


def each_tile(count, step, unroll=UNROLL):
    def body(index, carry):
        step(index)
        return carry

    lax.fori_loop(0, count, body, 0, unroll=min(unroll, count))


def add_tiles(first, count, source, target, w_ref, x_ref, acc_ref):
    def step(i):
        t = first + i
        acc_ref[target[t]] += jnp.dot(x_ref[source[t]], w_ref[t], preferred_element_type=F32)

    each_tile(count, step)


def first_kernel(
    tw_hbm, to_hbm, ob_hbm, w_hbm, signs_hbm, base_hbm, noise_hbm, cluster_hbm,
    z_ref, wo_ref, w_ref, turned_ref, inv_ref,
    tw, to, ob, signs_ref, base_ref, noise_ref, cluster_ref, x_ref, acc_ref, mass_ref, sems,
):
    small = [
        (signs_hbm, signs_ref),
        (cluster_hbm, cluster_ref),
        (base_hbm, base_ref),
        (noise_hbm, noise_ref),
        (tw_hbm, tw),
        (to_hbm, to),
        (ob_hbm, ob),
    ]
    copies = [pltpu.make_async_copy(source, target, sems.at[i]) for i, (source, target) in enumerate(small)]
    chunk = w_ref.shape[0] // CHUNKS
    loads = []
    for c in range(CHUNKS):
        part = pl.ds(c * chunk, chunk)
        loads.append(pltpu.make_async_copy(w_hbm.at[part], w_ref.at[part], sems.at[len(small) + c]))
    for copy in copies + loads:
        copy.start()
    acc_ref[...] = jnp.zeros_like(acc_ref)
    mass_ref[...] = jnp.zeros_like(mass_ref)
    for copy in copies:
        copy.wait()
    reps = signs_ref.shape[0]
    flips = flip_table(signs_ref)
    for b in range(WORK_BLOCKS):
        row = slice(b, b + 1)
        value = outcome(flips, base_ref[row], noise_ref[row], cluster_ref[row])
        wo_ref[b] = value
        x_ref[b, :reps] = value.astype(BF16)
        x_ref[b, reps:] = jnp.ones((EXTRA, CELLS), BF16)

    def step(t):
        tile = w_ref[t]
        acc_ref[to[t]] += jnp.dot(x_ref[tw[t]], tile, preferred_element_type=F32)
        turned = tile.T
        turned_ref[t] = turned
        mass_ref[tw[t]] += jnp.sum(turned.astype(F32).reshape(CELLS // 8, 8, CELLS), axis=0)

    for c in range(CHUNKS):
        loads[c].wait()
        each_tile(chunk, lambda i, c=c: step(c * chunk + i))
    for b in range(WORK_BLOCKS):
        inverse = 1.0 / (1.0 + jnp.sum(mass_ref[b], axis=0, keepdims=True))
        inv_ref[b] = jnp.broadcast_to(inverse, (8, CELLS))
    place = lax.broadcasted_iota(jnp.int32, (EXTRA, CELLS), 0)

    def finish(o):
        z_ref[o, :reps] = acc_ref[o, :reps].astype(BF16)
        mass = acc_ref[o, reps:]
        high = mass.astype(BF16).astype(F32)
        middle = (mass - high).astype(BF16).astype(F32)
        low = (mass - high) - middle
        flag = ob[0, o].astype(F32)
        tail = jnp.where(place == 0, high, jnp.where(place == 1, middle, jnp.where(place == 2, low, flag)))
        z_ref[o, reps:] = tail.astype(BF16)

    each_tile(acc_ref.shape[0], finish, 8)


def sweep_kernel(last, *refs):
    if last:
        tw, to, w_ref, turned_ref, f_ref, wo_ref, inv_ref, z_ref, out_hbm, accw_ref, x_ref, accz_ref, out_ref, sem = refs
    else:
        tw, to, w_ref, turned_ref, f_ref, wo_ref, inv_ref, z_ref, accw_ref, x_ref, accz_ref = refs
    tiles = w_ref.shape[0]
    accw_ref[...] = jnp.zeros_like(accw_ref)
    accz_ref[...] = jnp.zeros_like(accz_ref)
    add_tiles(0, tiles, to, tw, turned_ref, f_ref, accw_ref)
    for b in range(WORK_BLOCKS):
        worker = wo_ref[b] - accw_ref[b] * inv_ref[b, :1]
        if last:
            out_ref[:, b * CELLS : (b + 1) * CELLS] = worker
        x_ref[b] = worker.astype(BF16)
    if last:
        copy = pltpu.make_async_copy(out_ref, out_hbm, sem)
        copy.start()
    add_tiles(0, tiles, tw, to, w_ref, x_ref, accz_ref)
    z_ref[...] = accz_ref[...].astype(BF16)
    if last:
        copy.wait()


def halves(value):
    high = value.astype(BF16)
    return high, (value - high.astype(F32)).astype(BF16)


def product(left, right, dims):
    (a, b), (c, d) = halves(left), halves(right)

    def dot(p, q):
        return lax.dot_general(p, q, (dims, ((), ())), preferred_element_type=F32)

    return (dot(a, d) + dot(b, c)) + dot(a, c)


def gather_sums(z_ref, flags_ref, reps):
    zero = jnp.zeros((reps, CELLS), F32)

    def body(s, carry):
        first, second = carry
        part = z_ref[s, :reps].astype(F32)
        upper = jnp.broadcast_to(flags_ref[s, :1], part.shape) > 0.5
        return first + jnp.where(upper, 0.0, part), second + jnp.where(upper, part, 0.0)

    return lax.fori_loop(0, z_ref.shape[0], body, (zero, zero), unroll=4)


def scatter_firms(firms, flags_ref, send_ref):
    first, second = firms

    def step(s):
        upper = jnp.broadcast_to(flags_ref[s, :1], first.shape) > 0.5
        send_ref[s] = jnp.where(upper, second, first).astype(BF16)

    each_tile(send_ref.shape[0], step, 8)


def open_firm_kernel(z_ref, signs_ref, base_ref, noise_ref, cluster_ref, send_ref, fo_ref, inv_ref, flags_ref, now_ref):
    reps = signs_ref.shape[0]
    owners = z_ref.shape[0]
    mass = [jnp.zeros((1, CELLS), F32), jnp.zeros((1, CELLS), F32)]
    for s in range(owners):
        tail = z_ref[s, reps:].astype(F32)
        flags_ref[s] = jnp.broadcast_to(tail[3:4], (8, CELLS))
        part = tail[0:1] + tail[1:2] + tail[2:3]
        upper = tail[3:4] > 0.5
        mass = [mass[0] + jnp.where(upper, 0.0, part), mass[1] + jnp.where(upper, part, 0.0)]
    sums = gather_sums(z_ref, flags_ref, reps)
    flips = flip_table(signs_ref)
    firms = []
    for j in range(FIRM_BLOCKS):
        row = slice(j, j + 1)
        inverse = 1.0 / (1.0 + mass[j])
        value = outcome(flips, base_ref[row], noise_ref[row], cluster_ref[row])
        fo_ref[j] = value
        inv_ref[j] = jnp.broadcast_to(inverse, (8, CELLS))
        firm = value - sums[j] * inverse
        now_ref[j] = firm
        firms.append(firm)
    scatter_firms(firms, flags_ref, send_ref)


def next_firms(omega, z_ref, fo_ref, inv_ref, flags_ref, older_ref):
    sums = gather_sums(z_ref, flags_ref, z_ref.shape[1])
    firms = []
    for j in range(FIRM_BLOCKS):
        target = fo_ref[j] - sums[j] * inv_ref[j, :1]
        if older_ref is None:
            firms.append(omega * target)
        else:
            firms.append(older_ref[j] + omega * (target - older_ref[j]))
    return firms


def firm_kernel(omega, has_older, *refs):
    (z_ref, fo_ref, inv_ref, flags_ref), refs = refs[:4], refs[4:]
    older_ref = refs[0] if has_older else None
    send_ref, *now_ref = refs[1:] if has_older else refs
    firms = next_firms(omega, z_ref, fo_ref, inv_ref, flags_ref, older_ref)
    if now_ref:
        for j in range(FIRM_BLOCKS):
            now_ref[0][j] = firms[j]
    scatter_firms(firms, flags_ref, send_ref)


def close_firm_kernel(omega, z_ref, fo_ref, inv_ref, flags_ref, older_ref, cov_ref, white_ref, firm_ref, part_ref):
    firms = next_firms(omega, z_ref, fo_ref, inv_ref, flags_ref, older_ref)
    for j in range(FIRM_BLOCKS):
        firm_ref[:, j * CELLS : (j + 1) * CELLS] = firms[j]
    projected = product(firm_ref[...], cov_ref[...], ((1,), (0,)))
    whitened = product(projected, white_ref[...], ((1,), (1,)))
    reps = whitened.shape[0]
    columns = whitened.shape[1] // CELLS
    for c in range(columns):
        part_ref[pl.ds(c, reps, stride=columns)] = whitened[:, c * CELLS : (c + 1) * CELLS]


def total_kernel(part_ref, out_ref):
    total = jnp.sum(part_ref[...], axis=0)
    for s in range(out_ref.shape[0]):
        out_ref[s] = total


def moment_kernel(share, all_ref, coef_ref, moment_ref, rows_ref):
    reps, covars = coef_ref.shape
    columns = covars // CELLS
    share_rows = moment_ref.shape[1]
    in_block = CELLS // share_rows
    own = all_ref[pl.ds(share[0] // in_block, reps, stride=columns)]
    for c in range(columns):
        other = all_ref[pl.ds(c, reps, stride=columns)]
        coef_ref[:, c * CELLS : (c + 1) * CELLS] = other
        rows_ref[:, c * CELLS : (c + 1) * CELLS] = lax.dot_general(
            own, other, (((0,), (0,)), ((), ())), precision=HIGHEST, preferred_element_type=F32
        )
    start = pl.multiple_of((share[0] % in_block) * share_rows, share_rows)
    for g in range(moment_ref.shape[0]):
        moment_ref[g] = rows_ref[pl.ds(start, share_rows)]


def keep(value):
    return pltpu.with_memory_space_constraint(value, pltpu.VMEM)


def call(kernel, inputs, outputs, scratch=(), scalars=0, name=None, specs=None, out_specs=None):
    return pl.pallas_call(
        kernel,
        in_specs=specs or [SMEM] * scalars + [VMEM] * (len(inputs) - scalars),
        out_specs=out_specs or [VMEM] * len(outputs),
        out_shape=[pltpu.VMEM(*item[:2]) if len(item) > 2 else jax.ShapeDtypeStruct(*item) for item in outputs],
        scratch_shapes=[item if not isinstance(item, tuple) else pltpu.VMEM(*item) for item in scratch],
        compiler_params=PARAMS,
        name=name,
    )(*inputs)


def body(
    tiles_w,
    tile_worker,
    tile_owner,
    owner_block,
    worker_base,
    worker_noise,
    worker_cluster,
    firm_base,
    firm_noise,
    firm_cluster,
    signs,
    covariates,
    whitening,
):
    owners = lax.axis_size("tiles")
    groups = lax.axis_size("reps")
    reps = signs.shape[0]
    covars = whitening.shape[0]
    omegas = chebyshev_weights(SWEEPS)

    def exchange(values, axes="tiles"):
        return lax.all_to_all(values, axes, 0, 0, tiled=True)

    def rows(values):
        return values.reshape(-1, CELLS)

    push_shape = ((owners, reps, CELLS), BF16)
    work_shape = ((WORK_BLOCKS, reps, CELLS), F32)
    firm_shape = ((FIRM_BLOCKS, reps, CELLS), F32)
    tiles = tiles_w.shape[0]
    held_shape = (tiles_w.shape, BF16, "keep")
    inverse_shape = ((WORK_BLOCKS, 8, CELLS), F32)
    inputs = (tile_worker, tile_owner, owner_block, tiles_w, signs)
    inputs += (rows(worker_base), rows(worker_noise), rows(worker_cluster))
    z, worker_outcome, held, turned, worker_inverse = call(
        first_kernel,
        tuple(pltpu.with_memory_space_constraint(x, pltpu.HBM) for x in inputs),
        (((owners, reps + EXTRA, CELLS), BF16), work_shape, held_shape, held_shape, inverse_shape),
        (
            pltpu.SMEM((tiles,), jnp.int32),
            pltpu.SMEM((tiles,), jnp.int32),
            pltpu.SMEM(owner_block.shape, jnp.int32),
            (signs.shape, jnp.int32),
            ((WORK_BLOCKS, CELLS), F32),
            ((WORK_BLOCKS, CELLS), F32),
            ((WORK_BLOCKS, CELLS), jnp.int32),
            ((WORK_BLOCKS, reps + EXTRA, CELLS), BF16),
            ((owners, reps + EXTRA, CELLS), F32),
            inverse_shape,
            pltpu.SemaphoreType.DMA((7 + CHUNKS,)),
        ),
        specs=[HBM] * 8,
        name="first_push",
    )
    share = lax.axis_index("tiles").astype(jnp.int32).reshape(1)
    share, z = lax.optimization_barrier((share, z))
    z = exchange(z)
    send, firm_outcome, firm_inverse, flags, newer = call(
        open_firm_kernel,
        (z, signs, rows(firm_base), rows(firm_noise), rows(firm_cluster)),
        (push_shape, firm_shape, ((FIRM_BLOCKS, 8, CELLS), F32), ((owners, 8, CELLS), F32), firm_shape),
        name="first_firm",
    )
    older = None
    scratch = (work_shape, ((WORK_BLOCKS, reps, CELLS), BF16), ((owners, reps, CELLS), F32))
    for k in range(1, SWEEPS):
        last = k == SWEEPS - 1
        f = exchange(send)
        outputs, more, out_specs = (push_shape,), (), [VMEM]
        if last:
            whole = ((reps, WORK_BLOCKS * CELLS), F32)
            outputs += (whole,)
            more = (whole, pltpu.SemaphoreType.DMA)
            out_specs.append(HBM)
        z, *rest = call(
            lambda *refs, e=last: sweep_kernel(e, *refs),
            (tile_worker, tile_owner, keep(held), keep(turned), f, worker_outcome, worker_inverse),
            outputs,
            scratch + more,
            scalars=2,
            out_specs=out_specs,
            name="sweep_close" if last else "sweep",
        )
        z = exchange(z)
        inputs = (z, firm_outcome, firm_inverse, flags) + (() if older is None else (older,))
        if not last:
            send, *now = call(
                lambda *refs, w=omegas[k], h=older is not None: firm_kernel(w, h, *refs),
                inputs,
                (push_shape, firm_shape) if k < SWEEPS - 2 else (push_shape,),
                name="firm",
            )
            older, newer = newer, now[0] if now else None
        else:
            firm_effect, part = call(
                lambda *refs, w=omegas[k]: close_firm_kernel(w, *refs),
                inputs + (covariates, whitening),
                (((reps, FIRM_BLOCKS * CELLS), F32), ((reps * covars // CELLS, CELLS), F32)),
                name="close_firm",
            )
    part = exchange(part.reshape(owners, -1, CELLS))
    (spread,) = call(total_kernel, (part,), ((part.shape, F32),), name="total")
    everything = exchange(spread)
    coefficients, moments = call(
        moment_kernel,
        (share, everything.reshape(-1, CELLS)),
        (((reps, covars), F32), ((groups, covars // owners, covars), F32)),
        (((CELLS, covars), F32),),
        scalars=1,
        name="moment",
    )
    moments = exchange(moments, "reps")
    covariance = jnp.sum(moments, axis=0) / (reps * groups)
    return (rest[0], firm_effect, coefficients, covariance)


def solution(mesh):
    placed = (
        P("tiles", None, None),
        P("tiles"),
        P("tiles"),
        P("tiles", None),
        P("tiles"),
        P("tiles"),
        P("tiles"),
        P("tiles"),
        P("tiles"),
        P("tiles"),
        P("reps", None),
        P("tiles", None),
        P(),
    )
    return jax.shard_map(
        body,
        mesh=mesh,
        in_specs=placed,
        out_specs=(P("reps", "tiles"), P("reps", "tiles"), P("reps", None), P("tiles", None)),
        check_vma=False,
    )
```

```python
import jax
import jax.numpy as jnp
from jax import lax
from jax.experimental import pallas as pl
from jax.experimental.pallas import tpu as pltpu
from jax.sharding import PartitionSpec as P

WORK_BLOCKS = 16
FIRM_BLOCKS = 2
SWEEPS = 6
CELLS = 128
EXTRA = 8
SPECTRAL = 0.8
UNROLL = 64
CHUNKS = 4

F32 = jnp.float32
BF16 = jnp.bfloat16
HIGHEST = lax.Precision.HIGHEST

VMEM = pl.BlockSpec(memory_space=pltpu.VMEM)
SMEM = pl.BlockSpec(memory_space=pltpu.SMEM)
HBM = pl.BlockSpec(memory_space=pltpu.HBM)
ANY = pl.BlockSpec(memory_space=pl.ANY)
PARAMS = pltpu.CompilerParams(vmem_limit_bytes=20 << 20)


def chebyshev_weights(count):
    weights = [1.0, 1.0 / (1.0 - 0.5 * SPECTRAL * SPECTRAL)]
    while len(weights) < count:
        weights.append(1.0 / (1.0 - 0.25 * SPECTRAL * SPECTRAL * weights[-1]))
    return weights


def flip_table(signs_ref):
    return (2 * signs_ref[...] - 1).astype(F32).astype(BF16)


def outcome(flips, base, noise, cluster):
    hot = lax.broadcasted_iota(jnp.int32, (flips.shape[1], CELLS), 0) == cluster
    values = jnp.dot(flips, jnp.where(hot, 1.0, 0.0).astype(BF16), preferred_element_type=F32)
    return base + noise * values


def each_tile(count, step, unroll=UNROLL):
    def body(index, carry):
        step(index)
        return carry

    lax.fori_loop(0, count, body, 0, unroll=min(unroll, count))


def add_tiles(first, count, source, target, w_ref, x_ref, acc_ref):
    def step(i):
        t = first + i
        acc_ref[target[t]] += jnp.dot(x_ref[source[t]], w_ref[t], preferred_element_type=F32)

    each_tile(count, step)


def first_kernel(
    tw_hbm, to_hbm, ob_hbm, w_hbm, signs_hbm, base_hbm, noise_hbm, cluster_hbm,
    z_ref, wo_ref, w_ref, turned_ref, inv_ref,
    tw, to, ob, signs_ref, base_ref, noise_ref, cluster_ref, x_ref, acc_ref, mass_ref, sems,
):
    small = [
        (signs_hbm, signs_ref),
        (cluster_hbm, cluster_ref),
        (base_hbm, base_ref),
        (noise_hbm, noise_ref),
        (tw_hbm, tw),
        (to_hbm, to),
        (ob_hbm, ob),
    ]
    copies = [pltpu.make_async_copy(source, target, sems.at[i]) for i, (source, target) in enumerate(small)]
    chunk = w_ref.shape[0] // CHUNKS
    loads = []
    for c in range(CHUNKS):
        part = pl.ds(c * chunk, chunk)
        loads.append(pltpu.make_async_copy(w_hbm.at[part], w_ref.at[part], sems.at[len(small) + c]))
    for copy in copies + loads:
        copy.start()
    acc_ref[...] = jnp.zeros_like(acc_ref)
    mass_ref[...] = jnp.zeros_like(mass_ref)
    for copy in copies:
        copy.wait()
    reps = signs_ref.shape[0]
    flips = flip_table(signs_ref)
    for b in range(WORK_BLOCKS):
        row = slice(b, b + 1)
        value = outcome(flips, base_ref[row], noise_ref[row], cluster_ref[row])
        wo_ref[b] = value
        x_ref[b, :reps] = value.astype(BF16)
        x_ref[b, reps:] = jnp.ones((EXTRA, CELLS), BF16)

    def step(t):
        tile = w_ref[t]
        acc_ref[to[t]] += jnp.dot(x_ref[tw[t]], tile, preferred_element_type=F32)
        turned = tile.T
        turned_ref[t] = turned
        mass_ref[tw[t]] += jnp.sum(turned.astype(F32).reshape(CELLS // 8, 8, CELLS), axis=0)

    for c in range(CHUNKS):
        loads[c].wait()
        each_tile(chunk, lambda i, c=c: step(c * chunk + i))
    for b in range(WORK_BLOCKS):
        inverse = 1.0 / (1.0 + jnp.sum(mass_ref[b], axis=0, keepdims=True))
        inv_ref[b] = jnp.broadcast_to(inverse, (8, CELLS))
    place = lax.broadcasted_iota(jnp.int32, (EXTRA, CELLS), 0)

    def finish(o):
        z_ref[o, :reps] = acc_ref[o, :reps].astype(BF16)
        mass = acc_ref[o, reps:]
        high = mass.astype(BF16).astype(F32)
        middle = (mass - high).astype(BF16).astype(F32)
        low = (mass - high) - middle
        flag = ob[0, o].astype(F32)
        tail = jnp.where(place == 0, high, jnp.where(place == 1, middle, jnp.where(place == 2, low, flag)))
        z_ref[o, reps:] = tail.astype(BF16)

    each_tile(acc_ref.shape[0], finish, 8)


def sweep_kernel(last, *refs):
    (tw_any, to_any, w_ref, turned_ref, f_ref, wo_ref, inv_ref), (z_ref, *refs) = refs[:7], refs[7:]
    if last:
        out_hbm, *refs = refs
    accw_ref, x_ref, accz_ref, tw, to, sems, *refs = refs
    tables = [pltpu.make_async_copy(tw_any, tw, sems.at[0]), pltpu.make_async_copy(to_any, to, sems.at[1])]
    for table in tables:
        table.start()
    tiles = w_ref.shape[0]
    accw_ref[...] = jnp.zeros_like(accw_ref)
    accz_ref[...] = jnp.zeros_like(accz_ref)
    for table in tables:
        table.wait()
    add_tiles(0, tiles, to, tw, turned_ref, f_ref, accw_ref)
    if last:
        (out_ref,) = refs
    for b in range(WORK_BLOCKS):
        worker = wo_ref[b] - accw_ref[b] * inv_ref[b, :1]
        if last:
            out_ref[:, b * CELLS : (b + 1) * CELLS] = worker
        x_ref[b] = worker.astype(BF16)
    if last:
        copy = pltpu.make_async_copy(out_ref, out_hbm, sems.at[2])
        copy.start()
    add_tiles(0, tiles, tw, to, w_ref, x_ref, accz_ref)
    z_ref[...] = accz_ref[...].astype(BF16)
    if last:
        copy.wait()


def halves(value):
    high = value.astype(BF16)
    return high, (value - high.astype(F32)).astype(BF16)


def product(left, right, dims):
    (a, b), (c, d) = halves(left), halves(right)

    def dot(p, q):
        return lax.dot_general(p, q, (dims, ((), ())), preferred_element_type=F32)

    return (dot(a, d) + dot(b, c)) + dot(a, c)


def gather_sums(z_ref, flags_ref, reps):
    zero = jnp.zeros((reps, CELLS), F32)

    def body(s, carry):
        first, second = carry
        part = z_ref[s, :reps].astype(F32)
        upper = jnp.broadcast_to(flags_ref[s, :1], part.shape) > 0.5
        return first + jnp.where(upper, 0.0, part), second + jnp.where(upper, part, 0.0)

    return lax.fori_loop(0, z_ref.shape[0], body, (zero, zero), unroll=4)


def scatter_firms(firms, flags_ref, send_ref):
    first, second = firms

    def step(s):
        upper = jnp.broadcast_to(flags_ref[s, :1], first.shape) > 0.5
        send_ref[s] = jnp.where(upper, second, first).astype(BF16)

    each_tile(send_ref.shape[0], step, 8)


def open_firm_kernel(z_ref, signs_ref, base_ref, noise_ref, cluster_ref, send_ref, fo_ref, inv_ref, flags_ref, now_ref):
    reps = signs_ref.shape[0]
    owners = z_ref.shape[0]
    mass = [jnp.zeros((1, CELLS), F32), jnp.zeros((1, CELLS), F32)]
    for s in range(owners):
        tail = z_ref[s, reps:].astype(F32)
        flags_ref[s] = jnp.broadcast_to(tail[3:4], (8, CELLS))
        part = tail[0:1] + tail[1:2] + tail[2:3]
        upper = tail[3:4] > 0.5
        mass = [mass[0] + jnp.where(upper, 0.0, part), mass[1] + jnp.where(upper, part, 0.0)]
    sums = gather_sums(z_ref, flags_ref, reps)
    flips = flip_table(signs_ref)
    firms = []
    for j in range(FIRM_BLOCKS):
        row = slice(j, j + 1)
        inverse = 1.0 / (1.0 + mass[j])
        value = outcome(flips, base_ref[row], noise_ref[row], cluster_ref[row])
        fo_ref[j] = value
        inv_ref[j] = jnp.broadcast_to(inverse, (8, CELLS))
        firm = value - sums[j] * inverse
        now_ref[j] = firm
        firms.append(firm)
    scatter_firms(firms, flags_ref, send_ref)


def next_firms(omega, z_ref, fo_ref, inv_ref, flags_ref, older_ref):
    sums = gather_sums(z_ref, flags_ref, z_ref.shape[1])
    firms = []
    for j in range(FIRM_BLOCKS):
        target = fo_ref[j] - sums[j] * inv_ref[j, :1]
        if older_ref is None:
            firms.append(omega * target)
        else:
            firms.append(older_ref[j] + omega * (target - older_ref[j]))
    return firms


def firm_kernel(omega, has_older, *refs):
    (z_ref, fo_ref, inv_ref, flags_ref), refs = refs[:4], refs[4:]
    older_ref = refs[0] if has_older else None
    send_ref, *now_ref = refs[1:] if has_older else refs
    firms = next_firms(omega, z_ref, fo_ref, inv_ref, flags_ref, older_ref)
    if now_ref:
        for j in range(FIRM_BLOCKS):
            now_ref[0][j] = firms[j]
    scatter_firms(firms, flags_ref, send_ref)


def close_firm_kernel(omega, z_ref, fo_ref, inv_ref, flags_ref, older_ref, cov_ref, white_ref, now_ref, part_ref):
    firms = next_firms(omega, z_ref, fo_ref, inv_ref, flags_ref, older_ref)
    for j in range(FIRM_BLOCKS):
        now_ref[j] = firms[j]
    projected = product(jnp.concatenate(firms, axis=1), cov_ref[...], ((1,), (0,)))
    whitened = product(projected, white_ref[...], ((1,), (1,)))
    reps = whitened.shape[0]
    columns = whitened.shape[1] // CELLS
    for c in range(columns):
        part_ref[pl.ds(c, reps, stride=columns)] = whitened[:, c * CELLS : (c + 1) * CELLS]


def total_kernel(part_ref, out_ref):
    total = jnp.sum(part_ref[...], axis=0)
    for s in range(out_ref.shape[0]):
        out_ref[s] = total


def moment_kernel(share, all_ref, moment_ref, rows_ref):
    share_rows, covars = moment_ref.shape
    columns = covars // CELLS
    reps = all_ref.shape[0] // columns
    in_block = CELLS // share_rows
    own = all_ref[pl.ds(share[0] // in_block, reps, stride=columns)]
    for c in range(columns):
        other = all_ref[pl.ds(c, reps, stride=columns)]
        rows_ref[:, c * CELLS : (c + 1) * CELLS] = product(own, other, ((0,), (0,)))
    start = pl.multiple_of((share[0] % in_block) * share_rows, share_rows)
    moment_ref[...] = rows_ref[pl.ds(start, share_rows)]


def emit_kernel(all_ref, now_ref, coef_ref, firm_ref):
    reps, covars = coef_ref.shape
    columns = covars // CELLS
    for c in range(columns):
        coef_ref[:, c * CELLS : (c + 1) * CELLS] = all_ref[pl.ds(c, reps, stride=columns)]
    for j in range(FIRM_BLOCKS):
        firm_ref[:, j * CELLS : (j + 1) * CELLS] = now_ref[j]


def keep(value):
    return pltpu.with_memory_space_constraint(value, pltpu.VMEM)


def call(kernel, inputs, outputs, scratch=(), scalars=0, name=None, specs=None, out_specs=None):
    return pl.pallas_call(
        kernel,
        in_specs=specs or [SMEM] * scalars + [VMEM] * (len(inputs) - scalars),
        out_specs=out_specs or [VMEM] * len(outputs),
        out_shape=[pltpu.VMEM(*item[:2]) if len(item) > 2 else jax.ShapeDtypeStruct(*item) for item in outputs],
        scratch_shapes=[item if not isinstance(item, tuple) else pltpu.VMEM(*item) for item in scratch],
        compiler_params=PARAMS,
        name=name,
    )(*inputs)


def body(
    tiles_w,
    tile_worker,
    tile_owner,
    owner_block,
    worker_base,
    worker_noise,
    worker_cluster,
    firm_base,
    firm_noise,
    firm_cluster,
    signs,
    covariates,
    whitening,
):
    owners = lax.axis_size("tiles")
    groups = lax.axis_size("reps")
    reps = signs.shape[0]
    covars = whitening.shape[0]
    omegas = chebyshev_weights(SWEEPS)

    def exchange(values, axes="tiles"):
        return lax.all_to_all(values, axes, 0, 0, tiled=True)

    def rows(values):
        return values.reshape(-1, CELLS)

    push_shape = ((owners, reps, CELLS), BF16)
    work_shape = ((WORK_BLOCKS, reps, CELLS), F32)
    firm_shape = ((FIRM_BLOCKS, reps, CELLS), F32)
    tiles = tiles_w.shape[0]
    held_shape = (tiles_w.shape, BF16, "keep")
    inverse_shape = ((WORK_BLOCKS, 8, CELLS), F32)
    inputs = (tile_worker, tile_owner, owner_block, tiles_w, signs)
    inputs += (rows(worker_base), rows(worker_noise), rows(worker_cluster))
    z, worker_outcome, held, turned, worker_inverse = call(
        first_kernel,
        tuple(pltpu.with_memory_space_constraint(x, pltpu.HBM) for x in inputs),
        (((owners, reps + EXTRA, CELLS), BF16), work_shape, held_shape, held_shape, inverse_shape),
        (
            pltpu.SMEM((tiles,), jnp.int32),
            pltpu.SMEM((tiles,), jnp.int32),
            pltpu.SMEM(owner_block.shape, jnp.int32),
            (signs.shape, jnp.int32),
            ((WORK_BLOCKS, CELLS), F32),
            ((WORK_BLOCKS, CELLS), F32),
            ((WORK_BLOCKS, CELLS), jnp.int32),
            ((WORK_BLOCKS, reps + EXTRA, CELLS), BF16),
            ((owners, reps + EXTRA, CELLS), F32),
            inverse_shape,
            pltpu.SemaphoreType.DMA((7 + CHUNKS,)),
        ),
        specs=[HBM] * 8,
        name="first_push",
    )
    share = lax.axis_index("tiles").astype(jnp.int32).reshape(1)
    share, z = lax.optimization_barrier((share, z))
    z = exchange(z)
    send, firm_outcome, firm_inverse, flags, newer = call(
        open_firm_kernel,
        (z, signs, rows(firm_base), rows(firm_noise), rows(firm_cluster)),
        (push_shape, firm_shape, ((FIRM_BLOCKS, 8, CELLS), F32), ((owners, 8, CELLS), F32), firm_shape),
        name="first_firm",
    )
    older = None
    scratch = (work_shape, ((WORK_BLOCKS, reps, CELLS), BF16), ((owners, reps, CELLS), F32))
    scratch += (pltpu.SMEM((tiles,), jnp.int32), pltpu.SMEM((tiles,), jnp.int32), pltpu.SemaphoreType.DMA((3,)))
    for k in range(1, SWEEPS):
        last = k == SWEEPS - 1
        f = exchange(send)
        outputs, more, out_specs = (push_shape,), (), [VMEM]
        if last:
            whole = ((reps, WORK_BLOCKS * CELLS), F32)
            outputs += (whole,)
            more = (whole,)
            out_specs.append(HBM)
        z, *rest = call(
            lambda *refs, e=last: sweep_kernel(e, *refs),
            (tile_worker, tile_owner, keep(held), keep(turned), f, worker_outcome, worker_inverse),
            outputs,
            scratch + more,
            specs=[ANY] * 2 + [VMEM] * 5,
            out_specs=out_specs,
            name="sweep_close" if last else "sweep",
        )
        z = exchange(z)
        inputs = (z, firm_outcome, firm_inverse, flags) + (() if older is None else (older,))
        if not last:
            send, *now = call(
                lambda *refs, w=omegas[k], h=older is not None: firm_kernel(w, h, *refs),
                inputs,
                (push_shape, firm_shape) if k < SWEEPS - 2 else (push_shape,),
                name="firm",
            )
            older, newer = newer, now[0] if now else None
        else:
            firms, part = call(
                lambda *refs, w=omegas[k]: close_firm_kernel(w, *refs),
                inputs + (covariates, whitening),
                (firm_shape, ((reps * covars // CELLS, CELLS), F32)),
                name="close_firm",
            )
    part = exchange(part.reshape(owners, -1, CELLS))
    (spread,) = call(total_kernel, (part,), ((part.shape, F32),), name="total")
    everything = exchange(spread).reshape(-1, CELLS)
    (moment,) = call(
        moment_kernel,
        (share, everything),
        (((covars // owners, covars), F32),),
        (((CELLS, covars), F32),),
        scalars=1,
        name="moment",
    )
    coefficients, firm_effect = call(
        emit_kernel,
        (everything, firms),
        (((reps, covars), F32), ((reps, FIRM_BLOCKS * CELLS), F32)),
        name="emit",
    )
    shifted = [lax.ppermute(moment, "reps", [(g, (g + d) % groups) for g in range(groups)]) for d in range(1, groups)]
    covariance = ((moment + shifted[1]) + (shifted[0] + shifted[2])) / (reps * groups)
    return (rest[0], firm_effect, coefficients, covariance)


def solution(mesh):
    placed = (
        P("tiles", None, None),
        P("tiles"),
        P("tiles"),
        P("tiles", None),
        P("tiles"),
        P("tiles"),
        P("tiles"),
        P("tiles"),
        P("tiles"),
        P("tiles"),
        P("reps", None),
        P("tiles", None),
        P(),
    )
    return jax.shard_map(
        body,
        mesh=mesh,
        in_specs=placed,
        out_specs=(P("reps", "tiles"), P("reps", "tiles"), P("reps", None), P("tiles", None)),
        check_vma=False,
    )
```

```python
import jax
import jax.numpy as jnp
from jax import lax
from jax.experimental import pallas as pl
from jax.experimental.pallas import tpu as pltpu
from jax.sharding import PartitionSpec as P

WORK_BLOCKS = 16
FIRM_BLOCKS = 2
SWEEPS = 6
CELLS = 128
EXTRA = 8
SPECTRAL = 0.8
UNROLL = 64
CHUNKS = 4

F32 = jnp.float32
BF16 = jnp.bfloat16
HIGHEST = lax.Precision.HIGHEST

VMEM = pl.BlockSpec(memory_space=pltpu.VMEM)
SMEM = pl.BlockSpec(memory_space=pltpu.SMEM)
HBM = pl.BlockSpec(memory_space=pltpu.HBM)
ANY = pl.BlockSpec(memory_space=pl.ANY)
PARAMS = pltpu.CompilerParams(vmem_limit_bytes=20 << 20)


def chebyshev_weights(count):
    weights = [1.0, 1.0 / (1.0 - 0.5 * SPECTRAL * SPECTRAL)]
    while len(weights) < count:
        weights.append(1.0 / (1.0 - 0.25 * SPECTRAL * SPECTRAL * weights[-1]))
    return weights


def flip_table(signs_ref):
    return (2 * signs_ref[...] - 1).astype(F32).astype(BF16)


def outcome(flips, base, noise, cluster):
    hot = lax.broadcasted_iota(jnp.int32, (flips.shape[1], CELLS), 0) == cluster
    values = jnp.dot(flips, jnp.where(hot, 1.0, 0.0).astype(BF16), preferred_element_type=F32)
    return base + noise * values


def each_tile(count, step, unroll=UNROLL):
    def body(index, carry):
        step(index)
        return carry

    lax.fori_loop(0, count, body, 0, unroll=min(unroll, count))


def add_pairs(count, row, plan, w_ref, x_ref, acc_ref):
    def step(p):
        i = 2 * p
        pair = jnp.concatenate([w_ref[plan[row, i]], w_ref[plan[row, i + 1]]], axis=1)
        both = jnp.dot(x_ref[plan[row + 2, i]], pair, preferred_element_type=F32)
        acc_ref[plan[row + 1, i]] += both[:, :CELLS]
        acc_ref[plan[row + 1, i + 1]] += both[:, CELLS:]

    each_tile(count, step, count)


def pair_plan(source, target, spare, slots):
    tiles = source.shape[1]
    along = jnp.broadcast_to(source, (tiles, tiles))
    down = along.T
    targets = jnp.broadcast_to(target, (tiles, tiles)).T
    row = lax.broadcasted_iota(jnp.int32, (tiles, tiles), 0)
    column = lax.broadcasted_iota(jnp.int32, (tiles, tiles), 1)
    same = along == down

    def count(mask, axis):
        return jnp.sum(jnp.where(mask, 1.0, 0.0), axis=axis, keepdims=True)

    size = count(same, 0)
    odd = size - 2.0 * jnp.floor(0.5 * size)
    width = 1.0 + jnp.where(count(same & (row < column), 0) == 0.0, odd, 0.0)
    place = jnp.sum(jnp.where(along < down, width, 0.0), axis=1, keepdims=True) + count(same & (column < row), 1)
    numbers = row.astype(F32)
    plans = ([], [], [])
    for base in range(0, slots, tiles):
        here = place == column.astype(F32) + base
        plans[0].append(jnp.sum(jnp.where(here, numbers, 0.0), axis=0, keepdims=True))
        plans[1].append(jnp.sum(jnp.where(here, targets - spare, 0.0), axis=0, keepdims=True) + spare)
        plans[2].append(jnp.sum(jnp.where(here, down, 0.0), axis=0, keepdims=True))
    return [jnp.concatenate(plan, axis=1).astype(jnp.int32) for plan in plans]


def first_kernel(
    tw_hbm, to_hbm, ob_hbm, w_hbm, signs_hbm, base_hbm, noise_hbm, cluster_hbm,
    z_ref, wo_ref, w_ref, turned_ref, inv_ref, plan_ref,
    tw, to, tw_row, to_row, ob, signs_ref, base_ref, noise_ref, cluster_ref, x_ref, acc_ref, mass_ref, sems,
):
    small = [
        (signs_hbm, signs_ref),
        (cluster_hbm, cluster_ref),
        (base_hbm, base_ref),
        (noise_hbm, noise_ref),
        (tw_hbm, tw),
        (to_hbm, to),
        (ob_hbm, ob),
        (tw_hbm, tw_row),
        (to_hbm, to_row),
    ]
    copies = [pltpu.make_async_copy(source, target, sems.at[i]) for i, (source, target) in enumerate(small)]
    chunk = w_ref.shape[0] // CHUNKS
    loads = []
    for c in range(CHUNKS):
        part = pl.ds(c * chunk, chunk)
        loads.append(pltpu.make_async_copy(w_hbm.at[part], w_ref.at[part], sems.at[len(small) + c]))
    for copy in copies + loads:
        copy.start()
    acc_ref[...] = jnp.zeros_like(acc_ref)
    mass_ref[...] = jnp.zeros_like(mass_ref)
    for copy in copies:
        copy.wait()
    reps = signs_ref.shape[0]
    flips = flip_table(signs_ref)
    for b in range(WORK_BLOCKS):
        row = slice(b, b + 1)
        value = outcome(flips, base_ref[row], noise_ref[row], cluster_ref[row])
        wo_ref[b] = value
        x_ref[b, :reps] = value.astype(BF16)
        x_ref[b, reps:] = jnp.ones((EXTRA, CELLS), BF16)

    def step(t):
        tile = w_ref[t]
        acc_ref[to[0, t]] += jnp.dot(x_ref[tw[0, t]], tile, preferred_element_type=F32)
        turned = tile.T
        turned_ref[t] = turned
        mass_ref[tw[0, t]] += jnp.sum(turned.astype(F32).reshape(CELLS // 8, 8, CELLS), axis=0)

    for c in range(CHUNKS):
        loads[c].wait()
        each_tile(chunk, lambda i, c=c: step(c * chunk + i))
        if c == 0:
            worker, owner = tw_row[...].astype(F32), to_row[...].astype(F32)
            pull = pair_plan(owner, worker, WORK_BLOCKS, plan_ref.shape[1])
            push = pair_plan(worker, owner, z_ref.shape[0], plan_ref.shape[1])
            for r, values in enumerate(pull + push):
                plan_ref[r : r + 1] = values
    for b in range(WORK_BLOCKS):
        inverse = 1.0 / (1.0 + jnp.sum(mass_ref[b], axis=0, keepdims=True))
        inv_ref[b] = jnp.broadcast_to(inverse, (8, CELLS))
    place = lax.broadcasted_iota(jnp.int32, (EXTRA, CELLS), 0)

    def finish(o):
        z_ref[o, :reps] = acc_ref[o, :reps].astype(BF16)
        mass = acc_ref[o, reps:]
        high = mass.astype(BF16).astype(F32)
        middle = (mass - high).astype(BF16).astype(F32)
        low = (mass - high) - middle
        flag = ob[0, o].astype(F32)
        tail = jnp.where(place == 0, high, jnp.where(place == 1, middle, jnp.where(place == 2, low, flag)))
        z_ref[o, reps:] = tail.astype(BF16)

    each_tile(acc_ref.shape[0], finish, 8)


def sweep_kernel(last, *refs):
    (plan_any, w_ref, turned_ref, f_ref, wo_ref, inv_ref), (z_ref, *refs) = refs[:6], refs[6:]
    if last:
        out_hbm, *refs = refs
    accw_ref, x_ref, accz_ref, plan, sems, *refs = refs
    tables = pltpu.make_async_copy(plan_any, plan, sems.at[0])
    tables.start()
    tiles, owners = w_ref.shape[0], z_ref.shape[0]
    accw_ref[...] = jnp.zeros_like(accw_ref)
    accz_ref[...] = jnp.zeros_like(accz_ref)
    tables.wait()
    add_pairs((tiles + owners) // 2, 0, plan, turned_ref, f_ref, accw_ref)
    if last:
        (out_ref,) = refs
    for b in range(WORK_BLOCKS):
        worker = wo_ref[b] - accw_ref[b] * inv_ref[b, :1]
        if last:
            out_ref[:, b * CELLS : (b + 1) * CELLS] = worker
        x_ref[b] = worker.astype(BF16)
    if last:
        copy = pltpu.make_async_copy(out_ref, out_hbm, sems.at[1])
        copy.start()
    add_pairs((tiles + WORK_BLOCKS) // 2, 3, plan, w_ref, x_ref, accz_ref)
    z_ref[...] = accz_ref[:owners].astype(BF16)
    if last:
        copy.wait()


def halves(value):
    high = value.astype(BF16)
    return high, (value - high.astype(F32)).astype(BF16)


def product(left, right, dims):
    (a, b), (c, d) = halves(left), halves(right)

    def dot(p, q):
        return lax.dot_general(p, q, (dims, ((), ())), preferred_element_type=F32)

    return (dot(a, d) + dot(b, c)) + dot(a, c)


def gather_sums(z_ref, flags_ref, reps):
    zero = jnp.zeros((reps, CELLS), F32)

    def body(s, carry):
        first, second = carry
        part = z_ref[s, :reps].astype(F32)
        upper = jnp.broadcast_to(flags_ref[s, :1], part.shape) > 0.5
        return first + jnp.where(upper, 0.0, part), second + jnp.where(upper, part, 0.0)

    return lax.fori_loop(0, z_ref.shape[0], body, (zero, zero), unroll=4)


def scatter_firms(firms, flags_ref, send_ref):
    first, second = firms

    def step(s):
        upper = jnp.broadcast_to(flags_ref[s, :1], first.shape) > 0.5
        send_ref[s] = jnp.where(upper, second, first).astype(BF16)

    each_tile(send_ref.shape[0], step, 8)


def open_firm_kernel(z_ref, signs_ref, base_ref, noise_ref, cluster_ref, send_ref, fo_ref, inv_ref, flags_ref, now_ref):
    reps = signs_ref.shape[0]
    owners = z_ref.shape[0]
    mass = [jnp.zeros((1, CELLS), F32), jnp.zeros((1, CELLS), F32)]
    for s in range(owners):
        tail = z_ref[s, reps:].astype(F32)
        flags_ref[s] = jnp.broadcast_to(tail[3:4], (8, CELLS))
        part = tail[0:1] + tail[1:2] + tail[2:3]
        upper = tail[3:4] > 0.5
        mass = [mass[0] + jnp.where(upper, 0.0, part), mass[1] + jnp.where(upper, part, 0.0)]
    sums = gather_sums(z_ref, flags_ref, reps)
    flips = flip_table(signs_ref)
    firms = []
    for j in range(FIRM_BLOCKS):
        row = slice(j, j + 1)
        inverse = 1.0 / (1.0 + mass[j])
        value = outcome(flips, base_ref[row], noise_ref[row], cluster_ref[row])
        fo_ref[j] = value
        inv_ref[j] = jnp.broadcast_to(inverse, (8, CELLS))
        firm = value - sums[j] * inverse
        now_ref[j] = firm
        firms.append(firm)
    scatter_firms(firms, flags_ref, send_ref)


def next_firms(omega, z_ref, fo_ref, inv_ref, flags_ref, older_ref):
    sums = gather_sums(z_ref, flags_ref, z_ref.shape[1])
    firms = []
    for j in range(FIRM_BLOCKS):
        target = fo_ref[j] - sums[j] * inv_ref[j, :1]
        if older_ref is None:
            firms.append(omega * target)
        else:
            firms.append(older_ref[j] + omega * (target - older_ref[j]))
    return firms


def firm_kernel(omega, has_older, *refs):
    (z_ref, fo_ref, inv_ref, flags_ref), refs = refs[:4], refs[4:]
    older_ref = refs[0] if has_older else None
    send_ref, *now_ref = refs[1:] if has_older else refs
    firms = next_firms(omega, z_ref, fo_ref, inv_ref, flags_ref, older_ref)
    if now_ref:
        for j in range(FIRM_BLOCKS):
            now_ref[0][j] = firms[j]
    scatter_firms(firms, flags_ref, send_ref)


def close_firm_kernel(omega, z_ref, fo_ref, inv_ref, flags_ref, older_ref, cov_ref, white_ref, now_ref, part_ref):
    firms = next_firms(omega, z_ref, fo_ref, inv_ref, flags_ref, older_ref)
    for j in range(FIRM_BLOCKS):
        now_ref[j] = firms[j]
    projected = product(jnp.concatenate(firms, axis=1), cov_ref[...], ((1,), (0,)))
    whitened = product(projected, white_ref[...], ((1,), (1,)))
    reps = whitened.shape[0]
    columns = whitened.shape[1] // CELLS
    for c in range(columns):
        part_ref[pl.ds(c, reps, stride=columns)] = whitened[:, c * CELLS : (c + 1) * CELLS]


def total_kernel(part_ref, out_ref):
    total = jnp.sum(part_ref[...], axis=0)
    for s in range(out_ref.shape[0]):
        out_ref[s] = total


def moment_kernel(share, all_ref, moment_ref, rows_ref):
    share_rows, covars = moment_ref.shape
    columns = covars // CELLS
    reps = all_ref.shape[0] // columns
    in_block = CELLS // share_rows
    own = all_ref[pl.ds(share[0] // in_block, reps, stride=columns)]
    for c in range(columns):
        other = all_ref[pl.ds(c, reps, stride=columns)]
        rows_ref[:, c * CELLS : (c + 1) * CELLS] = product(own, other, ((0,), (0,)))
    start = pl.multiple_of((share[0] % in_block) * share_rows, share_rows)
    moment_ref[...] = rows_ref[pl.ds(start, share_rows)]


def emit_kernel(all_ref, now_ref, coef_ref, firm_ref):
    reps, covars = coef_ref.shape
    columns = covars // CELLS
    for c in range(columns):
        coef_ref[:, c * CELLS : (c + 1) * CELLS] = all_ref[pl.ds(c, reps, stride=columns)]
    for j in range(FIRM_BLOCKS):
        firm_ref[:, j * CELLS : (j + 1) * CELLS] = now_ref[j]


def keep(value):
    return pltpu.with_memory_space_constraint(value, pltpu.VMEM)


def call(kernel, inputs, outputs, scratch=(), scalars=0, name=None, specs=None, out_specs=None):
    return pl.pallas_call(
        kernel,
        in_specs=specs or [SMEM] * scalars + [VMEM] * (len(inputs) - scalars),
        out_specs=out_specs or [VMEM] * len(outputs),
        out_shape=[pltpu.VMEM(*item[:2]) if len(item) > 2 else jax.ShapeDtypeStruct(*item) for item in outputs],
        scratch_shapes=[item if not isinstance(item, tuple) else pltpu.VMEM(*item) for item in scratch],
        compiler_params=PARAMS,
        name=name,
    )(*inputs)


def body(
    tiles_w,
    tile_worker,
    tile_owner,
    owner_block,
    worker_base,
    worker_noise,
    worker_cluster,
    firm_base,
    firm_noise,
    firm_cluster,
    signs,
    covariates,
    whitening,
):
    owners = lax.axis_size("tiles")
    groups = lax.axis_size("reps")
    reps = signs.shape[0]
    covars = whitening.shape[0]
    omegas = chebyshev_weights(SWEEPS)

    def exchange(values, axes="tiles"):
        return lax.all_to_all(values, axes, 0, 0, tiled=True)

    def rows(values):
        return values.reshape(-1, CELLS)

    push_shape = ((owners, reps, CELLS), BF16)
    work_shape = ((WORK_BLOCKS, reps, CELLS), F32)
    firm_shape = ((FIRM_BLOCKS, reps, CELLS), F32)
    tiles = tiles_w.shape[0]
    plan_shape = ((8, 2 * tiles), jnp.int32)
    held_shape = (tiles_w.shape, BF16, "keep")
    inverse_shape = ((WORK_BLOCKS, 8, CELLS), F32)
    inputs = (rows(tile_worker), rows(tile_owner), owner_block, tiles_w, signs)
    inputs += (rows(worker_base), rows(worker_noise), rows(worker_cluster))
    z, worker_outcome, held, turned, worker_inverse, plan = call(
        first_kernel,
        tuple(pltpu.with_memory_space_constraint(x, pltpu.HBM) for x in inputs),
        (((owners, reps + EXTRA, CELLS), BF16), work_shape, held_shape, held_shape, inverse_shape, plan_shape),
        (
            pltpu.SMEM((1, tiles), jnp.int32),
            pltpu.SMEM((1, tiles), jnp.int32),
            ((1, tiles), jnp.int32),
            ((1, tiles), jnp.int32),
            pltpu.SMEM(owner_block.shape, jnp.int32),
            (signs.shape, jnp.int32),
            ((WORK_BLOCKS, CELLS), F32),
            ((WORK_BLOCKS, CELLS), F32),
            ((WORK_BLOCKS, CELLS), jnp.int32),
            ((WORK_BLOCKS, reps + EXTRA, CELLS), BF16),
            ((owners, reps + EXTRA, CELLS), F32),
            inverse_shape,
            pltpu.SemaphoreType.DMA((9 + CHUNKS,)),
        ),
        specs=[HBM] * 8,
        name="first_push",
    )
    share = lax.axis_index("tiles").astype(jnp.int32).reshape(1)
    share, z = lax.optimization_barrier((share, z))
    z = exchange(z)
    send, firm_outcome, firm_inverse, flags, newer = call(
        open_firm_kernel,
        (z, signs, rows(firm_base), rows(firm_noise), rows(firm_cluster)),
        (push_shape, firm_shape, ((FIRM_BLOCKS, 8, CELLS), F32), ((owners, 8, CELLS), F32), firm_shape),
        name="first_firm",
    )
    older = None
    scratch = (((WORK_BLOCKS + 1, reps, CELLS), F32), ((WORK_BLOCKS, reps, CELLS), BF16))
    scratch += (((owners + 1, reps, CELLS), F32), pltpu.SMEM(*plan_shape), pltpu.SemaphoreType.DMA((2,)))
    for k in range(1, SWEEPS):
        last = k == SWEEPS - 1
        f = exchange(send)
        outputs, more, out_specs = (push_shape,), (), [VMEM]
        if last:
            whole = ((reps, WORK_BLOCKS * CELLS), F32)
            outputs += (whole,)
            more = (whole,)
            out_specs.append(HBM)
        z, *rest = call(
            lambda *refs, e=last: sweep_kernel(e, *refs),
            (plan, keep(held), keep(turned), f, worker_outcome, worker_inverse),
            outputs,
            scratch + more,
            specs=[ANY] + [VMEM] * 5,
            out_specs=out_specs,
            name="sweep_close" if last else "sweep",
        )
        z = exchange(z)
        inputs = (z, firm_outcome, firm_inverse, flags) + (() if older is None else (older,))
        if not last:
            send, *now = call(
                lambda *refs, w=omegas[k], h=older is not None: firm_kernel(w, h, *refs),
                inputs,
                (push_shape, firm_shape) if k < SWEEPS - 2 else (push_shape,),
                name="firm",
            )
            older, newer = newer, now[0] if now else None
        else:
            firms, part = call(
                lambda *refs, w=omegas[k]: close_firm_kernel(w, *refs),
                inputs + (covariates, whitening),
                (firm_shape, ((reps * covars // CELLS, CELLS), F32)),
                name="close_firm",
            )
    part = exchange(part.reshape(owners, -1, CELLS))
    (spread,) = call(total_kernel, (part,), ((part.shape, F32),), name="total")
    everything = exchange(spread).reshape(-1, CELLS)
    (moment,) = call(
        moment_kernel,
        (share, everything),
        (((covars // owners, covars), F32),),
        (((CELLS, covars), F32),),
        scalars=1,
        name="moment",
    )
    coefficients, firm_effect = call(
        emit_kernel,
        (everything, firms),
        (((reps, covars), F32), ((reps, FIRM_BLOCKS * CELLS), F32)),
        name="emit",
    )
    shifted = [lax.ppermute(moment, "reps", [(g, (g + d) % groups) for g in range(groups)]) for d in range(1, groups)]
    covariance = ((moment + shifted[1]) + (shifted[0] + shifted[2])) / (reps * groups)
    return (rest[0], firm_effect, coefficients, covariance)


def solution(mesh):
    placed = (
        P("tiles", None, None),
        P("tiles"),
        P("tiles"),
        P("tiles", None),
        P("tiles"),
        P("tiles"),
        P("tiles"),
        P("tiles"),
        P("tiles"),
        P("tiles"),
        P("reps", None),
        P("tiles", None),
        P(),
    )
    return jax.shard_map(
        body,
        mesh=mesh,
        in_specs=placed,
        out_specs=(P("reps", "tiles"), P("reps", "tiles"), P("reps", None), P("tiles", None)),
        check_vma=False,
    )
```

```python
import jax
import jax.numpy as jnp
from jax import lax
from jax.experimental import pallas as pl
from jax.experimental.pallas import tpu as pltpu
from jax.sharding import PartitionSpec as P

WORK_BLOCKS = 16
FIRM_BLOCKS = 2
CORES = 2
SWEEPS = 6
CELLS = 128
EXTRA = 8
SPECTRAL = 0.8
UNROLL = 64
CHUNKS = 4

F32 = jnp.float32
BF16 = jnp.bfloat16
HIGHEST = lax.Precision.HIGHEST

VMEM = pl.BlockSpec(memory_space=pltpu.VMEM)
SMEM = pl.BlockSpec(memory_space=pltpu.SMEM)
HBM = pl.BlockSpec(memory_space=pltpu.HBM)
ANY = pl.BlockSpec(memory_space=pl.ANY)
PARAMS = pltpu.CompilerParams(vmem_limit_bytes=20 << 20)


def chebyshev_weights(count):
    weights = [1.0, 1.0 / (1.0 - 0.5 * SPECTRAL * SPECTRAL)]
    while len(weights) < count:
        weights.append(1.0 / (1.0 - 0.25 * SPECTRAL * SPECTRAL * weights[-1]))
    return weights


def flip_table(signs_ref):
    return (2 * signs_ref[...] - 1).astype(F32).astype(BF16)


def outcome(flips, base, noise, cluster):
    hot = lax.broadcasted_iota(jnp.int32, (flips.shape[1], CELLS), 0) == cluster
    values = jnp.dot(flips, jnp.where(hot, 1.0, 0.0).astype(BF16), preferred_element_type=F32)
    return base + noise * values


def each_tile(count, step, unroll=UNROLL):
    def body(index, carry):
        step(index)
        return carry

    lax.fori_loop(0, count, body, 0, unroll=min(unroll, count))


def add_tiles(first, count, source, target, w_ref, x_ref, acc_ref):
    def step(i):
        t = first + i
        acc_ref[target[t]] += jnp.dot(x_ref[source[t]], w_ref[t], preferred_element_type=F32)

    each_tile(count, step)


def first_kernel(
    tw_hbm, to_hbm, ob_hbm, w_hbm, signs_hbm, base_hbm, noise_hbm, cluster_hbm,
    z_ref, wo_ref, w_ref, turned_ref, inv_ref,
    tw, to, ob, signs_ref, base_ref, noise_ref, cluster_ref, x_ref, acc_ref, mass_ref, sems,
):
    small = [
        (signs_hbm, signs_ref),
        (cluster_hbm, cluster_ref),
        (base_hbm, base_ref),
        (noise_hbm, noise_ref),
        (tw_hbm, tw),
        (to_hbm, to),
        (ob_hbm, ob),
    ]
    copies = [pltpu.make_async_copy(source, target, sems.at[i]) for i, (source, target) in enumerate(small)]
    chunk = w_ref.shape[0] // CHUNKS
    loads = []
    for c in range(CHUNKS):
        part = pl.ds(c * chunk, chunk)
        loads.append(pltpu.make_async_copy(w_hbm.at[part], w_ref.at[part], sems.at[len(small) + c]))
    for copy in copies + loads:
        copy.start()
    acc_ref[...] = jnp.zeros_like(acc_ref)
    mass_ref[...] = jnp.zeros_like(mass_ref)
    for copy in copies:
        copy.wait()
    reps = signs_ref.shape[0]
    flips = flip_table(signs_ref)
    for b in range(WORK_BLOCKS):
        row = slice(b, b + 1)
        value = outcome(flips, base_ref[row], noise_ref[row], cluster_ref[row])
        wo_ref[b] = value
        x_ref[b, :reps] = value.astype(BF16)
        x_ref[b, reps:] = jnp.ones((EXTRA, CELLS), BF16)

    def step(t):
        tile = w_ref[t]
        acc_ref[to[t]] += jnp.dot(x_ref[tw[t]], tile, preferred_element_type=F32)
        turned = tile.T
        turned_ref[t] = turned
        mass_ref[tw[t]] += jnp.sum(turned.astype(F32).reshape(CELLS // 8, 8, CELLS), axis=0)

    for c in range(CHUNKS):
        loads[c].wait()
        each_tile(chunk, lambda i, c=c: step(c * chunk + i))
    for b in range(WORK_BLOCKS):
        inverse = 1.0 / (1.0 + jnp.sum(mass_ref[b], axis=0, keepdims=True))
        inv_ref[b] = jnp.broadcast_to(inverse, (8, CELLS))
    place = lax.broadcasted_iota(jnp.int32, (EXTRA, CELLS), 0)

    def finish(o):
        z_ref[o, :reps] = acc_ref[o, :reps].astype(BF16)
        mass = acc_ref[o, reps:]
        high = mass.astype(BF16).astype(F32)
        middle = (mass - high).astype(BF16).astype(F32)
        low = (mass - high) - middle
        flag = ob[0, o].astype(F32)
        tail = jnp.where(place == 0, high, jnp.where(place == 1, middle, jnp.where(place == 2, low, flag)))
        z_ref[o, reps:] = tail.astype(BF16)

    each_tile(acc_ref.shape[0], finish, 8)


def sweep_kernel(last, *refs):
    (tw_any, to_any, w_ref, turned_ref, f_ref, wo_ref, inv_ref), (z_ref, *refs) = refs[:7], refs[7:]
    if last:
        out_hbm, *refs = refs
    accw_ref, x_ref, accz_ref, tw, to, sems, *refs = refs
    tables = [pltpu.make_async_copy(tw_any, tw, sems.at[0]), pltpu.make_async_copy(to_any, to, sems.at[1])]
    for table in tables:
        table.start()
    tiles = w_ref.shape[0]
    accw_ref[...] = jnp.zeros_like(accw_ref)
    accz_ref[...] = jnp.zeros_like(accz_ref)
    for table in tables:
        table.wait()
    add_tiles(0, tiles, to, tw, turned_ref, f_ref, accw_ref)
    if last:
        (out_ref,) = refs
    for b in range(WORK_BLOCKS):
        worker = wo_ref[b] - accw_ref[b] * inv_ref[b, :1]
        if last:
            out_ref[:, b * CELLS : (b + 1) * CELLS] = worker
        x_ref[b] = worker.astype(BF16)
    if last:
        copy = pltpu.make_async_copy(out_ref, out_hbm, sems.at[2])
        copy.start()
    add_tiles(0, tiles, tw, to, w_ref, x_ref, accz_ref)
    z_ref[...] = accz_ref[...].astype(BF16)
    if last:
        copy.wait()


def halves(value):
    high = value.astype(BF16)
    return high, (value - high.astype(F32)).astype(BF16)


def product(left, right, dims):
    (a, b), (c, d) = halves(left), halves(right)

    def dot(p, q):
        return lax.dot_general(p, q, (dims, ((), ())), preferred_element_type=F32)

    return (dot(a, d) + dot(b, c)) + dot(a, c)


def chip_sums(z_ref, flags_ref, reps, out_ref):
    zero = jnp.zeros((reps, CELLS), F32)
    for owner in range(CORES):

        def body(i, carry, owner=owner):
            first, second = carry
            part = z_ref[CORES * i + owner, :reps].astype(F32)
            upper = jnp.broadcast_to(flags_ref[CORES * i + owner, :1], part.shape) > 0.5
            return first + jnp.where(upper, 0.0, part), second + jnp.where(upper, part, 0.0)

        sums = lax.fori_loop(0, z_ref.shape[0] // CORES, body, (zero, zero), unroll=4)
        for j in range(FIRM_BLOCKS):
            out_ref[FIRM_BLOCKS * owner + j] = sums[j]


def scatter_firms(firms, flags_ref, send_ref):
    for owner in range(CORES):
        first, second = firms[FIRM_BLOCKS * owner : FIRM_BLOCKS * (owner + 1)]

        def step(i, owner=owner, first=first, second=second):
            upper = jnp.broadcast_to(flags_ref[CORES * i + owner, :1], first.shape) > 0.5
            send_ref[CORES * i + owner] = jnp.where(upper, second, first).astype(BF16)

        each_tile(send_ref.shape[0] // CORES, step, 8)


def open_sum_kernel(z_ref, signs_ref, base_ref, noise_ref, cluster_ref, pack_ref, flags_ref):
    reps = signs_ref.shape[0]
    blocks = CORES * FIRM_BLOCKS
    mass = [jnp.zeros((1, CELLS), F32)] * blocks
    for n in range(z_ref.shape[0]):
        tail = z_ref[n, reps:].astype(F32)
        flags_ref[n] = jnp.broadcast_to(tail[3:4], (8, CELLS))
        part = tail[0:1] + tail[1:2] + tail[2:3]
        upper = tail[3:4] > 0.5
        q = FIRM_BLOCKS * (n % CORES)
        mass[q] = mass[q] + jnp.where(upper, 0.0, part)
        mass[q + 1] = mass[q + 1] + jnp.where(upper, part, 0.0)
    chip_sums(z_ref, flags_ref, reps, pack_ref)
    flips = flip_table(signs_ref)
    for j in range(FIRM_BLOCKS):
        row = slice(j, j + 1)
        pack_ref[blocks + j] = outcome(flips, base_ref[row], noise_ref[row], cluster_ref[row])
    pack_ref[blocks + FIRM_BLOCKS] = jnp.zeros((reps, CELLS), F32)
    for q in range(blocks):
        pack_ref[blocks + FIRM_BLOCKS, q : q + 1] = mass[q]


def open_firm_kernel(share, mine_ref, theirs_ref, flags_ref, send_ref, fo_ref, inv_ref, now_ref):
    blocks = CORES * FIRM_BLOCKS
    core = share[0] % CORES
    last = blocks + FIRM_BLOCKS
    firms = []
    for q in range(blocks):
        own = q // FIRM_BLOCKS == core
        j = blocks + q % FIRM_BLOCKS
        value = jnp.where(own, mine_ref[j], theirs_ref[j])
        inverse = 1.0 / (1.0 + (mine_ref[last, q : q + 1] + theirs_ref[last, q : q + 1]))
        fo_ref[q] = value
        inv_ref[q] = jnp.broadcast_to(inverse, (8, CELLS))
        firm = value - (mine_ref[q] + theirs_ref[q]) * inverse
        now_ref[q] = firm
        firms.append(firm)
    scatter_firms(firms, flags_ref, send_ref)


def sum_kernel(z_ref, flags_ref, out_ref):
    chip_sums(z_ref, flags_ref, z_ref.shape[1], out_ref)


def next_firm(omega, q, mine_ref, theirs_ref, fo_ref, inv_ref, older_ref):
    target = fo_ref[q] - (mine_ref[q] + theirs_ref[q]) * inv_ref[q, :1]
    if older_ref is None:
        return omega * target
    return older_ref[q] + omega * (target - older_ref[q])


def firm_kernel(omega, has_older, *refs):
    (mine_ref, theirs_ref, fo_ref, inv_ref, flags_ref), refs = refs[:5], refs[5:]
    older_ref = refs[0] if has_older else None
    send_ref, *now_ref = refs[1:] if has_older else refs
    firms = []
    for q in range(CORES * FIRM_BLOCKS):
        firms.append(next_firm(omega, q, mine_ref, theirs_ref, fo_ref, inv_ref, older_ref))
        if now_ref:
            now_ref[0][q] = firms[q]
    scatter_firms(firms, flags_ref, send_ref)


def close_firm_kernel(
    omega, share, mine_ref, theirs_ref, fo_ref, inv_ref, older_ref, cov_ref, white_ref, now_ref, part_ref
):
    firms = []
    for j in range(FIRM_BLOCKS):
        q = FIRM_BLOCKS * (share[0] % CORES) + j
        firms.append(next_firm(omega, q, mine_ref, theirs_ref, fo_ref, inv_ref, older_ref))
        now_ref[j] = firms[j]
    projected = product(jnp.concatenate(firms, axis=1), cov_ref[...], ((1,), (0,)))
    whitened = product(projected, white_ref[...], ((1,), (1,)))
    reps = whitened.shape[0]
    columns = whitened.shape[1] // CELLS
    for c in range(columns):
        part_ref[pl.ds(c, reps, stride=columns)] = whitened[:, c * CELLS : (c + 1) * CELLS]


def total_kernel(part_ref, out_ref):
    total = jnp.sum(part_ref[...], axis=0)
    for s in range(out_ref.shape[0]):
        out_ref[s] = total


def moment_kernel(share, all_ref, moment_ref, rows_ref):
    share_rows, covars = moment_ref.shape
    columns = covars // CELLS
    reps = all_ref.shape[0] // columns
    in_block = CELLS // share_rows
    own = all_ref[pl.ds(share[0] // in_block, reps, stride=columns)]
    for c in range(columns):
        other = all_ref[pl.ds(c, reps, stride=columns)]
        rows_ref[:, c * CELLS : (c + 1) * CELLS] = product(own, other, ((0,), (0,)))
    start = pl.multiple_of((share[0] % in_block) * share_rows, share_rows)
    moment_ref[...] = rows_ref[pl.ds(start, share_rows)]


def emit_kernel(all_ref, now_ref, coef_ref, firm_ref):
    reps, covars = coef_ref.shape
    columns = covars // CELLS
    for c in range(columns):
        coef_ref[:, c * CELLS : (c + 1) * CELLS] = all_ref[pl.ds(c, reps, stride=columns)]
    for j in range(FIRM_BLOCKS):
        firm_ref[:, j * CELLS : (j + 1) * CELLS] = now_ref[j]


def keep(value):
    return pltpu.with_memory_space_constraint(value, pltpu.VMEM)


def call(kernel, inputs, outputs, scratch=(), scalars=0, name=None, specs=None, out_specs=None):
    return pl.pallas_call(
        kernel,
        in_specs=specs or [SMEM] * scalars + [VMEM] * (len(inputs) - scalars),
        out_specs=out_specs or [VMEM] * len(outputs),
        out_shape=[pltpu.VMEM(*item[:2]) if len(item) > 2 else jax.ShapeDtypeStruct(*item) for item in outputs],
        scratch_shapes=[item if not isinstance(item, tuple) else pltpu.VMEM(*item) for item in scratch],
        compiler_params=PARAMS,
        name=name,
    )(*inputs)


def body(
    tiles_w,
    tile_worker,
    tile_owner,
    owner_block,
    worker_base,
    worker_noise,
    worker_cluster,
    firm_base,
    firm_noise,
    firm_cluster,
    signs,
    covariates,
    whitening,
):
    owners = lax.axis_size("tiles")
    groups = lax.axis_size("reps")
    reps = signs.shape[0]
    covars = whitening.shape[0]
    omegas = chebyshev_weights(SWEEPS)

    def exchange(values, axes="tiles"):
        return lax.all_to_all(values, axes, 0, 0, tiled=True)

    def swap(values):
        return lax.ppermute(values, "tiles", [(t, t ^ 1) for t in range(owners)])

    def chips(values):
        groups_of = [list(range(c, owners, CORES)) for c in range(CORES)]
        joined = values.reshape(owners // CORES, -1, CELLS)
        moved = lax.all_to_all(joined, "tiles", 0, 0, tiled=True, axis_index_groups=groups_of)
        return moved.reshape(values.shape)

    def rows(values):
        return values.reshape(-1, CELLS)

    push_shape = ((owners, reps, CELLS), BF16)
    work_shape = ((WORK_BLOCKS, reps, CELLS), F32)
    firm_shape = ((FIRM_BLOCKS, reps, CELLS), F32)
    chip_shape = ((CORES * FIRM_BLOCKS, reps, CELLS), F32)
    flags_shape = ((owners, 8, CELLS), F32)
    tiles = tiles_w.shape[0]
    held_shape = (tiles_w.shape, BF16, "keep")
    inverse_shape = ((WORK_BLOCKS, 8, CELLS), F32)
    inputs = (tile_worker, tile_owner, owner_block, tiles_w, signs)
    inputs += (rows(worker_base), rows(worker_noise), rows(worker_cluster))
    z, worker_outcome, held, turned, worker_inverse = call(
        first_kernel,
        tuple(pltpu.with_memory_space_constraint(x, pltpu.HBM) for x in inputs),
        (((owners, reps + EXTRA, CELLS), BF16), work_shape, held_shape, held_shape, inverse_shape),
        (
            pltpu.SMEM((tiles,), jnp.int32),
            pltpu.SMEM((tiles,), jnp.int32),
            pltpu.SMEM(owner_block.shape, jnp.int32),
            (signs.shape, jnp.int32),
            ((WORK_BLOCKS, CELLS), F32),
            ((WORK_BLOCKS, CELLS), F32),
            ((WORK_BLOCKS, CELLS), jnp.int32),
            ((WORK_BLOCKS, reps + EXTRA, CELLS), BF16),
            ((owners, reps + EXTRA, CELLS), F32),
            inverse_shape,
            pltpu.SemaphoreType.DMA((7 + CHUNKS,)),
        ),
        specs=[HBM] * 8,
        name="first_push",
    )
    share = lax.axis_index("tiles").astype(jnp.int32).reshape(1)
    share, z = lax.optimization_barrier((share, z))
    z = chips(z)
    pack, flags = call(
        open_sum_kernel,
        (z, signs, rows(firm_base), rows(firm_noise), rows(firm_cluster)),
        (((CORES * FIRM_BLOCKS + FIRM_BLOCKS + 1, reps, CELLS), F32), flags_shape),
        name="first_sum",
    )
    send, firm_outcome, firm_inverse, newer = call(
        open_firm_kernel,
        (share, pack, swap(pack), flags),
        (push_shape, chip_shape, ((CORES * FIRM_BLOCKS, 8, CELLS), F32), chip_shape),
        scalars=1,
        name="first_firm",
    )
    older = None
    scratch = (work_shape, ((WORK_BLOCKS, reps, CELLS), BF16), ((owners, reps, CELLS), F32))
    scratch += (pltpu.SMEM((tiles,), jnp.int32), pltpu.SMEM((tiles,), jnp.int32), pltpu.SemaphoreType.DMA((3,)))
    for k in range(1, SWEEPS):
        last = k == SWEEPS - 1
        f = chips(send)
        outputs, more, out_specs = (push_shape,), (), [VMEM]
        if last:
            whole = ((reps, WORK_BLOCKS * CELLS), F32)
            outputs += (whole,)
            more = (whole,)
            out_specs.append(HBM)
        z, *rest = call(
            lambda *refs, e=last: sweep_kernel(e, *refs),
            (tile_worker, tile_owner, keep(held), keep(turned), f, worker_outcome, worker_inverse),
            outputs,
            scratch + more,
            specs=[ANY] * 2 + [VMEM] * 5,
            out_specs=out_specs,
            name="sweep_close" if last else "sweep",
        )
        z = chips(z)
        (sums,) = call(sum_kernel, (z, flags), (chip_shape,), name="sum")
        inputs = (sums, swap(sums), firm_outcome, firm_inverse)
        past = () if older is None else (older,)
        if not last:
            send, *now = call(
                lambda *refs, w=omegas[k], h=older is not None: firm_kernel(w, h, *refs),
                inputs + (flags,) + past,
                (push_shape, chip_shape) if k < SWEEPS - 2 else (push_shape,),
                name="firm",
            )
            older, newer = newer, now[0] if now else None
        else:
            firms, part = call(
                lambda *refs, w=omegas[k]: close_firm_kernel(w, *refs),
                (share,) + inputs + past + (covariates, whitening),
                (firm_shape, ((reps * covars // CELLS, CELLS), F32)),
                scalars=1,
                name="close_firm",
            )
    part = exchange(part.reshape(owners, -1, CELLS))
    (spread,) = call(total_kernel, (part,), ((part.shape, F32),), name="total")
    everything = exchange(spread).reshape(-1, CELLS)
    (moment,) = call(
        moment_kernel,
        (share, everything),
        (((covars // owners, covars), F32),),
        (((CELLS, covars), F32),),
        scalars=1,
        name="moment",
    )
    coefficients, firm_effect = call(
        emit_kernel,
        (everything, firms),
        (((reps, covars), F32), ((reps, FIRM_BLOCKS * CELLS), F32)),
        name="emit",
    )
    shifted = [lax.ppermute(moment, "reps", [(g, (g + d) % groups) for g in range(groups)]) for d in range(1, groups)]
    covariance = ((moment + shifted[1]) + (shifted[0] + shifted[2])) / (reps * groups)
    return (rest[0], firm_effect, coefficients, covariance)


def solution(mesh):
    placed = (
        P("tiles", None, None),
        P("tiles"),
        P("tiles"),
        P("tiles", None),
        P("tiles"),
        P("tiles"),
        P("tiles"),
        P("tiles"),
        P("tiles"),
        P("tiles"),
        P("reps", None),
        P("tiles", None),
        P(),
    )
    return jax.shard_map(
        body,
        mesh=mesh,
        in_specs=placed,
        out_specs=(P("reps", "tiles"), P("reps", "tiles"), P("reps", None), P("tiles", None)),
        check_vma=False,
    )
```

```python
import jax
import jax.numpy as jnp
from jax import lax
from jax.experimental import pallas as pl
from jax.experimental.pallas import tpu as pltpu
from jax.sharding import PartitionSpec as P

WORK_BLOCKS = 16
FIRM_BLOCKS = 2
SWEEPS = 6
CELLS = 128
EXTRA = 8
SPECTRAL = 0.8
UNROLL = 64
CHUNKS = 4

F32 = jnp.float32
BF16 = jnp.bfloat16
HIGHEST = lax.Precision.HIGHEST

VMEM = pl.BlockSpec(memory_space=pltpu.VMEM)
SMEM = pl.BlockSpec(memory_space=pltpu.SMEM)
HBM = pl.BlockSpec(memory_space=pltpu.HBM)
ANY = pl.BlockSpec(memory_space=pl.ANY)
PARAMS = pltpu.CompilerParams(vmem_limit_bytes=20 << 20)


def chebyshev_weights(count):
    weights = [1.0, 1.0 / (1.0 - 0.5 * SPECTRAL * SPECTRAL)]
    while len(weights) < count:
        weights.append(1.0 / (1.0 - 0.25 * SPECTRAL * SPECTRAL * weights[-1]))
    return weights


def flip_table(signs_ref):
    return (2 * signs_ref[...] - 1).astype(F32).astype(BF16)


def outcome(flips, base, noise, cluster):
    hot = lax.broadcasted_iota(jnp.int32, (flips.shape[1], CELLS), 0) == cluster
    values = jnp.dot(flips, jnp.where(hot, 1.0, 0.0).astype(BF16), preferred_element_type=F32)
    return base + noise * values


def each_tile(count, step, unroll=UNROLL):
    def body(index, carry):
        step(index)
        return carry

    lax.fori_loop(0, count, body, 0, unroll=min(unroll, count))


def add_pairs(count, row, plan, w_ref, x_ref, acc_ref):
    def step(p):
        i = 2 * p
        values = jnp.concatenate([x_ref[plan[row + 2, i]], x_ref[plan[row + 2, i + 1]]], axis=1)
        pair = jnp.concatenate([w_ref[plan[row, i]], w_ref[plan[row, i + 1]]], axis=0)
        acc_ref[plan[row + 1, i]] += jnp.dot(values, pair, preferred_element_type=F32)

    each_tile(count, step, count)


def pair_plan(target, source, slots):
    tiles = target.shape[1]
    along = jnp.broadcast_to(target, (tiles, tiles))
    down = along.T
    sources = jnp.broadcast_to(source, (tiles, tiles)).T
    row = lax.broadcasted_iota(jnp.int32, (tiles, tiles), 0)
    column = lax.broadcasted_iota(jnp.int32, (tiles, tiles), 1)
    same = along == down

    def count(mask, axis):
        return jnp.sum(jnp.where(mask, 1.0, 0.0), axis=axis, keepdims=True)

    size = count(same, 0)
    odd = size - 2.0 * jnp.floor(0.5 * size)
    width = 1.0 + jnp.where(count(same & (row < column), 0) == 0.0, odd, 0.0)
    place = jnp.sum(jnp.where(along < down, width, 0.0), axis=1, keepdims=True) + count(same & (column < row), 1)
    numbers = row.astype(F32) - tiles
    plans = ([], [], [])
    for base in range(0, slots, tiles):
        here = place == column.astype(F32) + base
        plans[0].append(jnp.sum(jnp.where(here, numbers, 0.0), axis=0, keepdims=True) + tiles)
        plans[1].append(jnp.sum(jnp.where(here, down, 0.0), axis=0, keepdims=True))
        plans[2].append(jnp.sum(jnp.where(here, sources, 0.0), axis=0, keepdims=True))
    return [jnp.concatenate(plan, axis=1).astype(jnp.int32) for plan in plans]


def first_kernel(
    tw_hbm, to_hbm, ob_hbm, w_hbm, signs_hbm, base_hbm, noise_hbm, cluster_hbm,
    z_ref, wo_ref, w_ref, turned_ref, inv_ref, plan_ref,
    tw, to, tw_row, to_row, ob, signs_ref, base_ref, noise_ref, cluster_ref, x_ref, acc_ref, mass_ref, sems,
):
    small = [
        (signs_hbm, signs_ref),
        (cluster_hbm, cluster_ref),
        (base_hbm, base_ref),
        (noise_hbm, noise_ref),
        (tw_hbm, tw),
        (to_hbm, to),
        (ob_hbm, ob),
        (tw_hbm, tw_row),
        (to_hbm, to_row),
    ]
    copies = [pltpu.make_async_copy(source, target, sems.at[i]) for i, (source, target) in enumerate(small)]
    tiles = w_hbm.shape[0]
    chunk = tiles // CHUNKS
    loads = []
    for c in range(CHUNKS):
        part = pl.ds(c * chunk, chunk)
        loads.append(pltpu.make_async_copy(w_hbm.at[part], w_ref.at[part], sems.at[len(small) + c]))
    for copy in copies + loads:
        copy.start()
    acc_ref[...] = jnp.zeros_like(acc_ref)
    mass_ref[...] = jnp.zeros_like(mass_ref)
    w_ref[tiles] = jnp.zeros((CELLS, CELLS), BF16)
    turned_ref[tiles] = jnp.zeros((CELLS, CELLS), BF16)
    for copy in copies:
        copy.wait()
    reps = signs_ref.shape[0]
    flips = flip_table(signs_ref)
    for b in range(WORK_BLOCKS):
        row = slice(b, b + 1)
        value = outcome(flips, base_ref[row], noise_ref[row], cluster_ref[row])
        wo_ref[b] = value
        x_ref[b, :reps] = value.astype(BF16)
        x_ref[b, reps:] = jnp.ones((EXTRA, CELLS), BF16)

    def step(t):
        tile = w_ref[t]
        acc_ref[to[0, t]] += jnp.dot(x_ref[tw[0, t]], tile, preferred_element_type=F32)
        turned = tile.T
        turned_ref[t] = turned
        mass_ref[tw[0, t]] += jnp.sum(turned.astype(F32).reshape(CELLS // 8, 8, CELLS), axis=0)

    for c in range(CHUNKS):
        loads[c].wait()
        each_tile(chunk, lambda i, c=c: step(c * chunk + i))
        if c == 0:
            worker, owner = tw_row[...].astype(F32), to_row[...].astype(F32)
            pull = pair_plan(worker, owner, plan_ref.shape[1])
            push = pair_plan(owner, worker, plan_ref.shape[1])
            for r, values in enumerate(pull + push):
                plan_ref[r : r + 1] = values
    for b in range(WORK_BLOCKS):
        inverse = 1.0 / (1.0 + jnp.sum(mass_ref[b], axis=0, keepdims=True))
        inv_ref[b] = jnp.broadcast_to(inverse, (8, CELLS))
    place = lax.broadcasted_iota(jnp.int32, (EXTRA, CELLS), 0)

    def finish(o):
        z_ref[o, :reps] = acc_ref[o, :reps].astype(BF16)
        mass = acc_ref[o, reps:]
        high = mass.astype(BF16).astype(F32)
        middle = (mass - high).astype(BF16).astype(F32)
        low = (mass - high) - middle
        flag = ob[0, o].astype(F32)
        tail = jnp.where(place == 0, high, jnp.where(place == 1, middle, jnp.where(place == 2, low, flag)))
        z_ref[o, reps:] = tail.astype(BF16)

    each_tile(acc_ref.shape[0], finish, 8)


def sweep_kernel(last, *refs):
    (plan_any, w_ref, turned_ref, f_ref, wo_ref, inv_ref), (z_ref, *refs) = refs[:6], refs[6:]
    if last:
        out_hbm, *refs = refs
    accw_ref, x_ref, accz_ref, plan, sems, *refs = refs
    tables = pltpu.make_async_copy(plan_any, plan, sems.at[0])
    tables.start()
    tiles, owners = w_ref.shape[0] - 1, z_ref.shape[0]
    accw_ref[...] = jnp.zeros_like(accw_ref)
    accz_ref[...] = jnp.zeros_like(accz_ref)
    tables.wait()
    add_pairs((tiles + WORK_BLOCKS) // 2, 0, plan, turned_ref, f_ref, accw_ref)
    if last:
        (out_ref,) = refs
    for b in range(WORK_BLOCKS):
        worker = wo_ref[b] - accw_ref[b] * inv_ref[b, :1]
        if last:
            out_ref[:, b * CELLS : (b + 1) * CELLS] = worker
        x_ref[b] = worker.astype(BF16)
    if last:
        copy = pltpu.make_async_copy(out_ref, out_hbm, sems.at[1])
        copy.start()
    add_pairs((tiles + owners) // 2, 3, plan, w_ref, x_ref, accz_ref)
    z_ref[...] = accz_ref[...].astype(BF16)
    if last:
        copy.wait()


def halves(value):
    high = value.astype(BF16)
    return high, (value - high.astype(F32)).astype(BF16)


def product(left, right, dims):
    (a, b), (c, d) = halves(left), halves(right)

    def dot(p, q):
        return lax.dot_general(p, q, (dims, ((), ())), preferred_element_type=F32)

    return (dot(a, d) + dot(b, c)) + dot(a, c)


def gather_sums(z_ref, flags_ref, reps):
    zero = jnp.zeros((reps, CELLS), F32)

    def body(s, carry):
        first, second = carry
        part = z_ref[s, :reps].astype(F32)
        upper = jnp.broadcast_to(flags_ref[s, :1], part.shape) > 0.5
        return first + jnp.where(upper, 0.0, part), second + jnp.where(upper, part, 0.0)

    return lax.fori_loop(0, z_ref.shape[0], body, (zero, zero), unroll=4)


def scatter_firms(firms, flags_ref, send_ref):
    first, second = firms

    def step(s):
        upper = jnp.broadcast_to(flags_ref[s, :1], first.shape) > 0.5
        send_ref[s] = jnp.where(upper, second, first).astype(BF16)

    each_tile(send_ref.shape[0], step, 8)


def open_firm_kernel(z_ref, signs_ref, base_ref, noise_ref, cluster_ref, send_ref, fo_ref, inv_ref, flags_ref, now_ref):
    reps = signs_ref.shape[0]
    owners = z_ref.shape[0]
    mass = [jnp.zeros((1, CELLS), F32), jnp.zeros((1, CELLS), F32)]
    for s in range(owners):
        tail = z_ref[s, reps:].astype(F32)
        flags_ref[s] = jnp.broadcast_to(tail[3:4], (8, CELLS))
        part = tail[0:1] + tail[1:2] + tail[2:3]
        upper = tail[3:4] > 0.5
        mass = [mass[0] + jnp.where(upper, 0.0, part), mass[1] + jnp.where(upper, part, 0.0)]
    sums = gather_sums(z_ref, flags_ref, reps)
    flips = flip_table(signs_ref)
    firms = []
    for j in range(FIRM_BLOCKS):
        row = slice(j, j + 1)
        inverse = 1.0 / (1.0 + mass[j])
        value = outcome(flips, base_ref[row], noise_ref[row], cluster_ref[row])
        fo_ref[j] = value
        inv_ref[j] = jnp.broadcast_to(inverse, (8, CELLS))
        firm = value - sums[j] * inverse
        now_ref[j] = firm
        firms.append(firm)
    scatter_firms(firms, flags_ref, send_ref)


def next_firms(omega, z_ref, fo_ref, inv_ref, flags_ref, older_ref):
    sums = gather_sums(z_ref, flags_ref, z_ref.shape[1])
    firms = []
    for j in range(FIRM_BLOCKS):
        target = fo_ref[j] - sums[j] * inv_ref[j, :1]
        if older_ref is None:
            firms.append(omega * target)
        else:
            firms.append(older_ref[j] + omega * (target - older_ref[j]))
    return firms


def firm_kernel(omega, has_older, *refs):
    (z_ref, fo_ref, inv_ref, flags_ref), refs = refs[:4], refs[4:]
    older_ref = refs[0] if has_older else None
    send_ref, *now_ref = refs[1:] if has_older else refs
    firms = next_firms(omega, z_ref, fo_ref, inv_ref, flags_ref, older_ref)
    if now_ref:
        for j in range(FIRM_BLOCKS):
            now_ref[0][j] = firms[j]
    scatter_firms(firms, flags_ref, send_ref)


def close_firm_kernel(omega, z_ref, fo_ref, inv_ref, flags_ref, older_ref, cov_ref, white_ref, now_ref, part_ref):
    firms = next_firms(omega, z_ref, fo_ref, inv_ref, flags_ref, older_ref)
    for j in range(FIRM_BLOCKS):
        now_ref[j] = firms[j]
    projected = product(jnp.concatenate(firms, axis=1), cov_ref[...], ((1,), (0,)))
    whitened = product(projected, white_ref[...], ((1,), (1,)))
    reps = whitened.shape[0]
    columns = whitened.shape[1] // CELLS
    for c in range(columns):
        part_ref[pl.ds(c, reps, stride=columns)] = whitened[:, c * CELLS : (c + 1) * CELLS]


def total_kernel(part_ref, out_ref):
    total = jnp.sum(part_ref[...], axis=0)
    for s in range(out_ref.shape[0]):
        out_ref[s] = total


def moment_kernel(share, all_ref, moment_ref, rows_ref):
    share_rows, covars = moment_ref.shape
    columns = covars // CELLS
    reps = all_ref.shape[0] // columns
    in_block = CELLS // share_rows
    own = all_ref[pl.ds(share[0] // in_block, reps, stride=columns)]
    for c in range(columns):
        other = all_ref[pl.ds(c, reps, stride=columns)]
        rows_ref[:, c * CELLS : (c + 1) * CELLS] = product(own, other, ((0,), (0,)))
    start = pl.multiple_of((share[0] % in_block) * share_rows, share_rows)
    moment_ref[...] = rows_ref[pl.ds(start, share_rows)]


def emit_kernel(all_ref, now_ref, coef_ref, firm_ref):
    reps, covars = coef_ref.shape
    columns = covars // CELLS
    for c in range(columns):
        coef_ref[:, c * CELLS : (c + 1) * CELLS] = all_ref[pl.ds(c, reps, stride=columns)]
    for j in range(FIRM_BLOCKS):
        firm_ref[:, j * CELLS : (j + 1) * CELLS] = now_ref[j]


def keep(value):
    return pltpu.with_memory_space_constraint(value, pltpu.VMEM)


def call(kernel, inputs, outputs, scratch=(), scalars=0, name=None, specs=None, out_specs=None):
    return pl.pallas_call(
        kernel,
        in_specs=specs or [SMEM] * scalars + [VMEM] * (len(inputs) - scalars),
        out_specs=out_specs or [VMEM] * len(outputs),
        out_shape=[pltpu.VMEM(*item[:2]) if len(item) > 2 else jax.ShapeDtypeStruct(*item) for item in outputs],
        scratch_shapes=[item if not isinstance(item, tuple) else pltpu.VMEM(*item) for item in scratch],
        compiler_params=PARAMS,
        name=name,
    )(*inputs)


def body(
    tiles_w,
    tile_worker,
    tile_owner,
    owner_block,
    worker_base,
    worker_noise,
    worker_cluster,
    firm_base,
    firm_noise,
    firm_cluster,
    signs,
    covariates,
    whitening,
):
    owners = lax.axis_size("tiles")
    groups = lax.axis_size("reps")
    reps = signs.shape[0]
    covars = whitening.shape[0]
    omegas = chebyshev_weights(SWEEPS)

    def exchange(values, axes="tiles"):
        return lax.all_to_all(values, axes, 0, 0, tiled=True)

    def rows(values):
        return values.reshape(-1, CELLS)

    push_shape = ((owners, reps, CELLS), BF16)
    work_shape = ((WORK_BLOCKS, reps, CELLS), F32)
    firm_shape = ((FIRM_BLOCKS, reps, CELLS), F32)
    tiles = tiles_w.shape[0]
    plan_shape = ((8, 2 * tiles), jnp.int32)
    held_shape = ((tiles + 1, CELLS, CELLS), BF16, "keep")
    inverse_shape = ((WORK_BLOCKS, 8, CELLS), F32)
    inputs = (rows(tile_worker), rows(tile_owner), owner_block, tiles_w, signs)
    inputs += (rows(worker_base), rows(worker_noise), rows(worker_cluster))
    z, worker_outcome, held, turned, worker_inverse, plan = call(
        first_kernel,
        tuple(pltpu.with_memory_space_constraint(x, pltpu.HBM) for x in inputs),
        (((owners, reps + EXTRA, CELLS), BF16), work_shape, held_shape, held_shape, inverse_shape, plan_shape),
        (
            pltpu.SMEM((1, tiles), jnp.int32),
            pltpu.SMEM((1, tiles), jnp.int32),
            ((1, tiles), jnp.int32),
            ((1, tiles), jnp.int32),
            pltpu.SMEM(owner_block.shape, jnp.int32),
            (signs.shape, jnp.int32),
            ((WORK_BLOCKS, CELLS), F32),
            ((WORK_BLOCKS, CELLS), F32),
            ((WORK_BLOCKS, CELLS), jnp.int32),
            ((WORK_BLOCKS, reps + EXTRA, CELLS), BF16),
            ((owners, reps + EXTRA, CELLS), F32),
            inverse_shape,
            pltpu.SemaphoreType.DMA((9 + CHUNKS,)),
        ),
        specs=[HBM] * 8,
        name="first_push",
    )
    share = lax.axis_index("tiles").astype(jnp.int32).reshape(1)
    share, z = lax.optimization_barrier((share, z))
    z = exchange(z)
    send, firm_outcome, firm_inverse, flags, newer = call(
        open_firm_kernel,
        (z, signs, rows(firm_base), rows(firm_noise), rows(firm_cluster)),
        (push_shape, firm_shape, ((FIRM_BLOCKS, 8, CELLS), F32), ((owners, 8, CELLS), F32), firm_shape),
        name="first_firm",
    )
    older = None
    scratch = (work_shape, ((WORK_BLOCKS, reps, CELLS), BF16))
    scratch += (((owners, reps, CELLS), F32), pltpu.SMEM(*plan_shape), pltpu.SemaphoreType.DMA((2,)))
    for k in range(1, SWEEPS):
        last = k == SWEEPS - 1
        f = exchange(send)
        outputs, more, out_specs = (push_shape,), (), [VMEM]
        if last:
            whole = ((reps, WORK_BLOCKS * CELLS), F32)
            outputs += (whole,)
            more = (whole,)
            out_specs.append(HBM)
        z, *rest = call(
            lambda *refs, e=last: sweep_kernel(e, *refs),
            (plan, keep(held), keep(turned), f, worker_outcome, worker_inverse),
            outputs,
            scratch + more,
            specs=[ANY] + [VMEM] * 5,
            out_specs=out_specs,
            name="sweep_close" if last else "sweep",
        )
        z = exchange(z)
        inputs = (z, firm_outcome, firm_inverse, flags) + (() if older is None else (older,))
        if not last:
            send, *now = call(
                lambda *refs, w=omegas[k], h=older is not None: firm_kernel(w, h, *refs),
                inputs,
                (push_shape, firm_shape) if k < SWEEPS - 2 else (push_shape,),
                name="firm",
            )
            older, newer = newer, now[0] if now else None
        else:
            firms, part = call(
                lambda *refs, w=omegas[k]: close_firm_kernel(w, *refs),
                inputs + (covariates, whitening),
                (firm_shape, ((reps * covars // CELLS, CELLS), F32)),
                name="close_firm",
            )
    part = exchange(part.reshape(owners, -1, CELLS))
    (spread,) = call(total_kernel, (part,), ((part.shape, F32),), name="total")
    everything = exchange(spread).reshape(-1, CELLS)
    (moment,) = call(
        moment_kernel,
        (share, everything),
        (((covars // owners, covars), F32),),
        (((CELLS, covars), F32),),
        scalars=1,
        name="moment",
    )
    coefficients, firm_effect = call(
        emit_kernel,
        (everything, firms),
        (((reps, covars), F32), ((reps, FIRM_BLOCKS * CELLS), F32)),
        name="emit",
    )
    shifted = [lax.ppermute(moment, "reps", [(g, (g + d) % groups) for g in range(groups)]) for d in range(1, groups)]
    covariance = ((moment + shifted[1]) + (shifted[0] + shifted[2])) / (reps * groups)
    return (rest[0], firm_effect, coefficients, covariance)


def solution(mesh):
    placed = (
        P("tiles", None, None),
        P("tiles"),
        P("tiles"),
        P("tiles", None),
        P("tiles"),
        P("tiles"),
        P("tiles"),
        P("tiles"),
        P("tiles"),
        P("tiles"),
        P("reps", None),
        P("tiles", None),
        P(),
    )
    return jax.shard_map(
        body,
        mesh=mesh,
        in_specs=placed,
        out_specs=(P("reps", "tiles"), P("reps", "tiles"), P("reps", None), P("tiles", None)),
        check_vma=False,
    )
```

```python
import jax
import jax.numpy as jnp
from jax import lax
from jax.experimental import pallas as pl
from jax.experimental.pallas import tpu as pltpu
from jax.sharding import PartitionSpec as P

WORK_BLOCKS = 16
FIRM_BLOCKS = 2
SWEEPS = 6
CELLS = 128
EXTRA = 8
SPECTRAL = 0.8
UNROLL = 64
CHUNKS = 4

F32 = jnp.float32
BF16 = jnp.bfloat16
HIGHEST = lax.Precision.HIGHEST

VMEM = pl.BlockSpec(memory_space=pltpu.VMEM)
SMEM = pl.BlockSpec(memory_space=pltpu.SMEM)
HBM = pl.BlockSpec(memory_space=pltpu.HBM)
ANY = pl.BlockSpec(memory_space=pl.ANY)
PARAMS = pltpu.CompilerParams(vmem_limit_bytes=20 << 20)


def chebyshev_weights(count):
    weights = [1.0, 1.0 / (1.0 - 0.5 * SPECTRAL * SPECTRAL)]
    while len(weights) < count:
        weights.append(1.0 / (1.0 - 0.25 * SPECTRAL * SPECTRAL * weights[-1]))
    return weights


def flip_table(signs_ref):
    return (2 * signs_ref[...] - 1).astype(F32).astype(BF16)


def outcome(flips, base, noise, cluster):
    hot = lax.broadcasted_iota(jnp.int32, (flips.shape[1], CELLS), 0) == cluster
    values = jnp.dot(flips, jnp.where(hot, 1.0, 0.0).astype(BF16), preferred_element_type=F32)
    return base + noise * values


def each_tile(count, step, unroll=UNROLL):
    def body(index, carry):
        step(index)
        return carry

    lax.fori_loop(0, count, body, 0, unroll=min(unroll, count))


def add_pairs(count, row, plan, w_ref, x_ref, acc_ref):
    def step(p):
        i = 2 * p
        values = jnp.concatenate([x_ref[plan[row + 2, i]], x_ref[plan[row + 2, i + 1]]], axis=1)
        pair = jnp.concatenate([w_ref[plan[row, i]], w_ref[plan[row, i + 1]]], axis=0)
        acc_ref[plan[row + 1, i]] += jnp.dot(values, pair, preferred_element_type=F32)

    each_tile(count, step, count)


def pair_plan(target, source, slots):
    tiles = target.shape[1]
    along = jnp.broadcast_to(target, (tiles, tiles))
    down = along.T
    sources = jnp.broadcast_to(source, (tiles, tiles)).T
    row = lax.broadcasted_iota(jnp.int32, (tiles, tiles), 0)
    column = lax.broadcasted_iota(jnp.int32, (tiles, tiles), 1)
    same = along == down

    def count(mask, axis):
        return jnp.sum(jnp.where(mask, 1.0, 0.0), axis=axis, keepdims=True)

    size = count(same, 0)
    odd = size - 2.0 * jnp.floor(0.5 * size)
    width = 1.0 + jnp.where(count(same & (row < column), 0) == 0.0, odd, 0.0)
    place = jnp.sum(jnp.where(along < down, width, 0.0), axis=1, keepdims=True) + count(same & (column < row), 1)
    numbers = row.astype(F32) - tiles
    plans = ([], [], [])
    for base in range(0, slots, tiles):
        here = place == column.astype(F32) + base
        plans[0].append(jnp.sum(jnp.where(here, numbers, 0.0), axis=0, keepdims=True) + tiles)
        plans[1].append(jnp.sum(jnp.where(here, down, 0.0), axis=0, keepdims=True))
        plans[2].append(jnp.sum(jnp.where(here, sources, 0.0), axis=0, keepdims=True))
    return [jnp.concatenate(plan, axis=1).astype(jnp.int32) for plan in plans]


def first_kernel(
    tw_hbm, to_hbm, ob_hbm, w_hbm, signs_hbm, base_hbm, noise_hbm, cluster_hbm,
    z_ref, wo_ref, w_ref, turned_ref, inv_ref, plan_ref,
    tw, to, tw_row, to_row, ob, signs_ref, base_ref, noise_ref, cluster_ref, x_ref, acc_ref, mass_ref, sems,
):
    small = [
        (signs_hbm, signs_ref),
        (cluster_hbm, cluster_ref),
        (base_hbm, base_ref),
        (noise_hbm, noise_ref),
        (tw_hbm, tw),
        (to_hbm, to),
        (ob_hbm, ob),
        (tw_hbm, tw_row),
        (to_hbm, to_row),
    ]
    copies = [pltpu.make_async_copy(source, target, sems.at[i]) for i, (source, target) in enumerate(small)]
    tiles = w_hbm.shape[0]
    chunk = tiles // CHUNKS
    loads = []
    for c in range(CHUNKS):
        part = pl.ds(c * chunk, chunk)
        loads.append(pltpu.make_async_copy(w_hbm.at[part], w_ref.at[part], sems.at[len(small) + c]))
    for copy in copies + loads:
        copy.start()
    acc_ref[...] = jnp.zeros_like(acc_ref)
    mass_ref[...] = jnp.zeros_like(mass_ref)
    w_ref[tiles] = jnp.zeros((CELLS, CELLS), BF16)
    turned_ref[tiles] = jnp.zeros((CELLS, CELLS), BF16)
    for copy in copies:
        copy.wait()
    reps = signs_ref.shape[0]
    flips = flip_table(signs_ref)
    for b in range(WORK_BLOCKS):
        row = slice(b, b + 1)
        value = outcome(flips, base_ref[row], noise_ref[row], cluster_ref[row])
        wo_ref[b] = value
        x_ref[b, :reps] = value.astype(BF16)
        x_ref[b, reps:] = jnp.ones((EXTRA, CELLS), BF16)

    def step(t):
        tile = w_ref[t]
        acc_ref[to[0, t]] += jnp.dot(x_ref[tw[0, t]], tile, preferred_element_type=F32)
        turned = tile.T
        turned_ref[t] = turned
        mass_ref[tw[0, t]] += jnp.sum(turned.astype(F32).reshape(CELLS // 8, 8, CELLS), axis=0)

    for c in range(CHUNKS):
        loads[c].wait()
        each_tile(chunk, lambda i, c=c: step(c * chunk + i))
        if c == 0:
            worker, owner = tw_row[...].astype(F32), to_row[...].astype(F32)
            pull = pair_plan(worker, owner, plan_ref.shape[1])
            push = pair_plan(owner, worker, plan_ref.shape[1])
            for r, values in enumerate(pull + push):
                plan_ref[r : r + 1] = values
    for b in range(WORK_BLOCKS):
        inverse = 1.0 / (1.0 + jnp.sum(mass_ref[b], axis=0, keepdims=True))
        inv_ref[b] = jnp.broadcast_to(inverse, (8, CELLS))
    place = lax.broadcasted_iota(jnp.int32, (EXTRA, CELLS), 0)

    def finish(o):
        z_ref[o, :reps] = acc_ref[o, :reps].astype(BF16)
        mass = acc_ref[o, reps:]
        high = mass.astype(BF16).astype(F32)
        middle = (mass - high).astype(BF16).astype(F32)
        low = (mass - high) - middle
        flag = ob[0, o].astype(F32)
        tail = jnp.where(place == 0, high, jnp.where(place == 1, middle, jnp.where(place == 2, low, flag)))
        z_ref[o, reps:] = tail.astype(BF16)

    each_tile(acc_ref.shape[0], finish, 8)


def sweep_kernel(last, *refs):
    plan_any, w_ref, turned_ref, f_ref, wo_ref, inv_ref, z_ref, *refs = refs
    if last:
        out_ref, *refs = refs
    accw_ref, x_ref, accz_ref, plan, sem = refs
    tables = pltpu.make_async_copy(plan_any, plan, sem)
    tables.start()
    tiles, owners = w_ref.shape[0] - 1, z_ref.shape[0]
    accw_ref[...] = jnp.zeros_like(accw_ref)
    accz_ref[...] = jnp.zeros_like(accz_ref)
    tables.wait()
    add_pairs((tiles + WORK_BLOCKS) // 2, 0, plan, turned_ref, f_ref, accw_ref)
    for b in range(WORK_BLOCKS):
        worker = wo_ref[b] - accw_ref[b] * inv_ref[b, :1]
        if last:
            out_ref[:, b * CELLS : (b + 1) * CELLS] = worker
        x_ref[b] = worker.astype(BF16)
    add_pairs((tiles + owners) // 2, 3, plan, w_ref, x_ref, accz_ref)
    z_ref[...] = accz_ref[...].astype(BF16)


def halves(value):
    high = value.astype(BF16)
    return high, (value - high.astype(F32)).astype(BF16)


def product(left, right, dims):
    (a, b), (c, d) = halves(left), halves(right)

    def dot(p, q):
        return lax.dot_general(p, q, (dims, ((), ())), preferred_element_type=F32)

    return (dot(a, d) + dot(b, c)) + dot(a, c)


def gather_sums(z_ref, flags_ref, reps):
    zero = jnp.zeros((reps, CELLS), F32)

    def body(s, carry):
        first, second = carry
        part = z_ref[s, :reps].astype(F32)
        upper = jnp.broadcast_to(flags_ref[s, :1], part.shape) > 0.5
        return first + jnp.where(upper, 0.0, part), second + jnp.where(upper, part, 0.0)

    return lax.fori_loop(0, z_ref.shape[0], body, (zero, zero), unroll=4)


def scatter_firms(firms, flags_ref, send_ref):
    first, second = firms

    def step(s):
        upper = jnp.broadcast_to(flags_ref[s, :1], first.shape) > 0.5
        send_ref[s] = jnp.where(upper, second, first).astype(BF16)

    each_tile(send_ref.shape[0], step, 8)


def open_firm_kernel(z_ref, signs_ref, base_ref, noise_ref, cluster_ref, send_ref, fo_ref, inv_ref, flags_ref, now_ref):
    reps = signs_ref.shape[0]
    owners = z_ref.shape[0]
    mass = [jnp.zeros((1, CELLS), F32), jnp.zeros((1, CELLS), F32)]
    for s in range(owners):
        tail = z_ref[s, reps:].astype(F32)
        flags_ref[s] = jnp.broadcast_to(tail[3:4], (8, CELLS))
        part = tail[0:1] + tail[1:2] + tail[2:3]
        upper = tail[3:4] > 0.5
        mass = [mass[0] + jnp.where(upper, 0.0, part), mass[1] + jnp.where(upper, part, 0.0)]
    sums = gather_sums(z_ref, flags_ref, reps)
    flips = flip_table(signs_ref)
    firms = []
    for j in range(FIRM_BLOCKS):
        row = slice(j, j + 1)
        inverse = 1.0 / (1.0 + mass[j])
        value = outcome(flips, base_ref[row], noise_ref[row], cluster_ref[row])
        fo_ref[j] = value
        inv_ref[j] = jnp.broadcast_to(inverse, (8, CELLS))
        firm = value - sums[j] * inverse
        now_ref[j] = firm
        firms.append(firm)
    scatter_firms(firms, flags_ref, send_ref)


def next_firms(omega, z_ref, fo_ref, inv_ref, flags_ref, older_ref):
    sums = gather_sums(z_ref, flags_ref, z_ref.shape[1])
    firms = []
    for j in range(FIRM_BLOCKS):
        target = fo_ref[j] - sums[j] * inv_ref[j, :1]
        if older_ref is None:
            firms.append(omega * target)
        else:
            firms.append(older_ref[j] + omega * (target - older_ref[j]))
    return firms


def firm_kernel(omega, has_older, *refs):
    (z_ref, fo_ref, inv_ref, flags_ref), refs = refs[:4], refs[4:]
    older_ref = refs[0] if has_older else None
    send_ref, *now_ref = refs[1:] if has_older else refs
    firms = next_firms(omega, z_ref, fo_ref, inv_ref, flags_ref, older_ref)
    if now_ref:
        for j in range(FIRM_BLOCKS):
            now_ref[0][j] = firms[j]
    scatter_firms(firms, flags_ref, send_ref)


def close_firm_kernel(omega, z_ref, fo_ref, inv_ref, flags_ref, older_ref, cov_ref, white_ref, now_ref, part_ref):
    firms = next_firms(omega, z_ref, fo_ref, inv_ref, flags_ref, older_ref)
    for j in range(FIRM_BLOCKS):
        now_ref[j] = firms[j]
    projected = product(jnp.concatenate(firms, axis=1), cov_ref[...], ((1,), (0,)))
    whitened = product(projected, white_ref[...], ((1,), (1,)))
    reps = whitened.shape[0]
    columns = whitened.shape[1] // CELLS
    for c in range(columns):
        part_ref[pl.ds(c, reps, stride=columns)] = whitened[:, c * CELLS : (c + 1) * CELLS]


def total_kernel(part_ref, out_ref):
    total = jnp.sum(part_ref[...], axis=0)
    for s in range(out_ref.shape[0]):
        out_ref[s] = total


def moment_kernel(share, all_ref, moment_ref, rows_ref):
    share_rows, covars = moment_ref.shape
    columns = covars // CELLS
    reps = all_ref.shape[0] // columns
    in_block = CELLS // share_rows
    own = all_ref[pl.ds(share[0] // in_block, reps, stride=columns)]
    for c in range(columns):
        other = all_ref[pl.ds(c, reps, stride=columns)]
        rows_ref[:, c * CELLS : (c + 1) * CELLS] = product(own, other, ((0,), (0,)))
    start = pl.multiple_of((share[0] % in_block) * share_rows, share_rows)
    moment_ref[...] = rows_ref[pl.ds(start, share_rows)]


def emit_kernel(all_ref, now_ref, worker_ref, coef_ref, firm_ref, out_hbm, sem):
    copy = pltpu.make_async_copy(worker_ref, out_hbm, sem)
    copy.start()
    reps, covars = coef_ref.shape
    columns = covars // CELLS
    for c in range(columns):
        coef_ref[:, c * CELLS : (c + 1) * CELLS] = all_ref[pl.ds(c, reps, stride=columns)]
    for j in range(FIRM_BLOCKS):
        firm_ref[:, j * CELLS : (j + 1) * CELLS] = now_ref[j]
    copy.wait()


def keep(value):
    return pltpu.with_memory_space_constraint(value, pltpu.VMEM)


def call(kernel, inputs, outputs, scratch=(), scalars=0, name=None, specs=None, out_specs=None):
    return pl.pallas_call(
        kernel,
        in_specs=specs or [SMEM] * scalars + [VMEM] * (len(inputs) - scalars),
        out_specs=out_specs or [VMEM] * len(outputs),
        out_shape=[pltpu.VMEM(*item[:2]) if len(item) > 2 else jax.ShapeDtypeStruct(*item) for item in outputs],
        scratch_shapes=[item if not isinstance(item, tuple) else pltpu.VMEM(*item) for item in scratch],
        compiler_params=PARAMS,
        name=name,
    )(*inputs)


def body(
    tiles_w,
    tile_worker,
    tile_owner,
    owner_block,
    worker_base,
    worker_noise,
    worker_cluster,
    firm_base,
    firm_noise,
    firm_cluster,
    signs,
    covariates,
    whitening,
):
    owners = lax.axis_size("tiles")
    groups = lax.axis_size("reps")
    reps = signs.shape[0]
    covars = whitening.shape[0]
    omegas = chebyshev_weights(SWEEPS)

    def exchange(values, axes="tiles"):
        return lax.all_to_all(values, axes, 0, 0, tiled=True)

    def rows(values):
        return values.reshape(-1, CELLS)

    push_shape = ((owners, reps, CELLS), BF16)
    work_shape = ((WORK_BLOCKS, reps, CELLS), F32)
    firm_shape = ((FIRM_BLOCKS, reps, CELLS), F32)
    tiles = tiles_w.shape[0]
    plan_shape = ((8, 2 * tiles), jnp.int32)
    held_shape = ((tiles + 1, CELLS, CELLS), BF16, "keep")
    inverse_shape = ((WORK_BLOCKS, 8, CELLS), F32)
    inputs = (rows(tile_worker), rows(tile_owner), owner_block, tiles_w, signs)
    inputs += (rows(worker_base), rows(worker_noise), rows(worker_cluster))
    z, worker_outcome, held, turned, worker_inverse, plan = call(
        first_kernel,
        tuple(pltpu.with_memory_space_constraint(x, pltpu.HBM) for x in inputs),
        (((owners, reps + EXTRA, CELLS), BF16), work_shape, held_shape, held_shape, inverse_shape, plan_shape),
        (
            pltpu.SMEM((1, tiles), jnp.int32),
            pltpu.SMEM((1, tiles), jnp.int32),
            ((1, tiles), jnp.int32),
            ((1, tiles), jnp.int32),
            pltpu.SMEM(owner_block.shape, jnp.int32),
            (signs.shape, jnp.int32),
            ((WORK_BLOCKS, CELLS), F32),
            ((WORK_BLOCKS, CELLS), F32),
            ((WORK_BLOCKS, CELLS), jnp.int32),
            ((WORK_BLOCKS, reps + EXTRA, CELLS), BF16),
            ((owners, reps + EXTRA, CELLS), F32),
            inverse_shape,
            pltpu.SemaphoreType.DMA((9 + CHUNKS,)),
        ),
        specs=[HBM] * 8,
        name="first_push",
    )
    share = lax.axis_index("tiles").astype(jnp.int32).reshape(1)
    share, z = lax.optimization_barrier((share, z))
    z = exchange(z)
    send, firm_outcome, firm_inverse, flags, newer = call(
        open_firm_kernel,
        (z, signs, rows(firm_base), rows(firm_noise), rows(firm_cluster)),
        (push_shape, firm_shape, ((FIRM_BLOCKS, 8, CELLS), F32), ((owners, 8, CELLS), F32), firm_shape),
        name="first_firm",
    )
    older = None
    scratch = (work_shape, ((WORK_BLOCKS, reps, CELLS), BF16))
    scratch += (((owners, reps, CELLS), F32), pltpu.SMEM(*plan_shape), pltpu.SemaphoreType.DMA)
    for k in range(1, SWEEPS):
        last = k == SWEEPS - 1
        f = exchange(send)
        outputs = (push_shape,)
        if last:
            outputs += (((reps, WORK_BLOCKS * CELLS), F32, "keep"),)
        z, *rest = call(
            lambda *refs, e=last: sweep_kernel(e, *refs),
            (plan, keep(held), keep(turned), f, worker_outcome, worker_inverse),
            outputs,
            scratch,
            specs=[ANY] + [VMEM] * 5,
            name="sweep_close" if last else "sweep",
        )
        z = exchange(z)
        inputs = (z, firm_outcome, firm_inverse, flags) + (() if older is None else (older,))
        if not last:
            send, *now = call(
                lambda *refs, w=omegas[k], h=older is not None: firm_kernel(w, h, *refs),
                inputs,
                (push_shape, firm_shape) if k < SWEEPS - 2 else (push_shape,),
                name="firm",
            )
            older, newer = newer, now[0] if now else None
        else:
            firms, part = call(
                lambda *refs, w=omegas[k]: close_firm_kernel(w, *refs),
                inputs + (covariates, whitening),
                (firm_shape, ((reps * covars // CELLS, CELLS), F32)),
                name="close_firm",
            )
    part = exchange(part.reshape(owners, -1, CELLS))
    (spread,) = call(total_kernel, (part,), ((part.shape, F32),), name="total")
    everything = exchange(spread).reshape(-1, CELLS)
    (moment,) = call(
        moment_kernel,
        (share, everything),
        (((covars // owners, covars), F32),),
        (((CELLS, covars), F32),),
        scalars=1,
        name="moment",
    )
    workers = keep(rest[0])
    coefficients, firm_effect, worker_effect = call(
        emit_kernel,
        (everything, firms, workers),
        (((reps, covars), F32), ((reps, FIRM_BLOCKS * CELLS), F32), (workers.shape, F32)),
        (pltpu.SemaphoreType.DMA,),
        out_specs=[VMEM, VMEM, HBM],
        name="emit",
    )
    shifted = [lax.ppermute(moment, "reps", [(g, (g + d) % groups) for g in range(groups)]) for d in range(1, groups)]
    covariance = ((moment + shifted[1]) + (shifted[0] + shifted[2])) / (reps * groups)
    return (worker_effect, firm_effect, coefficients, covariance)


def solution(mesh):
    placed = (
        P("tiles", None, None),
        P("tiles"),
        P("tiles"),
        P("tiles", None),
        P("tiles"),
        P("tiles"),
        P("tiles"),
        P("tiles"),
        P("tiles"),
        P("tiles"),
        P("reps", None),
        P("tiles", None),
        P(),
    )
    return jax.shard_map(
        body,
        mesh=mesh,
        in_specs=placed,
        out_specs=(P("reps", "tiles"), P("reps", "tiles"), P("reps", None), P("tiles", None)),
        check_vma=False,
    )
```

```python
import jax
import jax.numpy as jnp
from jax import lax
from jax.experimental import pallas as pl
from jax.experimental.pallas import tpu as pltpu
from jax.sharding import PartitionSpec as P

WORK_BLOCKS = 16
FIRM_BLOCKS = 2
SWEEPS = 6
CELLS = 128
EXTRA = 8
SPECTRAL = 0.8
UNROLL = 64
CHUNKS = 4

F32 = jnp.float32
BF16 = jnp.bfloat16
HIGHEST = lax.Precision.HIGHEST

VMEM = pl.BlockSpec(memory_space=pltpu.VMEM)
SMEM = pl.BlockSpec(memory_space=pltpu.SMEM)
HBM = pl.BlockSpec(memory_space=pltpu.HBM)
ANY = pl.BlockSpec(memory_space=pl.ANY)
PARAMS = pltpu.CompilerParams(vmem_limit_bytes=20 << 20)


def chebyshev_weights(count):
    weights = [1.0, 1.0 / (1.0 - 0.5 * SPECTRAL * SPECTRAL)]
    while len(weights) < count:
        weights.append(1.0 / (1.0 - 0.25 * SPECTRAL * SPECTRAL * weights[-1]))
    return weights


def flip_table(signs_ref):
    return (2 * signs_ref[...] - 1).astype(F32).astype(BF16)


def outcome(flips, base, noise, cluster):
    hot = lax.broadcasted_iota(jnp.int32, (flips.shape[1], CELLS), 0) == cluster
    values = jnp.dot(flips, jnp.where(hot, 1.0, 0.0).astype(BF16), preferred_element_type=F32)
    return base + noise * values


def each_tile(count, step, unroll=UNROLL):
    def body(index, carry):
        step(index)
        return carry

    lax.fori_loop(0, count, body, 0, unroll=min(unroll, count))


def add_pairs(count, row, plan, w_ref, x_ref, acc_ref):
    def step(p):
        i = 2 * p
        values = jnp.concatenate([x_ref[plan[row + 2, i]], x_ref[plan[row + 2, i + 1]]], axis=1)
        pair = jnp.concatenate([w_ref[plan[row, i]], w_ref[plan[row, i + 1]]], axis=0)
        acc_ref[plan[row + 1, i]] += jnp.dot(values, pair, preferred_element_type=F32)

    each_tile(count, step, count)


def pair_plan(target, source, slots):
    tiles = target.shape[1]
    along = jnp.broadcast_to(target, (tiles, tiles))
    down = along.T
    sources = jnp.broadcast_to(source, (tiles, tiles)).T
    row = lax.broadcasted_iota(jnp.int32, (tiles, tiles), 0)
    column = lax.broadcasted_iota(jnp.int32, (tiles, tiles), 1)
    same = along == down

    def count(mask, axis):
        return jnp.sum(jnp.where(mask, 1.0, 0.0), axis=axis, keepdims=True)

    size = count(same, 0)
    odd = size - 2.0 * jnp.floor(0.5 * size)
    width = 1.0 + jnp.where(count(same & (row < column), 0) == 0.0, odd, 0.0)
    place = jnp.sum(jnp.where(along < down, width, 0.0), axis=1, keepdims=True) + count(same & (column < row), 1)
    numbers = row.astype(F32) - tiles
    plans = ([], [], [])
    for base in range(0, slots, tiles):
        here = place == column.astype(F32) + base
        plans[0].append(jnp.sum(jnp.where(here, numbers, 0.0), axis=0, keepdims=True) + tiles)
        plans[1].append(jnp.sum(jnp.where(here, down, 0.0), axis=0, keepdims=True))
        plans[2].append(jnp.sum(jnp.where(here, sources, 0.0), axis=0, keepdims=True))
    return [jnp.concatenate(plan, axis=1).astype(jnp.int32) for plan in plans]


def first_kernel(
    tw_hbm, to_hbm, ob_hbm, w_hbm, signs_hbm, base_hbm, noise_hbm, cluster_hbm,
    z_ref, wo_ref, w_ref, turned_ref, inv_ref, plan_ref,
    tw, to, tw_row, to_row, ob, signs_ref, base_ref, noise_ref, cluster_ref, x_ref, acc_ref, mass_ref, sems,
):
    small = [
        (signs_hbm, signs_ref),
        (cluster_hbm, cluster_ref),
        (base_hbm, base_ref),
        (noise_hbm, noise_ref),
        (tw_hbm, tw),
        (to_hbm, to),
        (ob_hbm, ob),
        (tw_hbm, tw_row),
        (to_hbm, to_row),
    ]
    copies = [pltpu.make_async_copy(source, target, sems.at[i]) for i, (source, target) in enumerate(small)]
    tiles = w_hbm.shape[0]
    chunk = tiles // CHUNKS
    loads = []
    for c in range(CHUNKS):
        part = pl.ds(c * chunk, chunk)
        loads.append(pltpu.make_async_copy(w_hbm.at[part], w_ref.at[part], sems.at[len(small) + c]))
    for copy in copies + loads:
        copy.start()
    acc_ref[...] = jnp.zeros_like(acc_ref)
    mass_ref[...] = jnp.zeros_like(mass_ref)
    w_ref[tiles] = jnp.zeros((CELLS, CELLS), BF16)
    turned_ref[tiles] = jnp.zeros((CELLS, CELLS), BF16)
    for copy in copies:
        copy.wait()
    reps = signs_ref.shape[0]
    flips = flip_table(signs_ref)
    for b in range(WORK_BLOCKS):
        row = slice(b, b + 1)
        value = outcome(flips, base_ref[row], noise_ref[row], cluster_ref[row])
        wo_ref[b] = value
        x_ref[b, :reps] = value.astype(BF16)
        x_ref[b, reps:] = jnp.ones((EXTRA, CELLS), BF16)

    def step(t):
        tile = w_ref[t]
        acc_ref[to[0, t]] += jnp.dot(x_ref[tw[0, t]], tile, preferred_element_type=F32)
        turned = tile.T
        turned_ref[t] = turned
        mass_ref[tw[0, t]] += jnp.sum(turned.astype(F32).reshape(CELLS // 8, 8, CELLS), axis=0)

    for c in range(CHUNKS):
        loads[c].wait()
        each_tile(chunk, lambda i, c=c: step(c * chunk + i))
        if c == 0:
            worker, owner = tw_row[...].astype(F32), to_row[...].astype(F32)
            pull = pair_plan(worker, owner, plan_ref.shape[1])
            push = pair_plan(owner, worker, plan_ref.shape[1])
            for r, values in enumerate(pull + push):
                plan_ref[r : r + 1] = values
    for b in range(WORK_BLOCKS):
        inverse = 1.0 / (1.0 + jnp.sum(mass_ref[b], axis=0, keepdims=True))
        inv_ref[b] = jnp.broadcast_to(inverse, (8, CELLS))
    place = lax.broadcasted_iota(jnp.int32, (EXTRA, CELLS), 0)

    def finish(o):
        z_ref[o, :reps] = acc_ref[o, :reps].astype(BF16)
        mass = acc_ref[o, reps:]
        high = mass.astype(BF16).astype(F32)
        middle = (mass - high).astype(BF16).astype(F32)
        low = (mass - high) - middle
        flag = ob[0, o].astype(F32)
        tail = jnp.where(place == 0, high, jnp.where(place == 1, middle, jnp.where(place == 2, low, flag)))
        z_ref[o, reps:] = tail.astype(BF16)

    each_tile(acc_ref.shape[0], finish, 8)


def sweep_kernel(last, *refs):
    plan_any, w_ref, turned_ref, f_ref, wo_ref, inv_ref, z_ref, *refs = refs
    if last:
        out_ref, *refs = refs
    accw_ref, x_ref, accz_ref, plan, sem = refs
    tables = pltpu.make_async_copy(plan_any, plan, sem)
    tables.start()
    tiles, owners = w_ref.shape[0] - 1, z_ref.shape[0]
    accw_ref[...] = jnp.zeros_like(accw_ref)
    accz_ref[...] = jnp.zeros_like(accz_ref)
    tables.wait()
    add_pairs((tiles + WORK_BLOCKS) // 2, 0, plan, turned_ref, f_ref, accw_ref)
    for b in range(WORK_BLOCKS):
        worker = wo_ref[b] - accw_ref[b] * inv_ref[b, :1]
        if last:
            out_ref[:, b * CELLS : (b + 1) * CELLS] = worker
        x_ref[b] = worker.astype(BF16)
    add_pairs((tiles + owners) // 2, 3, plan, w_ref, x_ref, accz_ref)
    z_ref[...] = accz_ref[...].astype(BF16)


def halves(value):
    high = value.astype(BF16)
    return high, (value - high.astype(F32)).astype(BF16)


def product(left, right, dims):
    (a, b), (c, d) = halves(left), halves(right)

    def dot(p, q):
        return lax.dot_general(p, q, (dims, ((), ())), preferred_element_type=F32)

    rows = a.shape[1 - dims[0][0]]
    both = dot(jnp.concatenate([a, b], axis=1 - dims[0][0]), c)
    return (dot(a, d) + both[rows:]) + both[:rows]


def gather_sums(z_ref, flags_ref, reps):
    zero = jnp.zeros((reps, CELLS), F32)

    def body(s, carry):
        first, second = carry
        part = z_ref[s, :reps].astype(F32)
        upper = jnp.broadcast_to(flags_ref[s, :1], part.shape) > 0.5
        return first + jnp.where(upper, 0.0, part), second + jnp.where(upper, part, 0.0)

    return lax.fori_loop(0, z_ref.shape[0], body, (zero, zero), unroll=16)


def scatter_firms(firms, flags_ref, send_ref):
    first, second = firms

    def step(s):
        upper = jnp.broadcast_to(flags_ref[s, :1], first.shape) > 0.5
        send_ref[s] = jnp.where(upper, second, first).astype(BF16)

    each_tile(send_ref.shape[0], step, 16)


def open_firm_kernel(z_ref, signs_ref, base_ref, noise_ref, cluster_ref, send_ref, fo_ref, inv_ref, flags_ref, now_ref):
    reps = signs_ref.shape[0]
    owners = z_ref.shape[0]
    mass = [jnp.zeros((1, CELLS), F32), jnp.zeros((1, CELLS), F32)]
    for s in range(owners):
        tail = z_ref[s, reps:].astype(F32)
        flags_ref[s] = jnp.broadcast_to(tail[3:4], (8, CELLS))
        part = tail[0:1] + tail[1:2] + tail[2:3]
        upper = tail[3:4] > 0.5
        mass = [mass[0] + jnp.where(upper, 0.0, part), mass[1] + jnp.where(upper, part, 0.0)]
    sums = gather_sums(z_ref, flags_ref, reps)
    flips = flip_table(signs_ref)
    firms = []
    for j in range(FIRM_BLOCKS):
        row = slice(j, j + 1)
        inverse = 1.0 / (1.0 + mass[j])
        value = outcome(flips, base_ref[row], noise_ref[row], cluster_ref[row])
        fo_ref[j] = value
        inv_ref[j] = jnp.broadcast_to(inverse, (8, CELLS))
        firm = value - sums[j] * inverse
        now_ref[j] = firm
        firms.append(firm)
    scatter_firms(firms, flags_ref, send_ref)


def next_firms(omega, z_ref, fo_ref, inv_ref, flags_ref, older_ref):
    sums = gather_sums(z_ref, flags_ref, z_ref.shape[1])
    firms = []
    for j in range(FIRM_BLOCKS):
        target = fo_ref[j] - sums[j] * inv_ref[j, :1]
        if older_ref is None:
            firms.append(omega * target)
        else:
            firms.append(older_ref[j] + omega * (target - older_ref[j]))
    return firms


def firm_kernel(omega, has_older, *refs):
    (z_ref, fo_ref, inv_ref, flags_ref), refs = refs[:4], refs[4:]
    older_ref = refs[0] if has_older else None
    send_ref, *now_ref = refs[1:] if has_older else refs
    firms = next_firms(omega, z_ref, fo_ref, inv_ref, flags_ref, older_ref)
    if now_ref:
        for j in range(FIRM_BLOCKS):
            now_ref[0][j] = firms[j]
    scatter_firms(firms, flags_ref, send_ref)


def close_firm_kernel(omega, z_ref, fo_ref, inv_ref, flags_ref, older_ref, cov_ref, white_ref, now_ref, part_ref):
    firms = next_firms(omega, z_ref, fo_ref, inv_ref, flags_ref, older_ref)
    for j in range(FIRM_BLOCKS):
        now_ref[j] = firms[j]
    projected = product(jnp.concatenate(firms, axis=1), cov_ref[...], ((1,), (0,)))
    whitened = product(projected, white_ref[...], ((1,), (1,)))
    reps = whitened.shape[0]
    columns = whitened.shape[1] // CELLS
    for c in range(columns):
        part_ref[pl.ds(c, reps, stride=columns)] = whitened[:, c * CELLS : (c + 1) * CELLS]


def total_kernel(part_ref, out_ref):
    total = jnp.sum(part_ref[...], axis=0)
    for s in range(out_ref.shape[0]):
        out_ref[s] = total


def moment_kernel(share, all_ref, moment_ref, rows_ref):
    share_rows, covars = moment_ref.shape
    columns = covars // CELLS
    reps = all_ref.shape[0] // columns
    in_block = CELLS // share_rows
    own = all_ref[pl.ds(share[0] // in_block, reps, stride=columns)]
    for c in range(columns):
        other = all_ref[pl.ds(c, reps, stride=columns)]
        rows_ref[:, c * CELLS : (c + 1) * CELLS] = product(own, other, ((0,), (0,)))
    start = pl.multiple_of((share[0] % in_block) * share_rows, share_rows)
    moment_ref[...] = rows_ref[pl.ds(start, share_rows)]


def emit_kernel(all_ref, now_ref, worker_ref, coef_ref, firm_ref, out_hbm, sem):
    copy = pltpu.make_async_copy(worker_ref, out_hbm, sem)
    copy.start()
    reps, covars = coef_ref.shape
    columns = covars // CELLS
    for c in range(columns):
        coef_ref[:, c * CELLS : (c + 1) * CELLS] = all_ref[pl.ds(c, reps, stride=columns)]
    for j in range(FIRM_BLOCKS):
        firm_ref[:, j * CELLS : (j + 1) * CELLS] = now_ref[j]
    copy.wait()


def keep(value):
    return pltpu.with_memory_space_constraint(value, pltpu.VMEM)


def call(kernel, inputs, outputs, scratch=(), scalars=0, name=None, specs=None, out_specs=None):
    return pl.pallas_call(
        kernel,
        in_specs=specs or [SMEM] * scalars + [VMEM] * (len(inputs) - scalars),
        out_specs=out_specs or [VMEM] * len(outputs),
        out_shape=[pltpu.VMEM(*item[:2]) if len(item) > 2 else jax.ShapeDtypeStruct(*item) for item in outputs],
        scratch_shapes=[item if not isinstance(item, tuple) else pltpu.VMEM(*item) for item in scratch],
        compiler_params=PARAMS,
        name=name,
    )(*inputs)


def body(
    tiles_w,
    tile_worker,
    tile_owner,
    owner_block,
    worker_base,
    worker_noise,
    worker_cluster,
    firm_base,
    firm_noise,
    firm_cluster,
    signs,
    covariates,
    whitening,
):
    owners = lax.axis_size("tiles")
    groups = lax.axis_size("reps")
    reps = signs.shape[0]
    covars = whitening.shape[0]
    omegas = chebyshev_weights(SWEEPS)

    def exchange(values, axes="tiles"):
        return lax.all_to_all(values, axes, 0, 0, tiled=True)

    def rows(values):
        return values.reshape(-1, CELLS)

    push_shape = ((owners, reps, CELLS), BF16)
    work_shape = ((WORK_BLOCKS, reps, CELLS), F32)
    firm_shape = ((FIRM_BLOCKS, reps, CELLS), F32)
    tiles = tiles_w.shape[0]
    plan_shape = ((8, 2 * tiles), jnp.int32)
    held_shape = ((tiles + 1, CELLS, CELLS), BF16, "keep")
    inverse_shape = ((WORK_BLOCKS, 8, CELLS), F32)
    inputs = (rows(tile_worker), rows(tile_owner), owner_block, tiles_w, signs)
    inputs += (rows(worker_base), rows(worker_noise), rows(worker_cluster))
    z, worker_outcome, held, turned, worker_inverse, plan = call(
        first_kernel,
        tuple(pltpu.with_memory_space_constraint(x, pltpu.HBM) for x in inputs),
        (((owners, reps + EXTRA, CELLS), BF16), work_shape, held_shape, held_shape, inverse_shape, plan_shape),
        (
            pltpu.SMEM((1, tiles), jnp.int32),
            pltpu.SMEM((1, tiles), jnp.int32),
            ((1, tiles), jnp.int32),
            ((1, tiles), jnp.int32),
            pltpu.SMEM(owner_block.shape, jnp.int32),
            (signs.shape, jnp.int32),
            ((WORK_BLOCKS, CELLS), F32),
            ((WORK_BLOCKS, CELLS), F32),
            ((WORK_BLOCKS, CELLS), jnp.int32),
            ((WORK_BLOCKS, reps + EXTRA, CELLS), BF16),
            ((owners, reps + EXTRA, CELLS), F32),
            inverse_shape,
            pltpu.SemaphoreType.DMA((9 + CHUNKS,)),
        ),
        specs=[HBM] * 8,
        name="first_push",
    )
    share = lax.axis_index("tiles").astype(jnp.int32).reshape(1)
    share, z = lax.optimization_barrier((share, z))
    z = exchange(z)
    send, firm_outcome, firm_inverse, flags, newer = call(
        open_firm_kernel,
        (z, signs, rows(firm_base), rows(firm_noise), rows(firm_cluster)),
        (push_shape, firm_shape, ((FIRM_BLOCKS, 8, CELLS), F32), ((owners, 8, CELLS), F32), firm_shape),
        name="first_firm",
    )
    older = None
    scratch = (work_shape, ((WORK_BLOCKS, reps, CELLS), BF16))
    scratch += (((owners, reps, CELLS), F32), pltpu.SMEM(*plan_shape), pltpu.SemaphoreType.DMA)
    for k in range(1, SWEEPS):
        last = k == SWEEPS - 1
        f = exchange(send)
        outputs = (push_shape,)
        if last:
            outputs += (((reps, WORK_BLOCKS * CELLS), F32, "keep"),)
        z, *rest = call(
            lambda *refs, e=last: sweep_kernel(e, *refs),
            (plan, keep(held), keep(turned), f, worker_outcome, worker_inverse),
            outputs,
            scratch,
            specs=[ANY] + [VMEM] * 5,
            name="sweep_close" if last else "sweep",
        )
        z = exchange(z)
        inputs = (z, firm_outcome, firm_inverse, flags) + (() if older is None else (older,))
        if not last:
            send, *now = call(
                lambda *refs, w=omegas[k], h=older is not None: firm_kernel(w, h, *refs),
                inputs,
                (push_shape, firm_shape) if k < SWEEPS - 2 else (push_shape,),
                name="firm",
            )
            older, newer = newer, now[0] if now else None
        else:
            firms, part = call(
                lambda *refs, w=omegas[k]: close_firm_kernel(w, *refs),
                inputs + (covariates, whitening),
                (firm_shape, ((reps * covars // CELLS, CELLS), F32)),
                name="close_firm",
            )
    part = exchange(part.reshape(owners, -1, CELLS))
    (spread,) = call(total_kernel, (part,), ((part.shape, F32),), name="total")
    everything = exchange(spread).reshape(-1, CELLS)
    (moment,) = call(
        moment_kernel,
        (share, everything),
        (((covars // owners, covars), F32),),
        (((CELLS, covars), F32),),
        scalars=1,
        name="moment",
    )
    workers = keep(rest[0])
    coefficients, firm_effect, worker_effect = call(
        emit_kernel,
        (everything, firms, workers),
        (((reps, covars), F32), ((reps, FIRM_BLOCKS * CELLS), F32), (workers.shape, F32)),
        (pltpu.SemaphoreType.DMA,),
        out_specs=[VMEM, VMEM, HBM],
        name="emit",
    )
    shifted = [lax.ppermute(moment, "reps", [(g, (g + d) % groups) for g in range(groups)]) for d in range(1, groups)]
    covariance = ((moment + shifted[1]) + (shifted[0] + shifted[2])) / (reps * groups)
    return (worker_effect, firm_effect, coefficients, covariance)


def solution(mesh):
    placed = (
        P("tiles", None, None),
        P("tiles"),
        P("tiles"),
        P("tiles", None),
        P("tiles"),
        P("tiles"),
        P("tiles"),
        P("tiles"),
        P("tiles"),
        P("tiles"),
        P("reps", None),
        P("tiles", None),
        P(),
    )
    return jax.shard_map(
        body,
        mesh=mesh,
        in_specs=placed,
        out_specs=(P("reps", "tiles"), P("reps", "tiles"), P("reps", None), P("tiles", None)),
        check_vma=False,
    )
```

```python
import jax
import jax.numpy as jnp
from jax import lax
from jax.experimental import pallas as pl
from jax.experimental.pallas import tpu as pltpu
from jax.sharding import PartitionSpec as P

WORK_BLOCKS = 16
FIRM_BLOCKS = 2
SWEEPS = 6
CELLS = 128
EXTRA = 8
SPECTRAL = 0.8
UNROLL = 64
CHUNKS = 2

F32 = jnp.float32
BF16 = jnp.bfloat16
HIGHEST = lax.Precision.HIGHEST

VMEM = pl.BlockSpec(memory_space=pltpu.VMEM)
SMEM = pl.BlockSpec(memory_space=pltpu.SMEM)
HBM = pl.BlockSpec(memory_space=pltpu.HBM)
ANY = pl.BlockSpec(memory_space=pl.ANY)
PARAMS = pltpu.CompilerParams(vmem_limit_bytes=20 << 20)


def chebyshev_weights(count):
    weights = [1.0, 1.0 / (1.0 - 0.5 * SPECTRAL * SPECTRAL)]
    while len(weights) < count:
        weights.append(1.0 / (1.0 - 0.25 * SPECTRAL * SPECTRAL * weights[-1]))
    return weights


def flip_table(signs_ref):
    return (2 * signs_ref[...] - 1).astype(F32).astype(BF16)


def outcome(flips, base, noise, cluster):
    hot = lax.broadcasted_iota(jnp.int32, (flips.shape[1], CELLS), 0) == cluster
    values = jnp.dot(flips, jnp.where(hot, 1.0, 0.0).astype(BF16), preferred_element_type=F32)
    return base + noise * values


def each_tile(count, step, unroll=UNROLL):
    def body(index, carry):
        step(index)
        return carry

    lax.fori_loop(0, count, body, 0, unroll=min(unroll, count))


def add_pairs(count, row, plan, w_ref, x_ref, acc_ref):
    def step(p):
        i = 2 * p
        values = jnp.concatenate([x_ref[plan[row + 2, i]], x_ref[plan[row + 2, i + 1]]], axis=1)
        pair = jnp.concatenate([w_ref[plan[row, i]], w_ref[plan[row, i + 1]]], axis=0)
        acc_ref[plan[row + 1, i]] += jnp.dot(values, pair, preferred_element_type=F32)

    each_tile(count, step, count)


def pair_plan(target, source, slots):
    tiles = target.shape[1]
    along = jnp.broadcast_to(target, (tiles, tiles))
    down = along.T
    sources = jnp.broadcast_to(source, (tiles, tiles)).T
    row = lax.broadcasted_iota(jnp.int32, (tiles, tiles), 0)
    column = lax.broadcasted_iota(jnp.int32, (tiles, tiles), 1)
    same = along == down

    def count(mask, axis):
        return jnp.sum(jnp.where(mask, 1.0, 0.0), axis=axis, keepdims=True)

    size = count(same, 0)
    odd = size - 2.0 * jnp.floor(0.5 * size)
    width = 1.0 + jnp.where(count(same & (row < column), 0) == 0.0, odd, 0.0)
    place = jnp.sum(jnp.where(along < down, width, 0.0), axis=1, keepdims=True) + count(same & (column < row), 1)
    numbers = row.astype(F32) - tiles
    plans = ([], [], [])
    for base in range(0, slots, tiles):
        here = place == column.astype(F32) + base
        plans[0].append(jnp.sum(jnp.where(here, numbers, 0.0), axis=0, keepdims=True) + tiles)
        plans[1].append(jnp.sum(jnp.where(here, down, 0.0), axis=0, keepdims=True))
        plans[2].append(jnp.sum(jnp.where(here, sources, 0.0), axis=0, keepdims=True))
    return [jnp.concatenate(plan, axis=1).astype(jnp.int32) for plan in plans]


def first_kernel(
    tw_hbm, to_hbm, ob_hbm, w_hbm, signs_hbm, base_hbm, noise_hbm, cluster_hbm,
    z_ref, wo_ref, w_ref, turned_ref, inv_ref, plan_ref,
    tw, to, tw_row, to_row, ob, signs_ref, base_ref, noise_ref, cluster_ref, x_ref, acc_ref, mass_ref, sems,
):
    small = [
        (signs_hbm, signs_ref),
        (cluster_hbm, cluster_ref),
        (base_hbm, base_ref),
        (noise_hbm, noise_ref),
        (tw_hbm, tw),
        (to_hbm, to),
        (ob_hbm, ob),
        (tw_hbm, tw_row),
        (to_hbm, to_row),
    ]
    copies = [pltpu.make_async_copy(source, target, sems.at[i]) for i, (source, target) in enumerate(small)]
    tiles = w_hbm.shape[0]
    chunk = tiles // CHUNKS
    loads = []
    for c in range(CHUNKS):
        part = pl.ds(c * chunk, chunk)
        loads.append(pltpu.make_async_copy(w_hbm.at[part], w_ref.at[part], sems.at[len(small) + c]))
    for copy in copies + loads:
        copy.start()
    acc_ref[...] = jnp.zeros_like(acc_ref)
    mass_ref[...] = jnp.zeros_like(mass_ref)
    w_ref[tiles] = jnp.zeros((CELLS, CELLS), BF16)
    turned_ref[tiles] = jnp.zeros((CELLS, CELLS), BF16)
    for copy in copies:
        copy.wait()
    reps = signs_ref.shape[0]
    flips = flip_table(signs_ref)
    for b in range(WORK_BLOCKS):
        row = slice(b, b + 1)
        value = outcome(flips, base_ref[row], noise_ref[row], cluster_ref[row])
        wo_ref[b] = value
        x_ref[b, :reps] = value.astype(BF16)
        x_ref[b, reps:] = jnp.ones((EXTRA, CELLS), BF16)

    def step(t):
        tile = w_ref[t]
        acc_ref[to[0, t]] += jnp.dot(x_ref[tw[0, t]], tile, preferred_element_type=F32)
        turned = tile.T
        turned_ref[t] = turned
        mass_ref[tw[0, t]] += jnp.sum(turned.astype(F32).reshape(CELLS // 8, 8, CELLS), axis=0)

    for c in range(CHUNKS):
        loads[c].wait()
        each_tile(chunk, lambda i, c=c: step(c * chunk + i))
        if c == 0:
            worker, owner = tw_row[...].astype(F32), to_row[...].astype(F32)
            pull = pair_plan(worker, owner, plan_ref.shape[1])
            push = pair_plan(owner, worker, plan_ref.shape[1])
            for r, values in enumerate(pull + push):
                plan_ref[r : r + 1] = values
    for b in range(WORK_BLOCKS):
        inverse = 1.0 / (1.0 + jnp.sum(mass_ref[b], axis=0, keepdims=True))
        inv_ref[b] = jnp.broadcast_to(inverse, (8, CELLS))
    place = lax.broadcasted_iota(jnp.int32, (EXTRA, CELLS), 0)

    def finish(o):
        z_ref[o, :reps] = acc_ref[o, :reps].astype(BF16)
        mass = acc_ref[o, reps:]
        high = mass.astype(BF16).astype(F32)
        middle = (mass - high).astype(BF16).astype(F32)
        low = (mass - high) - middle
        flag = ob[0, o].astype(F32)
        tail = jnp.where(place == 0, high, jnp.where(place == 1, middle, jnp.where(place == 2, low, flag)))
        z_ref[o, reps:] = tail.astype(BF16)

    each_tile(acc_ref.shape[0], finish, 8)


def sweep_kernel(last, *refs):
    plan_any, w_ref, turned_ref, f_ref, wo_ref, inv_ref, z_ref, *refs = refs
    if last:
        out_ref, *refs = refs
    accw_ref, x_ref, accz_ref, plan, sem = refs
    tables = pltpu.make_async_copy(plan_any, plan, sem)
    tables.start()
    tiles, owners = w_ref.shape[0] - 1, z_ref.shape[0]
    accw_ref[...] = jnp.zeros_like(accw_ref)
    accz_ref[...] = jnp.zeros_like(accz_ref)
    tables.wait()
    add_pairs((tiles + WORK_BLOCKS) // 2, 0, plan, turned_ref, f_ref, accw_ref)
    for b in range(WORK_BLOCKS):
        worker = wo_ref[b] - accw_ref[b] * inv_ref[b, :1]
        if last:
            out_ref[:, b * CELLS : (b + 1) * CELLS] = worker
        x_ref[b] = worker.astype(BF16)
    add_pairs((tiles + owners) // 2, 3, plan, w_ref, x_ref, accz_ref)
    z_ref[...] = accz_ref[...].astype(BF16)


def halves(value):
    high = value.astype(BF16)
    return high, (value - high.astype(F32)).astype(BF16)


def product(left, right, dims):
    (a, b), (c, d) = halves(left), halves(right)

    def dot(p, q):
        return lax.dot_general(p, q, (dims, ((), ())), preferred_element_type=F32)

    rows = a.shape[1 - dims[0][0]]
    both = dot(jnp.concatenate([a, b], axis=1 - dims[0][0]), c)
    return (dot(a, d) + both[rows:]) + both[:rows]


def gather_sums(z_ref, flags_ref, reps):
    zero = jnp.zeros((reps, CELLS), F32)

    def body(s, carry):
        first, second = carry
        part = z_ref[s, :reps].astype(F32)
        upper = jnp.broadcast_to(flags_ref[s, :1], part.shape) > 0.5
        return first + jnp.where(upper, 0.0, part), second + jnp.where(upper, part, 0.0)

    return lax.fori_loop(0, z_ref.shape[0], body, (zero, zero), unroll=16)


def scatter_firms(firms, flags_ref, send_ref):
    first, second = firms

    def step(s):
        upper = jnp.broadcast_to(flags_ref[s, :1], first.shape) > 0.5
        send_ref[s] = jnp.where(upper, second, first).astype(BF16)

    each_tile(send_ref.shape[0], step, 16)


def open_firm_kernel(z_ref, signs_ref, base_ref, noise_ref, cluster_ref, send_ref, fo_ref, inv_ref, flags_ref, now_ref):
    reps = signs_ref.shape[0]
    owners = z_ref.shape[0]
    mass = [jnp.zeros((1, CELLS), F32), jnp.zeros((1, CELLS), F32)]
    for s in range(owners):
        tail = z_ref[s, reps:].astype(F32)
        flags_ref[s] = jnp.broadcast_to(tail[3:4], (8, CELLS))
        part = tail[0:1] + tail[1:2] + tail[2:3]
        upper = tail[3:4] > 0.5
        mass = [mass[0] + jnp.where(upper, 0.0, part), mass[1] + jnp.where(upper, part, 0.0)]
    sums = gather_sums(z_ref, flags_ref, reps)
    flips = flip_table(signs_ref)
    firms = []
    for j in range(FIRM_BLOCKS):
        row = slice(j, j + 1)
        inverse = 1.0 / (1.0 + mass[j])
        value = outcome(flips, base_ref[row], noise_ref[row], cluster_ref[row])
        fo_ref[j] = value
        inv_ref[j] = jnp.broadcast_to(inverse, (8, CELLS))
        firm = value - sums[j] * inverse
        now_ref[j] = firm
        firms.append(firm)
    scatter_firms(firms, flags_ref, send_ref)


def next_firms(omega, z_ref, fo_ref, inv_ref, flags_ref, older_ref):
    sums = gather_sums(z_ref, flags_ref, z_ref.shape[1])
    firms = []
    for j in range(FIRM_BLOCKS):
        target = fo_ref[j] - sums[j] * inv_ref[j, :1]
        if older_ref is None:
            firms.append(omega * target)
        else:
            firms.append(older_ref[j] + omega * (target - older_ref[j]))
    return firms


def firm_kernel(omega, has_older, *refs):
    (z_ref, fo_ref, inv_ref, flags_ref), refs = refs[:4], refs[4:]
    older_ref = refs[0] if has_older else None
    send_ref, *now_ref = refs[1:] if has_older else refs
    firms = next_firms(omega, z_ref, fo_ref, inv_ref, flags_ref, older_ref)
    if now_ref:
        for j in range(FIRM_BLOCKS):
            now_ref[0][j] = firms[j]
    scatter_firms(firms, flags_ref, send_ref)


def close_firm_kernel(omega, z_ref, fo_ref, inv_ref, flags_ref, older_ref, cov_ref, white_ref, now_ref, part_ref):
    firms = next_firms(omega, z_ref, fo_ref, inv_ref, flags_ref, older_ref)
    for j in range(FIRM_BLOCKS):
        now_ref[j] = firms[j]
    projected = product(jnp.concatenate(firms, axis=1), cov_ref[...], ((1,), (0,)))
    whitened = product(projected, white_ref[...], ((1,), (1,)))
    reps = whitened.shape[0]
    columns = whitened.shape[1] // CELLS
    for c in range(columns):
        part_ref[pl.ds(c, reps, stride=columns)] = whitened[:, c * CELLS : (c + 1) * CELLS]


def total_kernel(part_ref, out_ref):
    total = jnp.sum(part_ref[...], axis=0)
    for s in range(out_ref.shape[0]):
        out_ref[s] = total


def moment_kernel(share, all_ref, moment_ref, rows_ref):
    share_rows, covars = moment_ref.shape
    columns = covars // CELLS
    reps = all_ref.shape[0] // columns
    in_block = CELLS // share_rows
    own = all_ref[pl.ds(share[0] // in_block, reps, stride=columns)]
    for c in range(columns):
        other = all_ref[pl.ds(c, reps, stride=columns)]
        rows_ref[:, c * CELLS : (c + 1) * CELLS] = product(own, other, ((0,), (0,)))
    start = pl.multiple_of((share[0] % in_block) * share_rows, share_rows)
    moment_ref[...] = rows_ref[pl.ds(start, share_rows)]


def emit_kernel(all_ref, now_ref, worker_ref, coef_ref, firm_ref, out_hbm, sem):
    copy = pltpu.make_async_copy(worker_ref, out_hbm, sem)
    copy.start()
    reps, covars = coef_ref.shape
    columns = covars // CELLS
    for c in range(columns):
        coef_ref[:, c * CELLS : (c + 1) * CELLS] = all_ref[pl.ds(c, reps, stride=columns)]
    for j in range(FIRM_BLOCKS):
        firm_ref[:, j * CELLS : (j + 1) * CELLS] = now_ref[j]
    copy.wait()


def keep(value):
    return pltpu.with_memory_space_constraint(value, pltpu.VMEM)


def call(kernel, inputs, outputs, scratch=(), scalars=0, name=None, specs=None, out_specs=None):
    return pl.pallas_call(
        kernel,
        in_specs=specs or [SMEM] * scalars + [VMEM] * (len(inputs) - scalars),
        out_specs=out_specs or [VMEM] * len(outputs),
        out_shape=[pltpu.VMEM(*item[:2]) if len(item) > 2 else jax.ShapeDtypeStruct(*item) for item in outputs],
        scratch_shapes=[item if not isinstance(item, tuple) else pltpu.VMEM(*item) for item in scratch],
        compiler_params=PARAMS,
        name=name,
    )(*inputs)


def body(
    tiles_w,
    tile_worker,
    tile_owner,
    owner_block,
    worker_base,
    worker_noise,
    worker_cluster,
    firm_base,
    firm_noise,
    firm_cluster,
    signs,
    covariates,
    whitening,
):
    owners = lax.axis_size("tiles")
    groups = lax.axis_size("reps")
    reps = signs.shape[0]
    covars = whitening.shape[0]
    omegas = chebyshev_weights(SWEEPS)

    def exchange(values, axes="tiles"):
        return lax.all_to_all(values, axes, 0, 0, tiled=True)

    def rows(values):
        return values.reshape(-1, CELLS)

    push_shape = ((owners, reps, CELLS), BF16)
    work_shape = ((WORK_BLOCKS, reps, CELLS), F32)
    firm_shape = ((FIRM_BLOCKS, reps, CELLS), F32)
    tiles = tiles_w.shape[0]
    plan_shape = ((8, 2 * tiles), jnp.int32)
    held_shape = ((tiles + 1, CELLS, CELLS), BF16, "keep")
    inverse_shape = ((WORK_BLOCKS, 8, CELLS), F32)
    inputs = (rows(tile_worker), rows(tile_owner), owner_block, tiles_w, signs)
    inputs += (rows(worker_base), rows(worker_noise), rows(worker_cluster))
    z, worker_outcome, held, turned, worker_inverse, plan = call(
        first_kernel,
        tuple(pltpu.with_memory_space_constraint(x, pltpu.HBM) for x in inputs),
        (((owners, reps + EXTRA, CELLS), BF16), work_shape, held_shape, held_shape, inverse_shape, plan_shape),
        (
            pltpu.SMEM((1, tiles), jnp.int32),
            pltpu.SMEM((1, tiles), jnp.int32),
            ((1, tiles), jnp.int32),
            ((1, tiles), jnp.int32),
            pltpu.SMEM(owner_block.shape, jnp.int32),
            (signs.shape, jnp.int32),
            ((WORK_BLOCKS, CELLS), F32),
            ((WORK_BLOCKS, CELLS), F32),
            ((WORK_BLOCKS, CELLS), jnp.int32),
            ((WORK_BLOCKS, reps + EXTRA, CELLS), BF16),
            ((owners, reps + EXTRA, CELLS), F32),
            inverse_shape,
            pltpu.SemaphoreType.DMA((9 + CHUNKS,)),
        ),
        specs=[HBM] * 8,
        name="first_push",
    )
    share = lax.axis_index("tiles").astype(jnp.int32).reshape(1)
    share, z = lax.optimization_barrier((share, z))
    z = exchange(z)
    send, firm_outcome, firm_inverse, flags, newer = call(
        open_firm_kernel,
        (z, signs, rows(firm_base), rows(firm_noise), rows(firm_cluster)),
        (push_shape, firm_shape, ((FIRM_BLOCKS, 8, CELLS), F32), ((owners, 8, CELLS), F32), firm_shape),
        name="first_firm",
    )
    older = None
    scratch = (work_shape, ((WORK_BLOCKS, reps, CELLS), BF16))
    scratch += (((owners, reps, CELLS), F32), pltpu.SMEM(*plan_shape), pltpu.SemaphoreType.DMA)
    for k in range(1, SWEEPS):
        last = k == SWEEPS - 1
        f = exchange(send)
        outputs = (push_shape,)
        if last:
            outputs += (((reps, WORK_BLOCKS * CELLS), F32, "keep"),)
        z, *rest = call(
            lambda *refs, e=last: sweep_kernel(e, *refs),
            (plan, keep(held), keep(turned), f, worker_outcome, worker_inverse),
            outputs,
            scratch,
            specs=[ANY] + [VMEM] * 5,
            name="sweep_close" if last else "sweep",
        )
        z = exchange(z)
        inputs = (z, firm_outcome, firm_inverse, flags) + (() if older is None else (older,))
        if not last:
            send, *now = call(
                lambda *refs, w=omegas[k], h=older is not None: firm_kernel(w, h, *refs),
                inputs,
                (push_shape, firm_shape) if k < SWEEPS - 2 else (push_shape,),
                name="firm",
            )
            older, newer = newer, now[0] if now else None
        else:
            firms, part = call(
                lambda *refs, w=omegas[k]: close_firm_kernel(w, *refs),
                inputs + (covariates, whitening),
                (firm_shape, ((reps * covars // CELLS, CELLS), F32)),
                name="close_firm",
            )
    part = exchange(part.reshape(owners, -1, CELLS))
    (spread,) = call(total_kernel, (part,), ((part.shape, F32),), name="total")
    everything = exchange(spread).reshape(-1, CELLS)
    (moment,) = call(
        moment_kernel,
        (share, everything),
        (((covars // owners, covars), F32),),
        (((CELLS, covars), F32),),
        scalars=1,
        name="moment",
    )
    workers = keep(rest[0])
    coefficients, firm_effect, worker_effect = call(
        emit_kernel,
        (everything, firms, workers),
        (((reps, covars), F32), ((reps, FIRM_BLOCKS * CELLS), F32), (workers.shape, F32)),
        (pltpu.SemaphoreType.DMA,),
        out_specs=[VMEM, VMEM, HBM],
        name="emit",
    )
    shifted = [lax.ppermute(moment, "reps", [(g, (g + d) % groups) for g in range(groups)]) for d in range(1, groups)]
    covariance = ((moment + shifted[1]) + (shifted[0] + shifted[2])) / (reps * groups)
    return (worker_effect, firm_effect, coefficients, covariance)


def solution(mesh):
    placed = (
        P("tiles", None, None),
        P("tiles"),
        P("tiles"),
        P("tiles", None),
        P("tiles"),
        P("tiles"),
        P("tiles"),
        P("tiles"),
        P("tiles"),
        P("tiles"),
        P("reps", None),
        P("tiles", None),
        P(),
    )
    return jax.shard_map(
        body,
        mesh=mesh,
        in_specs=placed,
        out_specs=(P("reps", "tiles"), P("reps", "tiles"), P("reps", None), P("tiles", None)),
        check_vma=False,
    )
```

```python
import jax
import jax.numpy as jnp
from jax import lax
from jax.experimental import pallas as pl
from jax.experimental.pallas import tpu as pltpu
from jax.sharding import PartitionSpec as P

WORK_BLOCKS = 16
FIRM_BLOCKS = 2
SWEEPS = 6
CELLS = 128
EXTRA = 8
SPECTRAL = 0.8
UNROLL = 64
CHUNKS = 4

F32 = jnp.float32
BF16 = jnp.bfloat16
HIGHEST = lax.Precision.HIGHEST

VMEM = pl.BlockSpec(memory_space=pltpu.VMEM)
SMEM = pl.BlockSpec(memory_space=pltpu.SMEM)
HBM = pl.BlockSpec(memory_space=pltpu.HBM)
ANY = pl.BlockSpec(memory_space=pl.ANY)
PARAMS = pltpu.CompilerParams(vmem_limit_bytes=20 << 20)


def chebyshev_weights(count):
    weights = [1.0, 1.0 / (1.0 - 0.5 * SPECTRAL * SPECTRAL)]
    while len(weights) < count:
        weights.append(1.0 / (1.0 - 0.25 * SPECTRAL * SPECTRAL * weights[-1]))
    return weights


def flip_table(signs_ref):
    return (2 * signs_ref[...] - 1).astype(F32).astype(BF16)


def outcome(flips, base, noise, cluster):
    hot = lax.broadcasted_iota(jnp.int32, (flips.shape[1], CELLS), 0) == cluster
    values = jnp.dot(flips, jnp.where(hot, 1.0, 0.0).astype(BF16), preferred_element_type=F32)
    return base + noise * values


def each_tile(count, step, unroll=UNROLL):
    def body(index, carry):
        step(index)
        return carry

    lax.fori_loop(0, count, body, 0, unroll=min(unroll, count))


def add_pairs(count, row, plan, w_ref, x_ref, acc_ref):
    def step(p):
        i = 2 * p
        values = jnp.concatenate([x_ref[plan[row + 2, i]], x_ref[plan[row + 2, i + 1]]], axis=1)
        pair = jnp.concatenate([w_ref[plan[row, i]], w_ref[plan[row, i + 1]]], axis=0)
        acc_ref[plan[row + 1, i]] += jnp.dot(values, pair, preferred_element_type=F32)

    each_tile(count, step, count)


def pair_plan(target, source, slots):
    tiles = target.shape[1]
    along = jnp.broadcast_to(target, (tiles, tiles))
    down = along.T
    sources = jnp.broadcast_to(source, (tiles, tiles)).T
    row = lax.broadcasted_iota(jnp.int32, (tiles, tiles), 0)
    column = lax.broadcasted_iota(jnp.int32, (tiles, tiles), 1)
    same = along == down

    def count(mask, axis):
        return jnp.sum(jnp.where(mask, 1.0, 0.0), axis=axis, keepdims=True)

    size = count(same, 0)
    odd = size - 2.0 * jnp.floor(0.5 * size)
    width = 1.0 + jnp.where(count(same & (row < column), 0) == 0.0, odd, 0.0)
    place = jnp.sum(jnp.where(along < down, width, 0.0), axis=1, keepdims=True) + count(same & (column < row), 1)
    numbers = row.astype(F32) - tiles
    plans = ([], [], [])
    for base in range(0, slots, tiles):
        here = place == column.astype(F32) + base
        plans[0].append(jnp.sum(jnp.where(here, numbers, 0.0), axis=0, keepdims=True) + tiles)
        plans[1].append(jnp.sum(jnp.where(here, down, 0.0), axis=0, keepdims=True))
        plans[2].append(jnp.sum(jnp.where(here, sources, 0.0), axis=0, keepdims=True))
    return [jnp.concatenate(plan, axis=1).astype(jnp.int32) for plan in plans]


def first_kernel(
    tw_hbm, to_hbm, ob_hbm, w_hbm, signs_hbm, base_hbm, noise_hbm, cluster_hbm,
    z_ref, wo_ref, w_ref, turned_ref, inv_ref, plan_ref,
    tw, to, tw_row, to_row, ob, signs_ref, base_ref, noise_ref, cluster_ref, x_ref, acc_ref, mass_ref, sems,
):
    small = [
        (signs_hbm, signs_ref),
        (cluster_hbm, cluster_ref),
        (base_hbm, base_ref),
        (noise_hbm, noise_ref),
        (tw_hbm, tw),
        (to_hbm, to),
        (ob_hbm, ob),
        (tw_hbm, tw_row),
        (to_hbm, to_row),
    ]
    copies = [pltpu.make_async_copy(source, target, sems.at[i]) for i, (source, target) in enumerate(small)]
    tiles = w_hbm.shape[0]
    chunk = tiles // CHUNKS
    loads = []
    for c in range(CHUNKS):
        part = pl.ds(c * chunk, chunk)
        loads.append(pltpu.make_async_copy(w_hbm.at[part], w_ref.at[part], sems.at[len(small) + c]))
    for copy in copies + loads:
        copy.start()
    acc_ref[...] = jnp.zeros_like(acc_ref)
    mass_ref[...] = jnp.zeros_like(mass_ref)
    w_ref[tiles] = jnp.zeros((CELLS, CELLS), BF16)
    turned_ref[tiles] = jnp.zeros((CELLS, CELLS), BF16)
    for copy in copies:
        copy.wait()
    reps = signs_ref.shape[0]
    flips = flip_table(signs_ref)
    for b in range(WORK_BLOCKS):
        row = slice(b, b + 1)
        value = outcome(flips, base_ref[row], noise_ref[row], cluster_ref[row])
        wo_ref[b] = value
        x_ref[b, :reps] = value.astype(BF16)
        x_ref[b, reps:] = jnp.ones((EXTRA, CELLS), BF16)

    def step(t):
        tile = w_ref[t]
        acc_ref[to[0, t]] += jnp.dot(x_ref[tw[0, t]], tile, preferred_element_type=F32)
        turned = tile.T
        turned_ref[t] = turned
        mass_ref[tw[0, t]] += jnp.sum(turned.astype(F32).reshape(CELLS // 8, 8, CELLS), axis=0)

    worker, owner = tw_row[...].astype(F32), to_row[...].astype(F32)
    pull = pair_plan(worker, owner, plan_ref.shape[1])
    push = pair_plan(owner, worker, plan_ref.shape[1])
    for r, values in enumerate(pull + push):
        plan_ref[r : r + 1] = values
    for c in range(CHUNKS):
        loads[c].wait()
        each_tile(chunk, lambda i, c=c: step(c * chunk + i))
    for b in range(WORK_BLOCKS):
        inverse = 1.0 / (1.0 + jnp.sum(mass_ref[b], axis=0, keepdims=True))
        inv_ref[b] = jnp.broadcast_to(inverse, (8, CELLS))
    place = lax.broadcasted_iota(jnp.int32, (EXTRA, CELLS), 0)

    def finish(o):
        z_ref[o, :reps] = acc_ref[o, :reps].astype(BF16)
        mass = acc_ref[o, reps:]
        high = mass.astype(BF16).astype(F32)
        middle = (mass - high).astype(BF16).astype(F32)
        low = (mass - high) - middle
        flag = ob[0, o].astype(F32)
        tail = jnp.where(place == 0, high, jnp.where(place == 1, middle, jnp.where(place == 2, low, flag)))
        z_ref[o, reps:] = tail.astype(BF16)

    each_tile(acc_ref.shape[0], finish, 8)


def sweep_kernel(last, *refs):
    plan_any, w_ref, turned_ref, f_ref, wo_ref, inv_ref, z_ref, *refs = refs
    if last:
        out_ref, *refs = refs
    accw_ref, x_ref, accz_ref, plan, sem = refs
    tables = pltpu.make_async_copy(plan_any, plan, sem)
    tables.start()
    tiles, owners = w_ref.shape[0] - 1, z_ref.shape[0]
    accw_ref[...] = jnp.zeros_like(accw_ref)
    accz_ref[...] = jnp.zeros_like(accz_ref)
    tables.wait()
    add_pairs((tiles + WORK_BLOCKS) // 2, 0, plan, turned_ref, f_ref, accw_ref)
    for b in range(WORK_BLOCKS):
        worker = wo_ref[b] - accw_ref[b] * inv_ref[b, :1]
        if last:
            out_ref[:, b * CELLS : (b + 1) * CELLS] = worker
        x_ref[b] = worker.astype(BF16)
    add_pairs((tiles + owners) // 2, 3, plan, w_ref, x_ref, accz_ref)
    z_ref[...] = accz_ref[...].astype(BF16)


def halves(value):
    high = value.astype(BF16)
    return high, (value - high.astype(F32)).astype(BF16)


def product(left, right, dims):
    (a, b), (c, d) = halves(left), halves(right)

    def dot(p, q):
        return lax.dot_general(p, q, (dims, ((), ())), preferred_element_type=F32)

    rows = a.shape[1 - dims[0][0]]
    both = dot(jnp.concatenate([a, b], axis=1 - dims[0][0]), c)
    return (dot(a, d) + both[rows:]) + both[:rows]


def gather_sums(z_ref, flags_ref, reps):
    zero = jnp.zeros((reps, CELLS), F32)

    def body(s, carry):
        first, second = carry
        part = z_ref[s, :reps].astype(F32)
        upper = jnp.broadcast_to(flags_ref[s, :1], part.shape) > 0.5
        return first + jnp.where(upper, 0.0, part), second + jnp.where(upper, part, 0.0)

    return lax.fori_loop(0, z_ref.shape[0], body, (zero, zero), unroll=16)


def scatter_firms(firms, flags_ref, send_ref):
    first, second = firms

    def step(s):
        upper = jnp.broadcast_to(flags_ref[s, :1], first.shape) > 0.5
        send_ref[s] = jnp.where(upper, second, first).astype(BF16)

    each_tile(send_ref.shape[0], step, 16)


def open_firm_kernel(z_ref, signs_ref, base_ref, noise_ref, cluster_ref, send_ref, fo_ref, inv_ref, flags_ref, now_ref):
    reps = signs_ref.shape[0]
    owners = z_ref.shape[0]
    mass = [jnp.zeros((1, CELLS), F32), jnp.zeros((1, CELLS), F32)]
    for s in range(owners):
        tail = z_ref[s, reps:].astype(F32)
        flags_ref[s] = jnp.broadcast_to(tail[3:4], (8, CELLS))
        part = tail[0:1] + tail[1:2] + tail[2:3]
        upper = tail[3:4] > 0.5
        mass = [mass[0] + jnp.where(upper, 0.0, part), mass[1] + jnp.where(upper, part, 0.0)]
    sums = gather_sums(z_ref, flags_ref, reps)
    flips = flip_table(signs_ref)
    firms = []
    for j in range(FIRM_BLOCKS):
        row = slice(j, j + 1)
        inverse = 1.0 / (1.0 + mass[j])
        value = outcome(flips, base_ref[row], noise_ref[row], cluster_ref[row])
        fo_ref[j] = value
        inv_ref[j] = jnp.broadcast_to(inverse, (8, CELLS))
        firm = value - sums[j] * inverse
        now_ref[j] = firm
        firms.append(firm)
    scatter_firms(firms, flags_ref, send_ref)


def next_firms(omega, z_ref, fo_ref, inv_ref, flags_ref, older_ref):
    sums = gather_sums(z_ref, flags_ref, z_ref.shape[1])
    firms = []
    for j in range(FIRM_BLOCKS):
        target = fo_ref[j] - sums[j] * inv_ref[j, :1]
        if older_ref is None:
            firms.append(omega * target)
        else:
            firms.append(older_ref[j] + omega * (target - older_ref[j]))
    return firms


def firm_kernel(omega, has_older, *refs):
    (z_ref, fo_ref, inv_ref, flags_ref), refs = refs[:4], refs[4:]
    older_ref = refs[0] if has_older else None
    send_ref, *now_ref = refs[1:] if has_older else refs
    firms = next_firms(omega, z_ref, fo_ref, inv_ref, flags_ref, older_ref)
    if now_ref:
        for j in range(FIRM_BLOCKS):
            now_ref[0][j] = firms[j]
    scatter_firms(firms, flags_ref, send_ref)


def close_firm_kernel(omega, z_ref, fo_ref, inv_ref, flags_ref, older_ref, cov_ref, white_ref, now_ref, part_ref):
    firms = next_firms(omega, z_ref, fo_ref, inv_ref, flags_ref, older_ref)
    for j in range(FIRM_BLOCKS):
        now_ref[j] = firms[j]
    projected = product(jnp.concatenate(firms, axis=1), cov_ref[...], ((1,), (0,)))
    whitened = product(projected, white_ref[...], ((1,), (1,)))
    reps = whitened.shape[0]
    columns = whitened.shape[1] // CELLS
    for c in range(columns):
        part_ref[pl.ds(c, reps, stride=columns)] = whitened[:, c * CELLS : (c + 1) * CELLS]


def total_kernel(part_ref, out_ref):
    total = jnp.sum(part_ref[...], axis=0)
    for s in range(out_ref.shape[0]):
        out_ref[s] = total


def moment_kernel(share, all_ref, moment_ref, rows_ref):
    share_rows, covars = moment_ref.shape
    columns = covars // CELLS
    reps = all_ref.shape[0] // columns
    in_block = CELLS // share_rows
    own = all_ref[pl.ds(share[0] // in_block, reps, stride=columns)]
    for c in range(columns):
        other = all_ref[pl.ds(c, reps, stride=columns)]
        rows_ref[:, c * CELLS : (c + 1) * CELLS] = product(own, other, ((0,), (0,)))
    start = pl.multiple_of((share[0] % in_block) * share_rows, share_rows)
    moment_ref[...] = rows_ref[pl.ds(start, share_rows)]


def emit_kernel(all_ref, now_ref, worker_ref, coef_ref, firm_ref, out_hbm, sem):
    copy = pltpu.make_async_copy(worker_ref, out_hbm, sem)
    copy.start()
    reps, covars = coef_ref.shape
    columns = covars // CELLS
    for c in range(columns):
        coef_ref[:, c * CELLS : (c + 1) * CELLS] = all_ref[pl.ds(c, reps, stride=columns)]
    for j in range(FIRM_BLOCKS):
        firm_ref[:, j * CELLS : (j + 1) * CELLS] = now_ref[j]
    copy.wait()


def keep(value):
    return pltpu.with_memory_space_constraint(value, pltpu.VMEM)


def call(kernel, inputs, outputs, scratch=(), scalars=0, name=None, specs=None, out_specs=None):
    return pl.pallas_call(
        kernel,
        in_specs=specs or [SMEM] * scalars + [VMEM] * (len(inputs) - scalars),
        out_specs=out_specs or [VMEM] * len(outputs),
        out_shape=[pltpu.VMEM(*item[:2]) if len(item) > 2 else jax.ShapeDtypeStruct(*item) for item in outputs],
        scratch_shapes=[item if not isinstance(item, tuple) else pltpu.VMEM(*item) for item in scratch],
        compiler_params=PARAMS,
        name=name,
    )(*inputs)


def body(
    tiles_w,
    tile_worker,
    tile_owner,
    owner_block,
    worker_base,
    worker_noise,
    worker_cluster,
    firm_base,
    firm_noise,
    firm_cluster,
    signs,
    covariates,
    whitening,
):
    owners = lax.axis_size("tiles")
    groups = lax.axis_size("reps")
    reps = signs.shape[0]
    covars = whitening.shape[0]
    omegas = chebyshev_weights(SWEEPS)

    def exchange(values, axes="tiles"):
        return lax.all_to_all(values, axes, 0, 0, tiled=True)

    def rows(values):
        return values.reshape(-1, CELLS)

    push_shape = ((owners, reps, CELLS), BF16)
    work_shape = ((WORK_BLOCKS, reps, CELLS), F32)
    firm_shape = ((FIRM_BLOCKS, reps, CELLS), F32)
    tiles = tiles_w.shape[0]
    plan_shape = ((8, 2 * tiles), jnp.int32)
    held_shape = ((tiles + 1, CELLS, CELLS), BF16, "keep")
    inverse_shape = ((WORK_BLOCKS, 8, CELLS), F32)
    inputs = (rows(tile_worker), rows(tile_owner), owner_block, tiles_w, signs)
    inputs += (rows(worker_base), rows(worker_noise), rows(worker_cluster))
    z, worker_outcome, held, turned, worker_inverse, plan = call(
        first_kernel,
        tuple(pltpu.with_memory_space_constraint(x, pltpu.HBM) for x in inputs),
        (((owners, reps + EXTRA, CELLS), BF16), work_shape, held_shape, held_shape, inverse_shape, plan_shape),
        (
            pltpu.SMEM((1, tiles), jnp.int32),
            pltpu.SMEM((1, tiles), jnp.int32),
            ((1, tiles), jnp.int32),
            ((1, tiles), jnp.int32),
            pltpu.SMEM(owner_block.shape, jnp.int32),
            (signs.shape, jnp.int32),
            ((WORK_BLOCKS, CELLS), F32),
            ((WORK_BLOCKS, CELLS), F32),
            ((WORK_BLOCKS, CELLS), jnp.int32),
            ((WORK_BLOCKS, reps + EXTRA, CELLS), BF16),
            ((owners, reps + EXTRA, CELLS), F32),
            inverse_shape,
            pltpu.SemaphoreType.DMA((9 + CHUNKS,)),
        ),
        specs=[HBM] * 8,
        name="first_push",
    )
    share = lax.axis_index("tiles").astype(jnp.int32).reshape(1)
    share, z = lax.optimization_barrier((share, z))
    z = exchange(z)
    send, firm_outcome, firm_inverse, flags, newer = call(
        open_firm_kernel,
        (z, signs, rows(firm_base), rows(firm_noise), rows(firm_cluster)),
        (push_shape, firm_shape, ((FIRM_BLOCKS, 8, CELLS), F32), ((owners, 8, CELLS), F32), firm_shape),
        name="first_firm",
    )
    older = None
    scratch = (work_shape, ((WORK_BLOCKS, reps, CELLS), BF16))
    scratch += (((owners, reps, CELLS), F32), pltpu.SMEM(*plan_shape), pltpu.SemaphoreType.DMA)
    for k in range(1, SWEEPS):
        last = k == SWEEPS - 1
        f = exchange(send)
        outputs = (push_shape,)
        if last:
            outputs += (((reps, WORK_BLOCKS * CELLS), F32, "keep"),)
        z, *rest = call(
            lambda *refs, e=last: sweep_kernel(e, *refs),
            (plan, keep(held), keep(turned), f, worker_outcome, worker_inverse),
            outputs,
            scratch,
            specs=[ANY] + [VMEM] * 5,
            name="sweep_close" if last else "sweep",
        )
        z = exchange(z)
        inputs = (z, firm_outcome, firm_inverse, flags) + (() if older is None else (older,))
        if not last:
            send, *now = call(
                lambda *refs, w=omegas[k], h=older is not None: firm_kernel(w, h, *refs),
                inputs,
                (push_shape, firm_shape) if k < SWEEPS - 2 else (push_shape,),
                name="firm",
            )
            older, newer = newer, now[0] if now else None
        else:
            firms, part = call(
                lambda *refs, w=omegas[k]: close_firm_kernel(w, *refs),
                inputs + (covariates, whitening),
                (firm_shape, ((reps * covars // CELLS, CELLS), F32)),
                name="close_firm",
            )
    part = exchange(part.reshape(owners, -1, CELLS))
    (spread,) = call(total_kernel, (part,), ((part.shape, F32),), name="total")
    everything = exchange(spread).reshape(-1, CELLS)
    (moment,) = call(
        moment_kernel,
        (share, everything),
        (((covars // owners, covars), F32),),
        (((CELLS, covars), F32),),
        scalars=1,
        name="moment",
    )
    workers = keep(rest[0])
    coefficients, firm_effect, worker_effect = call(
        emit_kernel,
        (everything, firms, workers),
        (((reps, covars), F32), ((reps, FIRM_BLOCKS * CELLS), F32), (workers.shape, F32)),
        (pltpu.SemaphoreType.DMA,),
        out_specs=[VMEM, VMEM, HBM],
        name="emit",
    )
    shifted = [lax.ppermute(moment, "reps", [(g, (g + d) % groups) for g in range(groups)]) for d in range(1, groups)]
    covariance = ((moment + shifted[1]) + (shifted[0] + shifted[2])) / (reps * groups)
    return (worker_effect, firm_effect, coefficients, covariance)


def solution(mesh):
    placed = (
        P("tiles", None, None),
        P("tiles"),
        P("tiles"),
        P("tiles", None),
        P("tiles"),
        P("tiles"),
        P("tiles"),
        P("tiles"),
        P("tiles"),
        P("tiles"),
        P("reps", None),
        P("tiles", None),
        P(),
    )
    return jax.shard_map(
        body,
        mesh=mesh,
        in_specs=placed,
        out_specs=(P("reps", "tiles"), P("reps", "tiles"), P("reps", None), P("tiles", None)),
        check_vma=False,
    )
```
